128 devices in a mesh: lon: 8 (over z, y_hi), lat: 16 (over y_lo, x, core).
Axes of the slice: x: 4, y: 4 (y_hi: 2, y_lo: 2; y = y_hi * 2 + y_lo), z: 4, core: 2. Of those that a mesh axis runs over, the one named last changes fastest.
Arguments:
- fields: float32 [4, 8, 1024, 3600], P(None, None, 'lat', 'lon'), may hold values from -6 to 6
- thickness: float32 [8], replicated, may hold values from 5 to 250
- cutoff: int32 [256], replicated, may hold values from 2 to 1800
- barotropic: float32 [3, 1024, 3600], P(None, 'lat', 'lon'), may hold values from -6 to 6
- land_sea: int32 [1024, 3600], P('lat', 'lon'), may hold values 0 or 1
Outputs:
- filtered_tracers: float32 [2, 8, 1024, 3600], P(None, None, 'lat', 'lon')
- velocity: float32 [2, 8, 1024, 3600], P(None, None, 'lat', 'lon')
- sea_level: float32 [1024, 3600], P('lat', 'lon')
The draws below stay inside these ranges and needn't reach their ends.
Inputs may be any that keep to these rules, and one draw needn't show every extreme that they name: `cutoff`: each filtered row's highest kept wavenumber.
All inputs are finite; a program needn't handle non-finite values. No bound on the sum of `land_sea` on one device may be relied on, other than what follows from the above.
Results may differ from the reference program's by a relative error of at most 0.0003.
Values sent between devices are 32-bit elements; how exact they have to be, the bound alone decides.
A program may use at most 128 MiB of HBM per device.

```python
import math
import jax
import jax.numpy as jnp
from jax import lax

NLON = 3600
LEV = 8
SUB = 20
NLAT = 1024
NPOLE = 128


def touch_ends(drawn, own_key, smallest, largest):
    extent = drawn.shape
    index_at = [jax.random.randint(jax.random.fold_in(own_key, axis), (), 0, extent[axis]) for axis in range(len(extent))]
    drawn = drawn.at[tuple(index_at)].set(smallest)
    longest = extent.index(max(extent))
    index_at[longest] = (index_at[longest] + 1) % extent[longest]
    return drawn.at[tuple(index_at)].set(largest)


def shard_levels(own_key, dims, split, least, top_value):
    def one(dim, shards_of):
        heights = jax.random.uniform(jax.random.fold_in(jax.random.fold_in(own_key, 6), dim), (shards_of,), jnp.float32, least / len(split), top_value / len(split))
        return jnp.repeat(jnp.exp(heights), dims[dim] // shards_of).reshape((-1,) + (1,) * (len(dims) - dim - 1))

    level = one(*split[0])
    for cut in split[1:]:
        level = level * one(*cut)
    return level


def gaussian(rng, dims, scale, most, shards=(), kind=jnp.bfloat16):
    drawn = scale * jax.random.normal(rng, dims, jnp.float32)
    if shards:
        drawn = drawn * shard_levels(rng, dims, shards, -0.22, 0.18)
    return jnp.clip(drawn, -most, most).astype(kind)


def setup_inputs(seed: int = 0) -> dict:
    arg_keys = jax.random.split(jax.random.key(seed), 6)
    fields = gaussian(arg_keys[0], (4, LEV, NLAT, NLON), 1.0, 6.0, ((2, 16), (3, 8)), jnp.float32)
    thickness = jnp.clip(jnp.exp(jax.random.uniform(arg_keys[1], (LEV,), jnp.float32, math.log(5.0), math.log(250.0))), 5.0, 250.0)
    cutoff = touch_ends(jax.random.randint(arg_keys[2], (2 * NPOLE,), 2, NLON // 2 + 1), jax.random.fold_in(arg_keys[2], 1), 2, (NLON // 2 + 1) - 1).astype(jnp.int32)
    barotropic = gaussian(arg_keys[3], (3, NLAT, NLON), 1.0, 6.0, ((1, 16), (2, 8)), jnp.float32)
    land_sea = touch_ends((jax.random.randint(arg_keys[4], (NLAT, NLON), 0, 5) < 4).astype(jnp.int32), jax.random.fold_in(arg_keys[4], 1), 0, 1)
    return {"fields": fields, "thickness": thickness, "cutoff": cutoff, "barotropic": barotropic, "land_sea": land_sea}


wave_coef = 0.65


def polar_filter(values, row_cuts):
    circle_len = values.shape[-1]
    spectrum = jnp.fft.rfft(values, axis=-1)
    wavenumber = jnp.arange(circle_len // 2 + 1)
    kept_mask = wavenumber[None, :] <= row_cuts[:, None]
    return jnp.fft.irfft(spectrum * kept_mask, n=circle_len, axis=-1).astype(values.dtype)


def reference(fields, thickness, cutoff, barotropic, land_sea):
    total_rows = fields.shape[2]
    pole_rows = cutoff.shape[0] // 2
    north_rows = polar_filter(fields[:, :, :pole_rows], cutoff[:pole_rows])
    south_rows = polar_filter(fields[:, :, total_rows - pole_rows:], cutoff[pole_rows:])
    filtered = jnp.concatenate([north_rows, fields[:, :, pole_rows:total_rows - pole_rows], south_rows], axis=2)
    ocean_cell = land_sea.astype(fields.dtype)
    row_number = jnp.arange(total_rows)
    east_open = ocean_cell * jnp.roll(ocean_cell, -1, 1)
    north_open = ocean_cell * jnp.roll(ocean_cell, -1, 0) * (row_number != total_rows - 1).astype(fields.dtype)[:, None]
    surface = barotropic[0]
    eastward = barotropic[1] * east_open
    northward = barotropic[2] * north_open
    for subcycle in range(SUB):
        divergence = eastward - jnp.roll(eastward, 1, 1) + northward - jnp.roll(northward, 1, 0)
        surface = surface - wave_coef * ocean_cell * divergence
        eastward = east_open * (eastward - wave_coef * (jnp.roll(surface, -1, 1) - surface))
        northward = north_open * (northward - wave_coef * (jnp.roll(surface, -1, 0) - surface))
    weights = thickness / jnp.sum(thickness)
    currents = filtered[2:]
    column = jnp.einsum("k,ckij->cij", weights, currents, precision=lax.Precision.HIGHEST)
    velocity = jnp.stack([east_open, north_open])[:, None] * (currents - column[:, None] + jnp.stack([eastward, northward])[:, None])
    return filtered[:2], velocity, surface
```

```python
import math

import jax
import jax.numpy as jnp
import ml_dtypes
import numpy as np
from jax import lax
from jax.experimental import pallas as pl
from jax.experimental.pallas import tpu as pltpu
from jax.sharding import PartitionSpec as P

MESH = pl.DeviceIdType.MESH
ANY = pl.ANY
VMEM = pltpu.VMEM

WAVE = 0.65
SUB = 20
POLE_DEV = 2
LON, LAT = 8, 16
ROWS, COLS = 64, 450
NLON = LON * COLS
NLAT = LAT * ROWS
LEV = 8
NF = 4
WIDE = 512
HALO = 24
EXT = ROWS + 2 * HALO
TILE = 8
LANE_TILES = ((0, 128), (128, 256), (256, 384), (384, COLS))


def tables():
    r = np.arange(COLS)
    angle = 2.0 * np.pi * ((r[:, None] * r[None, :]) % COLS) / COLS
    full = np.zeros((WIDE, 2 * WIDE), np.float64)
    full[:COLS, :COLS] = np.cos(angle)
    full[:COLS, WIDE : WIDE + COLS] = np.sin(angle)
    full = full.astype(np.float32)
    high = full.astype(ml_dtypes.bfloat16)
    low = (full - high.astype(np.float32)).astype(ml_dtypes.bfloat16)
    turn = 2.0 * np.pi * (np.arange(LON)[:, None] * r[None, :]) / NLON
    twist = np.zeros((2, LON, WIDE), np.float32)
    twist[0, :, :COLS] = np.cos(turn)
    twist[1, :, :COLS] = np.sin(turn)
    return high, low, twist


def butterflies(z, sign):
    n = len(z)
    if n == 1:
        return z
    even = butterflies(z[0::2], sign)
    odd = butterflies(z[1::2], sign)
    low, high = [], []
    for k in range(n // 2):
        er, ei = even[k]
        tr, ti = odd[k]
        if 4 * k == n:
            tr, ti = (-ti, tr) if sign > 0 else (ti, -tr)
        elif k:
            c = math.cos(2.0 * math.pi * k / n)
            s = sign * math.sin(2.0 * math.pi * k / n)
            tr, ti = c * tr - s * ti, c * ti + s * tr
        low.append((er + tr, ei + ti))
        high.append((er - tr, ei - ti))
    return low + high


def put_split(high_ref, low_ref, row, lanes, value):
    top = value.astype(jnp.bfloat16)
    high_ref[row : row + 16, lanes[0] : lanes[1]] = top
    low_ref[row : row + 16, lanes[0] : lanes[1]] = (value - top.astype(jnp.float32)).astype(jnp.bfloat16)


def multiply(high_ref, low_ref, wh_ref, wl_ref, out_ref):
    for block in range(4):
        cols = slice(block * 256, (block + 1) * 256)
        out_ref[:, cols] = (
            jnp.dot(high_ref[...], wh_ref[:, cols], preferred_element_type=jnp.float32)
            + jnp.dot(low_ref[...], wh_ref[:, cols], preferred_element_type=jnp.float32)
            + jnp.dot(high_ref[...], wl_ref[:, cols], preferred_element_type=jnp.float32)
        )


def filter_chunk(j, recv, back, twist, mask, yh, yl, wh, wl, prod):
    for lo, hi in LANE_TILES:
        z = []
        for d in range(LON):
            re = recv[j, d, 0:2, :, lo:hi].reshape(16, hi - lo)
            im = recv[j, d, 2:4, :, lo:hi].reshape(16, hi - lo)
            z.append((re, im))
        y = butterflies(z, -1)
        for s in range(LON):
            re, im = y[s]
            if s:
                c = twist[0, s : s + 1, lo:hi]
                n = twist[1, s : s + 1, lo:hi]
                re, im = re * c + im * n, im * c - re * n
            put_split(yh, yl, s * 32, (lo, hi), re)
            put_split(yh, yl, s * 32 + 16, (lo, hi), im)
    multiply(yh, yl, wh, wl, prod)
    for lo, hi in LANE_TILES:
        for s in range(LON):
            a = slice(s * 32, s * 32 + 16)
            b = slice(s * 32 + 16, s * 32 + 32)
            keep = mask[s, :, lo:hi]
            re = (prod[a, lo:hi] + prod[b, WIDE + lo : WIDE + hi]) * keep
            im = (prod[b, lo:hi] - prod[a, WIDE + lo : WIDE + hi]) * keep
            put_split(yh, yl, s * 32, (lo, hi), re)
            put_split(yh, yl, s * 32 + 16, (lo, hi), im)
    multiply(yh, yl, wh, wl, prod)
    for lo, hi in LANE_TILES:
        z = []
        for s in range(LON):
            a = slice(s * 32, s * 32 + 16)
            b = slice(s * 32 + 16, s * 32 + 32)
            re = prod[a, lo:hi] - prod[b, WIDE + lo : WIDE + hi]
            im = prod[b, lo:hi] + prod[a, WIDE + lo : WIDE + hi]
            if s:
                c = twist[0, s : s + 1, lo:hi]
                n = twist[1, s : s + 1, lo:hi]
                re, im = re * c - im * n, im * c + re * n
            z.append((re, im))
        x = butterflies(z, 1)
        for d in range(LON):
            back[j, d, 0:2, :, lo:hi] = x[d][0].reshape(2, 8, hi - lo)
            back[j, d, 2:4, :, lo:hi] = x[d][1].reshape(2, 8, hi - lo)


def wave_kernel(
    fields, baro, land, cutoff, wh_hbm, wl_hbm, twist,
    filt, state_out, open_out,
    recv, back, wh, wl, yh, yl, prod, mask,
    own, own_land, src4, st_c, st_l, st_r, ext, opens, res_state, res_open,
    fwd_send, fwd_recv, ret_send, ret_recv, halo_send, halo_recv, local_sem,
):
    lon = lax.axis_index("lon")
    lat = lax.axis_index("lat")
    polar = (lat < POLE_DEV) | (lat >= LAT - POLE_DEV)
    partner = lax.rem(lat + LAT // 2, LAT)
    worker = (partner < POLE_DEV) | (partner >= LAT - POLE_DEV)

    load_state = pltpu.make_async_copy(baro, own, local_sem.at[0])
    load_land = pltpu.make_async_copy(land, own_land, local_sem.at[1])
    load_state.start()
    load_land.start()
    load_wh = pltpu.make_async_copy(wh_hbm, wh, local_sem.at[2])
    load_wl = pltpu.make_async_copy(wl_hbm, wl, local_sem.at[3])

    @pl.when(worker)
    def _():
        load_wh.start()
        load_wl.start()

    def near(dx, dy):
        return {"lon": lax.rem(lon + dx + LON, LON), "lat": lax.rem(lat + dy + LAT, LAT)}

    sides = [(dx, dy) for dx in (-1, 0, 1) for dy in (-1, 0, 1) if (dx, dy) != (0, 0)]
    barrier = pltpu.get_barrier_semaphore()
    for dx, dy in sides:
        pl.semaphore_signal(barrier, inc=1, device_id=near(dx, dy), device_id_type=MESH)

    @pl.when(polar | worker)
    def _():
        def greet(t, _):
            pl.semaphore_signal(barrier, inc=1, device_id={"lon": t, "lat": partner}, device_id_type=MESH)
            return 0

        lax.fori_loop(0, LON, greet, 0)
        pl.semaphore_wait(barrier, len(sides) + LON)

    @pl.when(jnp.logical_not(polar | worker))
    def _():
        pl.semaphore_wait(barrier, len(sides))

    def send_level(j, _):
        def send_one(t, _):
            pltpu.make_async_remote_copy(
                src_ref=fields.at[:, j, pl.ds(pl.multiple_of(t * TILE, TILE), TILE), :],
                dst_ref=recv.at[j, lon],
                send_sem=fwd_send,
                recv_sem=fwd_recv.at[j],
                device_id={"lon": t, "lat": partner},
                device_id_type=MESH,
            ).start()
            return 0

        lax.fori_loop(0, LON, send_one, 0)
        return 0

    @pl.when(polar)
    def _():
        send_level(0, 0)

    load_state.wait()
    load_land.wait()
    for c in range(3):
        src4[c, :, 0:384] = own[c, :, 0:384]
        src4[c, :, 384:COLS] = own[c, :, 384:COLS]
    src4[3, :, 0:384] = own_land[:, 0:384].astype(jnp.float32)
    src4[3, :, 384:COLS] = own_land[:, 384:COLS].astype(jnp.float32)
    zero_pad = jnp.zeros((4, ROWS, WIDE - COLS), jnp.float32)
    src4[:, :, COLS:WIDE] = zero_pad

    row_src = {1: slice(ROWS - HALO, ROWS), 0: slice(0, ROWS), -1: slice(0, HALO)}
    row_dst = {1: slice(0, HALO), 0: slice(HALO, HALO + ROWS), -1: slice(HALO + ROWS, EXT)}
    copies = []
    for n, (dx, dy) in enumerate(sides):
        if dx == 0:
            src = src4.at[:, row_src[dy], :]
            dst = st_c.at[:, row_dst[dy], :]
        elif dx == 1:
            src = src4.at[:, row_src[dy], 384:512]
            dst = st_l.at[:, row_dst[dy], :]
        else:
            src = src4.at[:, row_src[dy], 0:128]
            dst = st_r.at[:, row_dst[dy], :]
        copy = pltpu.make_async_remote_copy(
            src_ref=src, dst_ref=dst, send_sem=halo_send.at[n], recv_sem=halo_recv.at[n],
            device_id=near(dx, dy), device_id_type=MESH,
        )
        copy.start()
        copies.append(copy)

    @pl.when(polar)
    def _():
        lax.fori_loop(1, LEV, send_level, 0)

    st_c[:, HALO : HALO + ROWS, :] = src4[...]
    for copy in copies:
        copy.wait()

    lane128 = lax.broadcasted_iota(jnp.int32, (EXT, 128), 1)
    for c in range(4):
        mid = pltpu.roll(st_c[c], HALO, 1)
        ext[c, :, 128:384] = mid[:, 128:384]
        left = pltpu.roll(st_l[c], 128 - (COLS - HALO - 384), 1)
        ext[c, :, 0:128] = jnp.where(lane128 < HALO, left, mid[:, 0:128])
        right = pltpu.roll(st_r[c], HALO + COLS - 384, 1)
        ext[c, :, 384:512] = jnp.where(lane128 >= HALO + COLS - 384, right, mid[:, 384:512])

    ocean = ext[3]
    row_id = lax.rem(lat * ROWS - HALO + NLAT + lax.broadcasted_iota(jnp.int32, (EXT, WIDE), 0), NLAT)
    east_open = ocean * pltpu.roll(ocean, WIDE - 1, 1)
    north_open = jnp.where(row_id == NLAT - 1, 0.0, ocean * pltpu.roll(ocean, EXT - 1, 0))
    opens[0] = east_open
    opens[1] = north_open
    ext[1] = ext[1] * east_open
    ext[2] = ext[2] * north_open
    ext[3] = WAVE * ocean

    def subcycle(_, carry):
        east = ext[1]
        north = ext[2]
        div = east - pltpu.roll(east, 1, 1) + north - pltpu.roll(north, 1, 0)
        surface = ext[0] - ext[3] * div
        ext[0] = surface
        ext[1] = opens[0] * (east - WAVE * (pltpu.roll(surface, WIDE - 1, 1) - surface))
        ext[2] = opens[1] * (north - WAVE * (pltpu.roll(surface, EXT - 1, 0) - surface))
        return carry

    lax.fori_loop(0, SUB, subcycle, 0)

    inner = slice(HALO, HALO + ROWS)
    for c in range(3):
        moved = pltpu.roll(ext[c, inner, :], WIDE - HALO, 1)
        res_state[c] = moved[:, :COLS]
    for c in range(2):
        moved = pltpu.roll(opens[c, inner, :], WIDE - HALO, 1)
        res_open[c] = moved[:, :COLS]
    save_state = pltpu.make_async_copy(res_state, state_out, local_sem.at[0])
    save_open = pltpu.make_async_copy(res_open, open_out, local_sem.at[1])
    save_state.start()
    save_open.start()

    @pl.when(worker)
    def _():
        load_wh.wait()
        load_wl.wait()
        top = jnp.where(partner < POLE_DEV, partner, partner - (LAT - 2 * POLE_DEV))
        first = top * ROWS + lon * TILE
        sub = lax.rem(lax.broadcasted_iota(jnp.int32, (16, WIDE), 0), TILE)
        wave = LON * lax.broadcasted_iota(jnp.int32, (16, WIDE), 1)
        limit = jnp.zeros((16, WIDE), jnp.int32)
        for i in range(TILE):
            limit = jnp.where(sub == i, cutoff[first + i], limit)
        for s in range(LON):
            m = wave + s
            folded = jnp.minimum(m, NLON - m)
            mask[s] = jnp.where(folded <= limit, 1.0 / NLON, 0.0)
        yh[...] = jnp.zeros_like(yh)
        yl[...] = jnp.zeros_like(yl)

        def chunk(j, _):
            pltpu.make_async_copy(recv.at[j], recv.at[j], fwd_recv.at[j]).wait()
            filter_chunk(j, recv, back, twist, mask, yh, yl, wh, wl, prod)

            def reply(d, _):
                pltpu.make_async_remote_copy(
                    src_ref=back.at[j, d],
                    dst_ref=filt.at[:, j, pl.ds(pl.multiple_of(lon * TILE, TILE), TILE), :],
                    send_sem=ret_send,
                    recv_sem=ret_recv,
                    device_id={"lon": d, "lat": partner},
                    device_id_type=MESH,
                ).start()
                return 0

            lax.fori_loop(0, LON, reply, 0)
            return 0

        lax.fori_loop(0, LEV, chunk, 0)
        pltpu.make_async_copy(back, back, ret_send).wait()

    @pl.when(polar)
    def _():
        pltpu.make_async_copy(fields, fields, fwd_send).wait()
        pltpu.make_async_copy(filt, filt, ret_recv).wait()

    save_state.wait()
    save_open.wait()


def final_kernel(polar, thick, fields, filt, state, opens, tracers, velocity, sea):
    total = thick[0]
    for k in range(1, LEV):
        total = total + thick[k]
    sea[...] = state[0]

    def finish(source):
        tracers[...] = source[0:2]
        for c in range(2):
            column = None
            for k in range(LEV):
                term = (thick[k] / total) * source[2 + c, k]
                column = term if column is None else column + term
            shift = state[1 + c] - column
            gate = opens[c]
            for k in range(LEV):
                velocity[c, k] = gate * (source[2 + c, k] + shift)

    @pl.when(polar[0] == 1)
    def _():
        finish(filt)

    @pl.when(polar[0] == 0)
    def _():
        finish(fields)


def body(fields, thickness, cutoff, barotropic, land_sea):
    f32 = jnp.float32
    high, low, twist = tables()
    sds = jax.ShapeDtypeStruct
    filt, state, opens = pl.pallas_call(
        wave_kernel,
        out_shape=(
            sds((NF, LEV, ROWS, COLS), f32),
            sds((3, ROWS, COLS), f32),
            sds((2, ROWS, COLS), f32),
        ),
        in_specs=[
            pl.BlockSpec(memory_space=ANY),
            pl.BlockSpec(memory_space=ANY),
            pl.BlockSpec(memory_space=ANY),
            pl.BlockSpec(memory_space=pltpu.SMEM),
            pl.BlockSpec(memory_space=ANY),
            pl.BlockSpec(memory_space=ANY),
            pl.BlockSpec(memory_space=VMEM),
        ],
        out_specs=[pl.BlockSpec(memory_space=ANY)] * 3,
        scratch_shapes=[
            VMEM((LEV, LON, NF, TILE, COLS), f32),
            VMEM((LEV, LON, NF, TILE, COLS), f32),
            VMEM((WIDE, 2 * WIDE), jnp.bfloat16),
            VMEM((WIDE, 2 * WIDE), jnp.bfloat16),
            VMEM((256, WIDE), jnp.bfloat16),
            VMEM((256, WIDE), jnp.bfloat16),
            VMEM((256, 2 * WIDE), f32),
            VMEM((LON, 16, WIDE), f32),
            VMEM((3, ROWS, COLS), f32),
            VMEM((ROWS, COLS), jnp.int32),
            VMEM((4, ROWS, WIDE), f32),
            VMEM((4, EXT, WIDE), f32),
            VMEM((4, EXT, 128), f32),
            VMEM((4, EXT, 128), f32),
            VMEM((4, EXT, WIDE), f32),
            VMEM((2, EXT, WIDE), f32),
            VMEM((3, ROWS, COLS), f32),
            VMEM((2, ROWS, COLS), f32),
            pltpu.SemaphoreType.DMA,
            pltpu.SemaphoreType.DMA((LEV,)),
            pltpu.SemaphoreType.DMA,
            pltpu.SemaphoreType.DMA,
            pltpu.SemaphoreType.DMA((8,)),
            pltpu.SemaphoreType.DMA((8,)),
            pltpu.SemaphoreType.DMA((4,)),
        ],
        compiler_params=pltpu.CompilerParams(
            collective_id=0, has_side_effects=True, vmem_limit_bytes=60 * 1024 * 1024
        ),
        name="wave",
    )(fields, barotropic, land_sea, cutoff, jnp.asarray(high), jnp.asarray(low), jnp.asarray(twist))

    lat = lax.axis_index("lat")
    polar = ((lat < POLE_DEV) | (lat >= LAT - POLE_DEV)).astype(jnp.int32).reshape(1)
    rows = lambda i, p: (0, i, 0)
    return tuple(
        pl.pallas_call(
            final_kernel,
            out_shape=(
                sds((2, LEV, ROWS, COLS), f32),
                sds((2, LEV, ROWS, COLS), f32),
                sds((ROWS, COLS), f32),
            ),
            grid_spec=pltpu.PrefetchScalarGridSpec(
                num_scalar_prefetch=1,
                grid=(ROWS // TILE,),
                in_specs=[
                    pl.BlockSpec(memory_space=pltpu.SMEM),
                    pl.BlockSpec((NF, LEV, TILE, COLS), lambda i, p: (0, 0, i * (1 - p[0]), 0)),
                    pl.BlockSpec((NF, LEV, TILE, COLS), lambda i, p: (0, 0, i * p[0], 0)),
                    pl.BlockSpec((3, TILE, COLS), rows),
                    pl.BlockSpec((2, TILE, COLS), rows),
                ],
                out_specs=[
                    pl.BlockSpec((2, LEV, TILE, COLS), lambda i, p: (0, 0, i, 0)),
                    pl.BlockSpec((2, LEV, TILE, COLS), lambda i, p: (0, 0, i, 0)),
                    pl.BlockSpec((TILE, COLS), lambda i, p: (i, 0)),
                ],
            ),
            name="final",
        )(polar, thickness, fields, filt, state, opens)
    )


def solution(mesh):
    return jax.shard_map(
        body,
        mesh=mesh,
        in_specs=(P(None, None, "lat", "lon"), P(), P(), P(None, "lat", "lon"), P("lat", "lon")),
        out_specs=(P(None, None, "lat", "lon"), P(None, None, "lat", "lon"), P("lat", "lon")),
        check_vma=False,
    )
```

```python
import math

import jax
import jax.numpy as jnp
import ml_dtypes
import numpy as np
from jax import lax
from jax.experimental import pallas as pl
from jax.experimental.pallas import tpu as pltpu
from jax.sharding import PartitionSpec as P

MESH = pl.DeviceIdType.MESH
ANY = pl.ANY
VMEM = pltpu.VMEM

WAVE = 0.65
SUB = 20
POLE_DEV = 2
LON, LAT = 8, 16
ROWS, COLS = 64, 450
NLON = LON * COLS
NLAT = LAT * ROWS
LEV = 8
NF = 4
WIDE = 512
HALO = 24
EXT = ROWS + 2 * HALO
TILE = 8
NEAR_LEV = 6
PER_CHUNK = 4
LANE_TILES = ((0, 128), (128, 256), (256, 384), (384, COLS))


def tables():
    r = np.arange(COLS)
    angle = 2.0 * np.pi * ((r[:, None] * r[None, :]) % COLS) / COLS
    full = np.zeros((WIDE, 2 * WIDE), np.float64)
    full[:COLS, :COLS] = np.cos(angle)
    full[:COLS, WIDE : WIDE + COLS] = np.sin(angle)
    full = full.astype(np.float32)
    high = full.astype(ml_dtypes.bfloat16)
    low = (full - high.astype(np.float32)).astype(ml_dtypes.bfloat16)
    turn = 2.0 * np.pi * (np.arange(LON)[:, None] * r[None, :]) / NLON
    twist = np.zeros((2, LON, WIDE), np.float32)
    twist[0, :, :COLS] = np.cos(turn)
    twist[1, :, :COLS] = np.sin(turn)
    return high, low, twist


def butterflies(z, sign):
    n = len(z)
    if n == 1:
        return z
    even = butterflies(z[0::2], sign)
    odd = butterflies(z[1::2], sign)
    low, high = [], []
    for k in range(n // 2):
        er, ei = even[k]
        tr, ti = odd[k]
        if 4 * k == n:
            tr, ti = (-ti, tr) if sign > 0 else (ti, -tr)
        elif k:
            c = math.cos(2.0 * math.pi * k / n)
            s = sign * math.sin(2.0 * math.pi * k / n)
            tr, ti = c * tr - s * ti, c * ti + s * tr
        low.append((er + tr, ei + ti))
        high.append((er - tr, ei - ti))
    return low + high


def put_split(high_ref, low_ref, row, lanes, value):
    top = value.astype(jnp.bfloat16)
    high_ref[row : row + 16, lanes[0] : lanes[1]] = top
    low_ref[row : row + 16, lanes[0] : lanes[1]] = (value - top.astype(jnp.float32)).astype(jnp.bfloat16)


def multiply(high_ref, low_ref, wh_ref, wl_ref, out_ref):
    for block in range(4):
        cols = slice(block * 256, (block + 1) * 256)
        out_ref[:, cols] = (
            jnp.dot(high_ref[...], wh_ref[:, cols], preferred_element_type=jnp.float32)
            + jnp.dot(low_ref[...], wh_ref[:, cols], preferred_element_type=jnp.float32)
            + jnp.dot(high_ref[...], wl_ref[:, cols], preferred_element_type=jnp.float32)
        )


def filter_chunk(j, recv, back, twist, mask, yh, yl, wh, wl, prod):
    for lo, hi in LANE_TILES:
        z = []
        for d in range(LON):
            re = recv[j, d, 0:2, :, lo:hi].reshape(16, hi - lo)
            im = recv[j, d, 2:4, :, lo:hi].reshape(16, hi - lo)
            z.append((re, im))
        y = butterflies(z, -1)
        for s in range(LON):
            re, im = y[s]
            if s:
                c = twist[0, s : s + 1, lo:hi]
                n = twist[1, s : s + 1, lo:hi]
                re, im = re * c + im * n, im * c - re * n
            put_split(yh, yl, s * 32, (lo, hi), re)
            put_split(yh, yl, s * 32 + 16, (lo, hi), im)
    multiply(yh, yl, wh, wl, prod)
    for lo, hi in LANE_TILES:
        for s in range(LON):
            a = slice(s * 32, s * 32 + 16)
            b = slice(s * 32 + 16, s * 32 + 32)
            keep = mask[s, :, lo:hi]
            re = (prod[a, lo:hi] + prod[b, WIDE + lo : WIDE + hi]) * keep
            im = (prod[b, lo:hi] - prod[a, WIDE + lo : WIDE + hi]) * keep
            put_split(yh, yl, s * 32, (lo, hi), re)
            put_split(yh, yl, s * 32 + 16, (lo, hi), im)
    multiply(yh, yl, wh, wl, prod)
    for lo, hi in LANE_TILES:
        z = []
        for s in range(LON):
            a = slice(s * 32, s * 32 + 16)
            b = slice(s * 32 + 16, s * 32 + 32)
            re = prod[a, lo:hi] - prod[b, WIDE + lo : WIDE + hi]
            im = prod[b, lo:hi] + prod[a, WIDE + lo : WIDE + hi]
            if s:
                c = twist[0, s : s + 1, lo:hi]
                n = twist[1, s : s + 1, lo:hi]
                re, im = re * c - im * n, im * c + re * n
            z.append((re, im))
        x = butterflies(z, 1)
        for d in range(LON):
            back[j, d, 0:2, :, lo:hi] = x[d][0].reshape(2, 8, hi - lo)
            back[j, d, 2:4, :, lo:hi] = x[d][1].reshape(2, 8, hi - lo)


def wave_kernel(
    fields, baro, land, cutoff, wh_hbm, wl_hbm, twist,
    filt, state_out, open_out,
    recv, back, relay, wh, wl, yh, yl, prod, mask,
    own, own_land, src4, edge_r, edge_l, st_c, st_l, st_r, ext, opens, res_state, res_open,
    fwd_send, fwd_recv, ret_send, ret_recv, relay_recv, relay_send, halo_send, halo_recv, local_sem,
):
    lon = lax.axis_index("lon")
    lat = lax.axis_index("lat")
    pair = lat // 2
    core = lax.rem(lat, 2)
    north = lax.rem(pair, 4) < 2
    polar = (pair == 0) | (pair == 7)
    near_y = (pair == 3) | (pair == 4)
    relays = (pair == 1) | (pair == 6)
    far = (pair == 2) | (pair == 5)
    worker = near_y | far
    home = jnp.where(north, 0, LAT - 2) + core
    y_lat = jnp.where(north, 8, 6) + core
    relay_lat = jnp.where(north, 2, 12) + core
    far_lat = jnp.where(north, 10, 4) + core

    load_state = pltpu.make_async_copy(baro, own, local_sem.at[0])
    load_land = pltpu.make_async_copy(land, own_land, local_sem.at[1])
    load_state.start()
    load_land.start()
    load_wh = pltpu.make_async_copy(wh_hbm, wh, local_sem.at[2])
    load_wl = pltpu.make_async_copy(wl_hbm, wl, local_sem.at[3])

    @pl.when(worker)
    def _():
        load_wh.start()
        load_wl.start()

    sides = [(dx, dy) for dy in (0, 1, -1) for dx in (-1, 0, 1) if (dx, dy) != (0, 0)]

    def near(dx, dy):
        return {"lon": lax.rem(lon + dx + LON, LON), "lat": lax.rem(lat + dy + LAT, LAT)}

    def inside(dy):
        return lat < LAT - 1 if dy > 0 else lat > 0

    def when_inside(dy, action):
        if dy == 0:
            action()
        else:
            pl.when(inside(dy))(action)

    barrier = pltpu.get_barrier_semaphore()

    def greet_at(lon_index, lat_index):
        pl.semaphore_signal(
            barrier, inc=1, device_id={"lon": lon_index, "lat": lat_index}, device_id_type=MESH
        )

    def greet_row(lat_index):
        def one(t, _):
            greet_at(t, lat_index)
            return 0

        lax.fori_loop(0, LON, one, 0)

    for dx, dy in sides:
        when_inside(dy, lambda dx=dx, dy=dy: greet_at(near(dx, dy)["lon"], near(dx, dy)["lat"]))

    @pl.when(polar)
    def _():
        greet_row(y_lat)
        greet_row(far_lat)
        greet_at(lon, relay_lat)

    @pl.when(near_y)
    def _():
        greet_row(home)

    @pl.when(far)
    def _():
        greet_row(home)
        greet_row(relay_lat)

    @pl.when(relays)
    def _():
        greet_row(far_lat)
        greet_at(lon, home)

    load_state.wait()
    load_land.wait()
    for c in range(3):
        src4[c, :, 0:384] = own[c, :, 0:384]
        src4[c, :, 384:COLS] = own[c, :, 384:COLS]
    src4[3, :, 0:384] = own_land[:, 0:384].astype(jnp.float32)
    src4[3, :, 384:COLS] = own_land[:, 384:COLS].astype(jnp.float32)
    src4[:, :, COLS:WIDE] = jnp.zeros((4, ROWS, WIDE - COLS), jnp.float32)
    st_c[:, HALO : HALO + ROWS, :] = src4[...]
    lane = lax.broadcasted_iota(jnp.int32, (ROWS, 128), 1)
    right_pack = jnp.zeros((ROWS, 128), jnp.float32)
    left_pack = right_pack
    for c in range(4):
        here = (lane >= c * HALO) & (lane < (c + 1) * HALO)
        right_edge = pltpu.roll(src4[c, :, 384:512], (c * HALO - (COLS - HALO - 384)) % 128, 1)
        left_edge = src4[c, :, 0:128]
        if c:
            left_edge = pltpu.roll(left_edge, c * HALO, 1)
        right_pack = jnp.where(here, right_edge, right_pack)
        left_pack = jnp.where(here, left_edge, left_pack)
    edge_r[...] = right_pack
    edge_l[...] = left_pack

    full = len(sides) - jnp.where((lat == 0) | (lat == LAT - 1), 3, 0)
    extra = jnp.where(polar, 2 * LON + 1, jnp.where(near_y, LON, jnp.where(far, 2 * LON, LON + 1)))
    pl.semaphore_wait(barrier, full + extra)

    def send_level(level, slot, lat_index):
        def send_one(t, _):
            pltpu.make_async_remote_copy(
                src_ref=fields.at[:, level, pl.ds(pl.multiple_of(t * TILE, TILE), TILE), :],
                dst_ref=recv.at[slot, lon],
                send_sem=fwd_send,
                recv_sem=fwd_recv.at[slot],
                device_id={"lon": t, "lat": lat_index},
                device_id_type=MESH,
            ).start()
            return 0

        lax.fori_loop(0, LON, send_one, 0)

    @pl.when(polar)
    def _():
        send_level(0, 0, y_lat)

    row_src = {1: slice(ROWS - HALO, ROWS), 0: slice(0, ROWS), -1: slice(0, HALO)}
    row_dst = {1: slice(0, HALO), 0: slice(HALO, HALO + ROWS), -1: slice(HALO + ROWS, EXT)}
    copies = []
    for n, (dx, dy) in enumerate(sides):
        if dx == 0:
            src = src4.at[:, row_src[dy], :]
            dst = st_c.at[:, row_dst[dy], :]
        else:
            src = (edge_r if dx == 1 else edge_l).at[row_src[dy], :]
            dst = (st_l if dx == 1 else st_r).at[row_dst[dy], :]
        copy = pltpu.make_async_remote_copy(
            src_ref=src, dst_ref=dst, send_sem=halo_send.at[n], recv_sem=halo_recv.at[n],
            device_id=near(dx, dy), device_id_type=MESH,
        )
        when_inside(dy, copy.start)
        copies.append((dy, copy))

    @pl.when(polar)
    def _():
        for level in range(NEAR_LEV, LEV):
            send_level(level, level - NEAR_LEV, far_lat)
            step = level - NEAR_LEV
            send_level(1 + step, 1 + step, y_lat)

        def more(level, _):
            send_level(level, level, y_lat)
            return 0

        lax.fori_loop(1 + LEV - NEAR_LEV, NEAR_LEV, more, 0)

    for dy, copy in copies:
        when_inside(dy, copy.wait_send)
        when_inside(-dy, copy.wait_recv)
    for dy in (1, -1):
        @pl.when(jnp.logical_not(inside(-dy)))
        def _(dy=dy):
            st_c[:, row_dst[dy], :] = jnp.zeros((4, HALO, WIDE), jnp.float32)
            st_l[row_dst[dy], :] = jnp.zeros((HALO, 128), jnp.float32)
            st_r[row_dst[dy], :] = jnp.zeros((HALO, 128), jnp.float32)

    lane_ext = lax.broadcasted_iota(jnp.int32, (EXT, 128), 1)
    edge = HALO + COLS - 384
    for c in range(4):
        mid = pltpu.roll(st_c[c], HALO, 1)
        ext[c, :, 128:384] = mid[:, 128:384]
        left = pltpu.roll(st_l[...], 128 - c * HALO, 1) if c else st_l[...]
        ext[c, :, 0:128] = jnp.where(lane_ext < HALO, left, mid[:, 0:128])
        right = pltpu.roll(st_r[...], (edge - c * HALO) % 128, 1)
        right = jnp.where(lane_ext < edge + HALO, right, 0.0)
        ext[c, :, 384:512] = jnp.where(lane_ext >= edge, right, mid[:, 384:512])

    ocean = ext[3]
    row_id = lat * ROWS - HALO + lax.broadcasted_iota(jnp.int32, (EXT, WIDE), 0)
    east_open = ocean * pltpu.roll(ocean, WIDE - 1, 1)
    north_open = jnp.where(row_id == NLAT - 1, 0.0, ocean * pltpu.roll(ocean, EXT - 1, 0))
    opens[0] = east_open
    opens[1] = north_open
    ext[1] = ext[1] * east_open
    ext[2] = ext[2] * north_open
    ext[3] = WAVE * ocean

    def subcycle(_, carry):
        east = ext[1]
        north = ext[2]
        div = east - pltpu.roll(east, 1, 1) + north - pltpu.roll(north, 1, 0)
        surface = ext[0] - ext[3] * div
        ext[0] = surface
        ext[1] = opens[0] * (east - WAVE * (pltpu.roll(surface, WIDE - 1, 1) - surface))
        ext[2] = opens[1] * (north - WAVE * (pltpu.roll(surface, EXT - 1, 0) - surface))
        return carry

    chunks = jnp.where(near_y, NEAR_LEV, jnp.where(far, LEV - NEAR_LEV, 0))

    @pl.when(worker)
    def _():
        load_wh.wait()
        load_wl.wait()
        first = (jnp.where(north, 0, 2) + core) * ROWS + lon * TILE
        sub = lax.rem(lax.broadcasted_iota(jnp.int32, (16, WIDE), 0), TILE)
        wave = LON * lax.broadcasted_iota(jnp.int32, (16, WIDE), 1)
        limit = jnp.zeros((16, WIDE), jnp.int32)
        for i in range(TILE):
            limit = jnp.where(sub == i, cutoff[first + i], limit)
        for s in range(LON):
            m = wave + s
            folded = jnp.minimum(m, NLON - m)
            mask[s] = jnp.where(folded <= limit, 1.0 / NLON, 0.0)
        yh[...] = jnp.zeros_like(yh)
        yl[...] = jnp.zeros_like(yl)

        def chunk(j, _):
            pltpu.make_async_copy(recv.at[j], recv.at[j], fwd_recv.at[j]).wait()
            filter_chunk(j, recv, back, twist, mask, yh, yl, wh, wl, prod)

            @pl.when(near_y)
            def _():
                def reply(d, _):
                    pltpu.make_async_remote_copy(
                        src_ref=back.at[j, d],
                        dst_ref=filt.at[:, j, pl.ds(pl.multiple_of(lon * TILE, TILE), TILE), :],
                        send_sem=ret_send.at[j],
                        recv_sem=ret_recv,
                        device_id={"lon": d, "lat": home},
                        device_id_type=MESH,
                    ).start()
                    return 0

                lax.fori_loop(0, LON, reply, 0)

            @pl.when(far)
            def _():
                def reply(d, _):
                    pltpu.make_async_remote_copy(
                        src_ref=back.at[j, d],
                        dst_ref=relay.at[j, lon],
                        send_sem=ret_send.at[j],
                        recv_sem=relay_recv.at[j, lon],
                        device_id={"lon": d, "lat": relay_lat},
                        device_id_type=MESH,
                    ).start()
                    return 0

                lax.fori_loop(0, LON, reply, 0)

            lax.fori_loop(0, jnp.where(j < SUB // PER_CHUNK, PER_CHUNK, 0), subcycle, 0)
            return 0

        lax.fori_loop(0, chunks, chunk, 0)

    left_over = SUB - PER_CHUNK * jnp.minimum(chunks, SUB // PER_CHUNK)
    lax.fori_loop(0, left_over, subcycle, 0)

    inner = slice(HALO, HALO + ROWS)
    for c in range(3):
        moved = pltpu.roll(ext[c, inner, :], WIDE - HALO, 1)
        res_state[c] = moved[:, :COLS]
    for c in range(2):
        moved = pltpu.roll(opens[c, inner, :], WIDE - HALO, 1)
        res_open[c] = moved[:, :COLS]
    save_state = pltpu.make_async_copy(res_state, state_out, local_sem.at[0])
    save_open = pltpu.make_async_copy(res_open, open_out, local_sem.at[1])
    save_state.start()
    save_open.start()

    @pl.when(relays)
    def _():
        for j in range(LEV - NEAR_LEV):
            def pass_on(t, _, j=j):
                here = relay.at[j, t]
                pltpu.make_async_copy(here, here, relay_recv.at[j, t]).wait()
                pltpu.make_async_remote_copy(
                    src_ref=here,
                    dst_ref=filt.at[:, NEAR_LEV + j, pl.ds(pl.multiple_of(t * TILE, TILE), TILE), :],
                    send_sem=relay_send,
                    recv_sem=ret_recv,
                    device_id={"lon": lon, "lat": home},
                    device_id_type=MESH,
                ).start()
                return 0

            lax.fori_loop(0, LON, pass_on, 0)
        pltpu.make_async_copy(relay, relay, relay_send).wait()

    @pl.when(worker)
    def _():
        def sent(j, _):
            pltpu.make_async_copy(back.at[j], back.at[j], ret_send.at[j]).wait()
            return 0

        lax.fori_loop(0, chunks, sent, 0)

    @pl.when(polar)
    def _():
        pltpu.make_async_copy(fields, fields, fwd_send).wait()
        pltpu.make_async_copy(filt, filt, ret_recv).wait()

    save_state.wait()
    save_open.wait()


def final_kernel(polar, thick, fields, filt, state, opens, tracers, velocity, sea):
    total = thick[0]
    for k in range(1, LEV):
        total = total + thick[k]
    sea[...] = state[0]

    def finish(source):
        tracers[...] = source[0:2]
        for c in range(2):
            column = None
            for k in range(LEV):
                term = (thick[k] / total) * source[2 + c, k]
                column = term if column is None else column + term
            shift = state[1 + c] - column
            gate = opens[c]
            for k in range(LEV):
                velocity[c, k] = gate * (source[2 + c, k] + shift)

    @pl.when(polar[0] == 1)
    def _():
        finish(filt)

    @pl.when(polar[0] == 0)
    def _():
        finish(fields)


def body(fields, thickness, cutoff, barotropic, land_sea):
    f32 = jnp.float32
    high, low, twist = tables()
    sds = jax.ShapeDtypeStruct
    filt, state, opens = pl.pallas_call(
        wave_kernel,
        out_shape=(
            sds((NF, LEV, ROWS, COLS), f32),
            sds((3, ROWS, COLS), f32),
            sds((2, ROWS, COLS), f32),
        ),
        in_specs=[
            pl.BlockSpec(memory_space=ANY),
            pl.BlockSpec(memory_space=ANY),
            pl.BlockSpec(memory_space=ANY),
            pl.BlockSpec(memory_space=pltpu.SMEM),
            pl.BlockSpec(memory_space=ANY),
            pl.BlockSpec(memory_space=ANY),
            pl.BlockSpec(memory_space=VMEM),
        ],
        out_specs=[pl.BlockSpec(memory_space=ANY)] * 3,
        scratch_shapes=[
            VMEM((NEAR_LEV, LON, NF, TILE, COLS), f32),
            VMEM((NEAR_LEV, LON, NF, TILE, COLS), f32),
            VMEM((LEV - NEAR_LEV, LON, NF, TILE, COLS), f32),
            VMEM((WIDE, 2 * WIDE), jnp.bfloat16),
            VMEM((WIDE, 2 * WIDE), jnp.bfloat16),
            VMEM((256, WIDE), jnp.bfloat16),
            VMEM((256, WIDE), jnp.bfloat16),
            VMEM((256, 2 * WIDE), f32),
            VMEM((LON, 16, WIDE), f32),
            VMEM((3, ROWS, COLS), f32),
            VMEM((ROWS, COLS), jnp.int32),
            VMEM((4, ROWS, WIDE), f32),
            VMEM((ROWS, 128), f32),
            VMEM((ROWS, 128), f32),
            VMEM((4, EXT, WIDE), f32),
            VMEM((EXT, 128), f32),
            VMEM((EXT, 128), f32),
            VMEM((4, EXT, WIDE), f32),
            VMEM((2, EXT, WIDE), f32),
            VMEM((3, ROWS, COLS), f32),
            VMEM((2, ROWS, COLS), f32),
            pltpu.SemaphoreType.DMA,
            pltpu.SemaphoreType.DMA((NEAR_LEV,)),
            pltpu.SemaphoreType.DMA((NEAR_LEV,)),
            pltpu.SemaphoreType.DMA,
            pltpu.SemaphoreType.DMA((LEV - NEAR_LEV, LON)),
            pltpu.SemaphoreType.DMA,
            pltpu.SemaphoreType.DMA((8,)),
            pltpu.SemaphoreType.DMA((8,)),
            pltpu.SemaphoreType.DMA((4,)),
        ],
        compiler_params=pltpu.CompilerParams(
            collective_id=0, has_side_effects=True, vmem_limit_bytes=60 * 1024 * 1024
        ),
        name="wave",
    )(fields, barotropic, land_sea, cutoff, jnp.asarray(high), jnp.asarray(low), jnp.asarray(twist))

    lat = lax.axis_index("lat")
    polar = ((lat < POLE_DEV) | (lat >= LAT - POLE_DEV)).astype(jnp.int32).reshape(1)
    rows = lambda i, p: (0, i, 0)
    return tuple(
        pl.pallas_call(
            final_kernel,
            out_shape=(
                sds((2, LEV, ROWS, COLS), f32),
                sds((2, LEV, ROWS, COLS), f32),
                sds((ROWS, COLS), f32),
            ),
            grid_spec=pltpu.PrefetchScalarGridSpec(
                num_scalar_prefetch=1,
                grid=(ROWS // TILE,),
                in_specs=[
                    pl.BlockSpec(memory_space=pltpu.SMEM),
                    pl.BlockSpec((NF, LEV, TILE, COLS), lambda i, p: (0, 0, i * (1 - p[0]), 0)),
                    pl.BlockSpec((NF, LEV, TILE, COLS), lambda i, p: (0, 0, i * p[0], 0)),
                    pl.BlockSpec((3, TILE, COLS), rows),
                    pl.BlockSpec((2, TILE, COLS), rows),
                ],
                out_specs=[
                    pl.BlockSpec((2, LEV, TILE, COLS), lambda i, p: (0, 0, i, 0)),
                    pl.BlockSpec((2, LEV, TILE, COLS), lambda i, p: (0, 0, i, 0)),
                    pl.BlockSpec((TILE, COLS), lambda i, p: (i, 0)),
                ],
            ),
            name="final",
        )(polar, thickness, fields, filt, state, opens)
    )


def solution(mesh):
    return jax.shard_map(
        body,
        mesh=mesh,
        in_specs=(P(None, None, "lat", "lon"), P(), P(), P(None, "lat", "lon"), P("lat", "lon")),
        out_specs=(P(None, None, "lat", "lon"), P(None, None, "lat", "lon"), P("lat", "lon")),
        check_vma=False,
    )
```

```python
import math

import jax
import jax.numpy as jnp
import ml_dtypes
import numpy as np
from jax import lax
from jax.experimental import pallas as pl
from jax.experimental.pallas import tpu as pltpu
from jax.sharding import PartitionSpec as P

MESH = pl.DeviceIdType.MESH
ANY = pl.ANY
VMEM = pltpu.VMEM

WAVE = 0.65
SUB = 20
POLE_DEV = 2
LON, LAT = 8, 16
ROWS, COLS = 64, 450
NLON = LON * COLS
NLAT = LAT * ROWS
LEV = 8
NF = 4
WIDE = 512
HALO = 24
EXT = ROWS + 2 * HALO
TILE = 8
CHUNKS = 16
NEAR = 11
FAR = CHUNKS - NEAR
PER_CHUNK = 2
LANE_TILES = ((0, 128), (128, 256), (256, 384), (384, COLS))


def tables():
    r = np.arange(COLS)
    angle = 2.0 * np.pi * ((r[:, None] * r[None, :]) % COLS) / COLS
    full = np.zeros((WIDE, 2 * WIDE), np.float64)
    full[:COLS, :COLS] = np.cos(angle)
    full[:COLS, WIDE : WIDE + COLS] = np.sin(angle)
    full = full.astype(np.float32)
    high = full.astype(ml_dtypes.bfloat16)
    low = (full - high.astype(np.float32)).astype(ml_dtypes.bfloat16)
    turn = 2.0 * np.pi * (np.arange(LON)[:, None] * r[None, :]) / NLON
    twist = np.zeros((2, LON, WIDE), np.float32)
    twist[0, :, :COLS] = np.cos(turn)
    twist[1, :, :COLS] = np.sin(turn)
    return high, low, twist


def butterflies(z, sign):
    n = len(z)
    if n == 1:
        return z
    even = butterflies(z[0::2], sign)
    odd = butterflies(z[1::2], sign)
    low, high = [], []
    for k in range(n // 2):
        er, ei = even[k]
        tr, ti = odd[k]
        if 4 * k == n:
            tr, ti = (-ti, tr) if sign > 0 else (ti, -tr)
        elif k:
            c = math.cos(2.0 * math.pi * k / n)
            s = sign * math.sin(2.0 * math.pi * k / n)
            tr, ti = c * tr - s * ti, c * ti + s * tr
        low.append((er + tr, ei + ti))
        high.append((er - tr, ei - ti))
    return low + high


def put_split(high_ref, low_ref, s, lanes, re, im):
    value = jnp.concatenate([re, im], axis=0)
    top = value.astype(jnp.bfloat16)
    rows = slice(s * 16, s * 16 + 16)
    high_ref[rows, lanes[0] : lanes[1]] = top
    low_ref[rows, lanes[0] : lanes[1]] = (value - top.astype(jnp.float32)).astype(jnp.bfloat16)


def multiply(high_ref, low_ref, wh_ref, wl_ref, out_ref):
    for block in range(4):
        cols = slice(block * 256, (block + 1) * 256)
        out_ref[:, cols] = (
            jnp.dot(high_ref[...], wh_ref[:, cols], preferred_element_type=jnp.float32)
            + jnp.dot(low_ref[...], wh_ref[:, cols], preferred_element_type=jnp.float32)
            + jnp.dot(high_ref[...], wl_ref[:, cols], preferred_element_type=jnp.float32)
        )


def filter_chunk(j, recv, back, twist, mask, yh, yl, wh, wl, prod):
    for lo, hi in LANE_TILES:
        z = [(recv[j, d, 0, :, lo:hi], recv[j, d, 1, :, lo:hi]) for d in range(LON)]
        y = butterflies(z, -1)
        for s in range(LON):
            re, im = y[s]
            if s:
                c = twist[0, s : s + 1, lo:hi]
                n = twist[1, s : s + 1, lo:hi]
                re, im = re * c + im * n, im * c - re * n
            put_split(yh, yl, s, (lo, hi), re, im)
    multiply(yh, yl, wh, wl, prod)
    for lo, hi in LANE_TILES:
        for s in range(LON):
            a = slice(s * 16, s * 16 + 8)
            b = slice(s * 16 + 8, s * 16 + 16)
            keep = mask[s, :, lo:hi]
            re = (prod[a, lo:hi] + prod[b, WIDE + lo : WIDE + hi]) * keep
            im = (prod[b, lo:hi] - prod[a, WIDE + lo : WIDE + hi]) * keep
            put_split(yh, yl, s, (lo, hi), re, im)
    multiply(yh, yl, wh, wl, prod)
    for lo, hi in LANE_TILES:
        z = []
        for s in range(LON):
            a = slice(s * 16, s * 16 + 8)
            b = slice(s * 16 + 8, s * 16 + 16)
            re = prod[a, lo:hi] - prod[b, WIDE + lo : WIDE + hi]
            im = prod[b, lo:hi] + prod[a, WIDE + lo : WIDE + hi]
            if s:
                c = twist[0, s : s + 1, lo:hi]
                n = twist[1, s : s + 1, lo:hi]
                re, im = re * c - im * n, im * c + re * n
            z.append((re, im))
        x = butterflies(z, 1)
        for d in range(LON):
            back[j, d, 0, :, lo:hi] = x[d][0]
            back[j, d, 1, :, lo:hi] = x[d][1]


def wave_kernel(
    fields, baro, land, cutoff, wh_hbm, wl_hbm, twist,
    filt, state_out, open_out,
    recv, back, relay, wh, wl, yh, yl, prod, mask,
    own, own_land, src4, edge_r, edge_l, st_c, st_l, st_r, ext, opens,
    fwd_send, fwd_recv, ret_send, ret_recv, relay_recv, relay_send, halo_send, halo_recv, local_sem,
):
    lon = lax.axis_index("lon")
    lat = lax.axis_index("lat")
    pair = lat // 2
    core = lax.rem(lat, 2)
    north = lax.rem(pair, 4) < 2
    polar = (pair == 0) | (pair == 7)
    near_y = (pair == 3) | (pair == 4)
    relays = (pair == 1) | (pair == 6)
    far = (pair == 2) | (pair == 5)
    worker = near_y | far
    home = jnp.where(north, 0, LAT - 2) + core
    y_lat = jnp.where(north, 8, 6) + core
    relay_lat = jnp.where(north, 2, 12) + core
    far_lat = jnp.where(north, 10, 4) + core

    load_state = pltpu.make_async_copy(baro, own, local_sem.at[0])
    load_land = pltpu.make_async_copy(land, own_land, local_sem.at[1])
    load_state.start()
    load_land.start()
    load_wh = pltpu.make_async_copy(wh_hbm, wh, local_sem.at[2])
    load_wl = pltpu.make_async_copy(wl_hbm, wl, local_sem.at[3])

    keep_own = pltpu.make_async_copy(fields, filt, local_sem.at[4])

    @pl.when(worker)
    def _():
        load_wh.start()
        load_wl.start()

    @pl.when(jnp.logical_not(polar))
    def _():
        keep_own.start()

    sides = [(dx, dy) for dy in (0, 1, -1) for dx in (-1, 0, 1) if (dx, dy) != (0, 0)]

    def near(dx, dy):
        return {"lon": lax.rem(lon + dx + LON, LON), "lat": lax.rem(lat + dy + LAT, LAT)}

    def inside(dy):
        return lat < LAT - 1 if dy > 0 else lat > 0

    def when_inside(dy, action):
        if dy == 0:
            action()
        else:
            pl.when(inside(dy))(action)

    barrier = pltpu.get_barrier_semaphore()

    def greet_at(lon_index, lat_index):
        pl.semaphore_signal(
            barrier, inc=1, device_id={"lon": lon_index, "lat": lat_index}, device_id_type=MESH
        )

    def greet_row(lat_index):
        def one(t, _):
            greet_at(t, lat_index)
            return 0

        lax.fori_loop(0, LON, one, 0)

    for dx, dy in sides:
        when_inside(dy, lambda dx=dx, dy=dy: greet_at(near(dx, dy)["lon"], near(dx, dy)["lat"]))

    @pl.when(polar)
    def _():
        greet_row(y_lat)
        greet_row(far_lat)
        greet_at(lon, relay_lat)

    @pl.when(near_y)
    def _():
        greet_row(home)

    @pl.when(far)
    def _():
        greet_row(home)
        greet_row(relay_lat)

    @pl.when(relays)
    def _():
        greet_row(far_lat)
        greet_at(lon, home)

    load_state.wait()
    load_land.wait()
    for c in range(3):
        src4[c, :, 0:384] = own[c, :, 0:384]
        src4[c, :, 384:COLS] = own[c, :, 384:COLS]
    src4[3, :, 0:384] = own_land[:, 0:384].astype(jnp.float32)
    src4[3, :, 384:COLS] = own_land[:, 384:COLS].astype(jnp.float32)
    src4[:, :, COLS:WIDE] = jnp.zeros((4, ROWS, WIDE - COLS), jnp.float32)
    st_c[:, HALO : HALO + ROWS, :] = src4[...]
    lane = lax.broadcasted_iota(jnp.int32, (ROWS, 128), 1)
    right_pack = jnp.zeros((ROWS, 128), jnp.float32)
    left_pack = right_pack
    for c in range(4):
        here = (lane >= c * HALO) & (lane < (c + 1) * HALO)
        right_edge = pltpu.roll(src4[c, :, 384:512], (c * HALO - (COLS - HALO - 384)) % 128, 1)
        left_edge = src4[c, :, 0:128]
        if c:
            left_edge = pltpu.roll(left_edge, c * HALO, 1)
        right_pack = jnp.where(here, right_edge, right_pack)
        left_pack = jnp.where(here, left_edge, left_pack)
    edge_r[...] = right_pack
    edge_l[...] = left_pack

    full = len(sides) - jnp.where((lat == 0) | (lat == LAT - 1), 3, 0)
    extra = jnp.where(polar, 2 * LON + 1, jnp.where(near_y, LON, jnp.where(far, 2 * LON, LON + 1)))
    pl.semaphore_wait(barrier, full + extra)

    def rows_of(ref, q, t):
        return ref.at[:, q // LEV, lax.rem(q, LEV), pl.ds(pl.multiple_of(t * TILE, TILE), TILE), :]

    def send_chunk(q, slot, lat_index):
        def send_one(t, _):
            pltpu.make_async_remote_copy(
                src_ref=rows_of(fields, q, t),
                dst_ref=recv.at[slot, lon],
                send_sem=fwd_send,
                recv_sem=fwd_recv.at[slot],
                device_id={"lon": t, "lat": lat_index},
                device_id_type=MESH,
            ).start()
            return 0

        lax.fori_loop(0, LON, send_one, 0)

    @pl.when(polar)
    def _():
        send_chunk(0, 0, y_lat)

    row_src = {1: slice(ROWS - HALO, ROWS), 0: slice(0, ROWS), -1: slice(0, HALO)}
    row_dst = {1: slice(0, HALO), 0: slice(HALO, HALO + ROWS), -1: slice(HALO + ROWS, EXT)}
    copies = []
    for n, (dx, dy) in enumerate(sides):
        if dx == 0:
            src = src4.at[:, row_src[dy], :]
            dst = st_c.at[:, row_dst[dy], :]
        else:
            src = (edge_r if dx == 1 else edge_l).at[row_src[dy], :]
            dst = (st_l if dx == 1 else st_r).at[row_dst[dy], :]
        copy = pltpu.make_async_remote_copy(
            src_ref=src, dst_ref=dst, send_sem=halo_send.at[n], recv_sem=halo_recv.at[n],
            device_id=near(dx, dy), device_id_type=MESH,
        )
        when_inside(dy, copy.start)
        copies.append((dy, copy))

    @pl.when(polar)
    def _():
        def more(k, _):
            send_chunk(NEAR + k, k, far_lat)
            send_chunk(2 * k + 1, 2 * k + 1, y_lat)
            send_chunk(2 * k + 2, 2 * k + 2, y_lat)
            return 0

        lax.fori_loop(0, FAR, more, 0)

    for dy, copy in copies:
        when_inside(dy, copy.wait_send)
        when_inside(-dy, copy.wait_recv)
    for dy in (1, -1):
        @pl.when(jnp.logical_not(inside(-dy)))
        def _(dy=dy):
            st_c[:, row_dst[dy], :] = jnp.zeros((4, HALO, WIDE), jnp.float32)
            st_l[row_dst[dy], :] = jnp.zeros((HALO, 128), jnp.float32)
            st_r[row_dst[dy], :] = jnp.zeros((HALO, 128), jnp.float32)

    lane_ext = lax.broadcasted_iota(jnp.int32, (EXT, 128), 1)
    edge = HALO + COLS - 384
    for c in range(4):
        mid = pltpu.roll(st_c[c], HALO, 1)
        ext[c, :, 128:384] = mid[:, 128:384]
        left = pltpu.roll(st_l[...], 128 - c * HALO, 1) if c else st_l[...]
        ext[c, :, 0:128] = jnp.where(lane_ext < HALO, left, mid[:, 0:128])
        right = pltpu.roll(st_r[...], (edge - c * HALO) % 128, 1)
        right = jnp.where(lane_ext < edge + HALO, right, 0.0)
        ext[c, :, 384:512] = jnp.where(lane_ext >= edge, right, mid[:, 384:512])

    ocean = ext[3]
    row_id = lat * ROWS - HALO + lax.broadcasted_iota(jnp.int32, (EXT, WIDE), 0)
    east_open = ocean * pltpu.roll(ocean, WIDE - 1, 1)
    north_open = jnp.where(row_id == NLAT - 1, 0.0, ocean * pltpu.roll(ocean, EXT - 1, 0))
    opens[0] = east_open
    opens[1] = north_open
    ext[1] = ext[1] * east_open
    ext[2] = ext[2] * north_open
    ext[3] = WAVE * ocean

    def subcycle(_, carry):
        east = ext[1]
        north = ext[2]
        div = east - pltpu.roll(east, 1, 1) + north - pltpu.roll(north, 1, 0)
        surface = ext[0] - ext[3] * div
        ext[0] = surface
        ext[1] = opens[0] * (east - WAVE * (pltpu.roll(surface, WIDE - 1, 1) - surface))
        ext[2] = opens[1] * (north - WAVE * (pltpu.roll(surface, EXT - 1, 0) - surface))
        return carry

    chunks = jnp.where(near_y, NEAR, jnp.where(far, FAR, 0))

    @pl.when(worker)
    def _():
        load_wh.wait()
        load_wl.wait()
        first = (jnp.where(north, 0, 2) + core) * ROWS + lon * TILE
        sub = lax.broadcasted_iota(jnp.int32, (TILE, WIDE), 0)
        wave = LON * lax.broadcasted_iota(jnp.int32, (TILE, WIDE), 1)
        limit = jnp.zeros((TILE, WIDE), jnp.int32)
        for i in range(TILE):
            limit = jnp.where(sub == i, cutoff[first + i], limit)
        for s in range(LON):
            m = wave + s
            folded = jnp.minimum(m, NLON - m)
            mask[s] = jnp.where(folded <= limit, 1.0 / NLON, 0.0)
        yh[...] = jnp.zeros_like(yh)
        yl[...] = jnp.zeros_like(yl)

        def chunk(j, _):
            pltpu.make_async_copy(recv.at[j], recv.at[j], fwd_recv.at[j]).wait()
            filter_chunk(j, recv, back, twist, mask, yh, yl, wh, wl, prod)

            @pl.when(near_y)
            def _():
                def reply(d, _):
                    pltpu.make_async_remote_copy(
                        src_ref=back.at[j, d],
                        dst_ref=rows_of(filt, j, lon),
                        send_sem=ret_send.at[j],
                        recv_sem=ret_recv,
                        device_id={"lon": d, "lat": home},
                        device_id_type=MESH,
                    ).start()
                    return 0

                lax.fori_loop(0, LON, reply, 0)

            @pl.when(far)
            def _():
                def reply(d, _):
                    pltpu.make_async_remote_copy(
                        src_ref=back.at[j, d],
                        dst_ref=relay.at[j, lon],
                        send_sem=ret_send.at[j],
                        recv_sem=relay_recv.at[j, lon],
                        device_id={"lon": d, "lat": relay_lat},
                        device_id_type=MESH,
                    ).start()
                    return 0

                lax.fori_loop(0, LON, reply, 0)

            lax.fori_loop(0, jnp.where(j < SUB // PER_CHUNK, PER_CHUNK, 0), subcycle, 0)
            return 0

        lax.fori_loop(0, chunks, chunk, 0)

    left_over = SUB - PER_CHUNK * jnp.minimum(chunks, SUB // PER_CHUNK)
    lax.fori_loop(0, left_over, subcycle, 0)

    inner = slice(HALO, HALO + ROWS)
    for c in range(3):
        moved = pltpu.roll(ext[c, inner, :], WIDE - HALO, 1)
        state_out[c] = moved[:, :COLS]
    for c in range(2):
        moved = pltpu.roll(opens[c, inner, :], WIDE - HALO, 1)
        open_out[c] = moved[:, :COLS]

    @pl.when(relays)
    def _():
        def pass_chunk(j, _):
            def pass_on(t, _):
                here = relay.at[j, t]
                pltpu.make_async_copy(here, here, relay_recv.at[j, t]).wait()
                pltpu.make_async_remote_copy(
                    src_ref=here,
                    dst_ref=rows_of(filt, NEAR + j, t),
                    send_sem=relay_send,
                    recv_sem=ret_recv,
                    device_id={"lon": lon, "lat": home},
                    device_id_type=MESH,
                ).start()
                return 0

            lax.fori_loop(0, LON, pass_on, 0)
            return 0

        lax.fori_loop(0, FAR, pass_chunk, 0)
        pltpu.make_async_copy(relay, relay, relay_send).wait()

    @pl.when(worker)
    def _():
        def sent(j, _):
            pltpu.make_async_copy(back.at[j], back.at[j], ret_send.at[j]).wait()
            return 0

        lax.fori_loop(0, chunks, sent, 0)

    @pl.when(polar)
    def _():
        pltpu.make_async_copy(fields, fields, fwd_send).wait()
        pltpu.make_async_copy(filt, filt, ret_recv).wait()

    @pl.when(jnp.logical_not(polar))
    def _():
        keep_own.wait()


def final_kernel(thick, held, state, opens, tracers, velocity, sea):
    total = thick[0]
    for k in range(1, LEV):
        total = total + thick[k]
    here = pl.ds(pl.multiple_of(pl.program_id(0) * TILE, TILE), TILE)
    sea[...] = state[0, here, :]
    for c in range(2):
        tracers[c] = held[0, c, :, here, :]
        column = None
        for k in range(LEV):
            term = (thick[k] / total) * held[1, c, k, here, :]
            column = term if column is None else column + term
        shift = state[1 + c, here, :] - column
        gate = opens[c, here, :]
        for k in range(LEV):
            velocity[c, k] = gate * (held[1, c, k, here, :] + shift)


def body(fields, thickness, cutoff, barotropic, land_sea):
    f32 = jnp.float32
    high, low, twist = tables()
    sds = jax.ShapeDtypeStruct
    split = fields.reshape(2, 2, LEV, ROWS, COLS)
    held, state, opens = pl.pallas_call(
        wave_kernel,
        out_shape=(
            VMEM((2, 2, LEV, ROWS, COLS), f32),
            VMEM((3, ROWS, COLS), f32),
            VMEM((2, ROWS, COLS), f32),
        ),
        in_specs=[
            pl.BlockSpec(memory_space=pltpu.HBM),
            pl.BlockSpec(memory_space=pltpu.HBM),
            pl.BlockSpec(memory_space=pltpu.HBM),
            pl.BlockSpec(memory_space=pltpu.SMEM),
            pl.BlockSpec(memory_space=pltpu.HBM),
            pl.BlockSpec(memory_space=pltpu.HBM),
            pl.BlockSpec(memory_space=VMEM),
        ],
        out_specs=[
            pl.BlockSpec(memory_space=VMEM),
            pl.BlockSpec(memory_space=VMEM),
            pl.BlockSpec(memory_space=VMEM),
        ],
        scratch_shapes=[
            VMEM((NEAR, LON, 2, TILE, COLS), f32),
            VMEM((NEAR, LON, 2, TILE, COLS), f32),
            VMEM((FAR, LON, 2, TILE, COLS), f32),
            VMEM((WIDE, 2 * WIDE), jnp.bfloat16),
            VMEM((WIDE, 2 * WIDE), jnp.bfloat16),
            VMEM((128, WIDE), jnp.bfloat16),
            VMEM((128, WIDE), jnp.bfloat16),
            VMEM((128, 2 * WIDE), f32),
            VMEM((LON, TILE, WIDE), f32),
            VMEM((3, ROWS, COLS), f32),
            VMEM((ROWS, COLS), jnp.int32),
            VMEM((4, ROWS, WIDE), f32),
            VMEM((ROWS, 128), f32),
            VMEM((ROWS, 128), f32),
            VMEM((4, EXT, WIDE), f32),
            VMEM((EXT, 128), f32),
            VMEM((EXT, 128), f32),
            VMEM((4, EXT, WIDE), f32),
            VMEM((2, EXT, WIDE), f32),
            pltpu.SemaphoreType.DMA,
            pltpu.SemaphoreType.DMA((NEAR,)),
            pltpu.SemaphoreType.DMA((NEAR,)),
            pltpu.SemaphoreType.DMA,
            pltpu.SemaphoreType.DMA((FAR, LON)),
            pltpu.SemaphoreType.DMA,
            pltpu.SemaphoreType.DMA((8,)),
            pltpu.SemaphoreType.DMA((8,)),
            pltpu.SemaphoreType.DMA((5,)),
        ],
        compiler_params=pltpu.CompilerParams(
            collective_id=0, has_side_effects=True, vmem_limit_bytes=58 * 1024 * 1024
        ),
        name="wave",
    )(split, barotropic, land_sea, cutoff, jnp.asarray(high), jnp.asarray(low), jnp.asarray(twist))

    return tuple(
        pl.pallas_call(
            final_kernel,
            out_shape=(
                sds((2, LEV, ROWS, COLS), f32),
                sds((2, LEV, ROWS, COLS), f32),
                sds((ROWS, COLS), f32),
            ),
            grid=(ROWS // TILE,),
            in_specs=[
                pl.BlockSpec(memory_space=pltpu.SMEM),
                pl.BlockSpec(memory_space=VMEM),
                pl.BlockSpec(memory_space=VMEM),
                pl.BlockSpec(memory_space=VMEM),
            ],
            out_specs=[
                pl.BlockSpec((2, LEV, TILE, COLS), lambda i: (0, 0, i, 0)),
                pl.BlockSpec((2, LEV, TILE, COLS), lambda i: (0, 0, i, 0)),
                pl.BlockSpec((TILE, COLS), lambda i: (i, 0)),
            ],
            compiler_params=pltpu.CompilerParams(vmem_limit_bytes=16 * 1024 * 1024),
            name="final",
        )(thickness, held, state, opens)
    )


def solution(mesh):
    return jax.shard_map(
        body,
        mesh=mesh,
        in_specs=(P(None, None, "lat", "lon"), P(), P(), P(None, "lat", "lon"), P("lat", "lon")),
        out_specs=(P(None, None, "lat", "lon"), P(None, None, "lat", "lon"), P("lat", "lon")),
        check_vma=False,
    )
```

```python
import math

import jax
import jax.numpy as jnp
import ml_dtypes
import numpy as np
from jax import lax
from jax.experimental import pallas as pl
from jax.experimental.pallas import tpu as pltpu
from jax.sharding import PartitionSpec as P

MESH = pl.DeviceIdType.MESH
ANY = pl.ANY
VMEM = pltpu.VMEM

WAVE = 0.65
SUB = 20
POLE_DEV = 2
LON, LAT = 8, 16
ROWS, COLS = 64, 450
NLON = LON * COLS
NLAT = LAT * ROWS
LEV = 8
NF = 4
WIDE = 512
HALO = 24
EXT = ROWS + 2 * HALO
TILE = 8
CHUNKS = 16
NEAR = 11
FAR = CHUNKS - NEAR
PER_CHUNK = 2
MAIN = 384
PACK = 2 * MAIN + 128
TAIL = COLS - MAIN
LANE_TILES = ((0, 128), (128, 256), (256, 384), (384, WIDE))


def tables():
    r = np.arange(COLS)
    angle = 2.0 * np.pi * ((r[:, None] * r[None, :]) % COLS) / COLS
    full = np.zeros((WIDE, 2 * WIDE), np.float64)
    full[:COLS, :COLS] = np.cos(angle)
    full[:COLS, WIDE : WIDE + COLS] = np.sin(angle)
    full = full.astype(np.float32)
    high = full.astype(ml_dtypes.bfloat16)
    low = (full - high.astype(np.float32)).astype(ml_dtypes.bfloat16)
    turn = 2.0 * np.pi * (np.arange(LON)[:, None] * r[None, :]) / NLON
    twist = np.zeros((2, LON, WIDE), np.float32)
    twist[0, :, :COLS] = np.cos(turn)
    twist[1, :, :COLS] = np.sin(turn)
    return high, low, twist


def butterflies(z, sign):
    n = len(z)
    if n == 1:
        return z
    even = butterflies(z[0::2], sign)
    odd = butterflies(z[1::2], sign)
    low, high = [], []
    for k in range(n // 2):
        er, ei = even[k]
        tr, ti = odd[k]
        if 4 * k == n:
            tr, ti = (-ti, tr) if sign > 0 else (ti, -tr)
        elif k:
            c = math.cos(2.0 * math.pi * k / n)
            s = sign * math.sin(2.0 * math.pi * k / n)
            tr, ti = c * tr - s * ti, c * ti + s * tr
        low.append((er + tr, ei + ti))
        high.append((er - tr, ei - ti))
    return low + high


def put_split(high_ref, low_ref, s, lanes, re, im):
    value = jnp.concatenate([re, im], axis=0)
    top = value.astype(jnp.bfloat16)
    rows = slice(s * 16, s * 16 + 16)
    high_ref[rows, lanes[0] : lanes[1]] = top
    low_ref[rows, lanes[0] : lanes[1]] = (value - top.astype(jnp.float32)).astype(jnp.bfloat16)


def multiply(high_ref, low_ref, wh_ref, wl_ref, out_ref):
    for block in range(4):
        cols = slice(block * 256, (block + 1) * 256)
        out_ref[:, cols] = (
            jnp.dot(high_ref[...], wh_ref[:, cols], preferred_element_type=jnp.float32)
            + jnp.dot(low_ref[...], wh_ref[:, cols], preferred_element_type=jnp.float32)
            + jnp.dot(high_ref[...], wl_ref[:, cols], preferred_element_type=jnp.float32)
        )


def lanes_of(rows):
    return lax.broadcasted_iota(jnp.int32, (rows, 128), 1)


def pack_tail(first, second):
    return jnp.where(lanes_of(first.shape[0]) < 64, first, pltpu.roll(second, 64, 1))


def pack_rest(q, first, second, rest):
    slot = lanes_of(first.shape[0]) // 2
    rest = jnp.where(slot == 2 * q, pltpu.roll(first, lax.rem(4 * q + 64, 128), 1), rest)
    return jnp.where(slot == 2 * q + 1, pltpu.roll(second, lax.rem(4 * q + 66, 128), 1), rest)


def unpack_tail(q, tail, rest):
    lane = lanes_of(tail.shape[0])
    first = jnp.where(lane < 64, tail, pltpu.roll(rest, (192 - 4 * q) % 128, 1))
    second = jnp.where(lane < 64, pltpu.roll(tail, 64, 1), pltpu.roll(rest, (190 - 4 * q) % 128, 1))
    return jnp.where(lane < TAIL, first, 0.0), jnp.where(lane < TAIL, second, 0.0)


def filter_chunk(j, q, recv, back, twist, mask, yh, yl, wh, wl, prod):
    got, recv_rest = recv
    back, back_rest = back
    for lo, hi in LANE_TILES:
        if lo < MAIN:
            z = [(got[j, d, :, lo:hi], got[j, d, :, MAIN + lo : MAIN + hi]) for d in range(LON)]
        else:
            part = jnp.minimum(q, 1)
            z = [unpack_tail(q, got[j, d, :, 2 * MAIN : PACK], recv_rest[part, d]) for d in range(LON)]
        y = butterflies(z, -1)
        for s in range(LON):
            re, im = y[s]
            if s:
                c = twist[0, s : s + 1, lo:hi]
                n = twist[1, s : s + 1, lo:hi]
                re, im = re * c + im * n, im * c - re * n
            put_split(yh, yl, s, (lo, hi), re, im)
    multiply(yh, yl, wh, wl, prod)
    for lo, hi in LANE_TILES:
        for s in range(LON):
            a = slice(s * 16, s * 16 + 8)
            b = slice(s * 16 + 8, s * 16 + 16)
            keep = mask[s, :, lo:hi]
            re = (prod[a, lo:hi] + prod[b, WIDE + lo : WIDE + hi]) * keep
            im = (prod[b, lo:hi] - prod[a, WIDE + lo : WIDE + hi]) * keep
            put_split(yh, yl, s, (lo, hi), re, im)
    multiply(yh, yl, wh, wl, prod)
    for lo, hi in LANE_TILES:
        z = []
        for s in range(LON):
            a = slice(s * 16, s * 16 + 8)
            b = slice(s * 16 + 8, s * 16 + 16)
            re = prod[a, lo:hi] - prod[b, WIDE + lo : WIDE + hi]
            im = prod[b, lo:hi] + prod[a, WIDE + lo : WIDE + hi]
            if s:
                c = twist[0, s : s + 1, lo:hi]
                n = twist[1, s : s + 1, lo:hi]
                re, im = re * c - im * n, im * c + re * n
            z.append((re, im))
        x = butterflies(z, 1)
        for d in range(LON):
            if lo < MAIN:
                back[j, d, :, lo:hi] = x[d][0]
                back[j, d, :, MAIN + lo : MAIN + hi] = x[d][1]
            else:
                back[j, d, :, 2 * MAIN : PACK] = pack_tail(*x[d])
                back_rest[d] = pack_rest(q, *x[d], back_rest[d])


def wave_kernel(
    fields, baro, land, cutoff, wh_hbm, wl_hbm, twist,
    held, ret, rest_in, state_out, open_out,
    recv, recv_rest, back, back_rest, relay, relay_rest, stage, packed, rest_out, wh, wl, yh, yl, prod, mask,
    own, own_land, src4, edge_r, edge_l, st_c, st_l, st_r, ext, opens,
    fwd_send, fwd_recv, fwd_rest, ret_send, ret_rest, ret_recv,
    relay_recv, relay_rests, relay_send, halo_send, halo_recv, local_sem, load_sem,
):
    lon = lax.axis_index("lon")
    lat = lax.axis_index("lat")
    pair = lat // 2
    core = lax.rem(lat, 2)
    north = lax.rem(pair, 4) < 2
    polar = (pair == 0) | (pair == 7)
    near_y = (pair == 3) | (pair == 4)
    relays = (pair == 1) | (pair == 6)
    far = (pair == 2) | (pair == 5)
    worker = near_y | far
    home = jnp.where(north, 0, LAT - 2) + core
    y_lat = jnp.where(north, 8, 6) + core
    relay_lat = jnp.where(north, 2, 12) + core
    far_lat = jnp.where(north, 10, 4) + core

    load_state = pltpu.make_async_copy(baro, own, local_sem.at[0])
    load_land = pltpu.make_async_copy(land, own_land, local_sem.at[1])
    load_state.start()
    load_land.start()
    load_wh = pltpu.make_async_copy(wh_hbm, wh, local_sem.at[2])
    load_wl = pltpu.make_async_copy(wl_hbm, wl, local_sem.at[3])

    keep_own = pltpu.make_async_copy(fields, held, local_sem.at[4])

    @pl.when(worker)
    def _():
        load_wh.start()
        load_wl.start()

    def load_chunk(q):
        at = (q // LEV, lax.rem(q, LEV))
        return pltpu.make_async_copy(
            fields.at[:, at[0], at[1]], held.at[:, at[0], at[1]], load_sem.at[q]
        )

    @pl.when(polar)
    def _():
        def start(q, _):
            load_chunk(q).start()
            return 0

        lax.fori_loop(0, CHUNKS, start, 0)

    @pl.when(jnp.logical_not(polar))
    def _():
        keep_own.start()

    sides = [(dx, dy) for dy in (0, 1, -1) for dx in (-1, 0, 1) if (dx, dy) != (0, 0)]

    def near(dx, dy):
        return {"lon": lax.rem(lon + dx + LON, LON), "lat": lax.rem(lat + dy + LAT, LAT)}

    def inside(dy):
        return lat < LAT - 1 if dy > 0 else lat > 0

    def when_inside(dy, action):
        if dy == 0:
            action()
        else:
            pl.when(inside(dy))(action)

    barrier = pltpu.get_barrier_semaphore()

    def greet_at(lon_index, lat_index):
        pl.semaphore_signal(
            barrier, inc=1, device_id={"lon": lon_index, "lat": lat_index}, device_id_type=MESH
        )

    def greet_row(lat_index):
        def one(t, _):
            greet_at(t, lat_index)
            return 0

        lax.fori_loop(0, LON, one, 0)

    for dx, dy in sides:
        when_inside(dy, lambda dx=dx, dy=dy: greet_at(near(dx, dy)["lon"], near(dx, dy)["lat"]))

    @pl.when(polar)
    def _():
        greet_row(y_lat)
        greet_row(far_lat)
        greet_at(lon, relay_lat)

    @pl.when(near_y)
    def _():
        greet_row(home)

    @pl.when(far)
    def _():
        greet_row(home)
        greet_row(relay_lat)

    @pl.when(relays)
    def _():
        greet_row(far_lat)
        greet_at(lon, home)

    load_state.wait()
    load_land.wait()
    for c in range(3):
        src4[c, :, 0:384] = own[c, :, 0:384]
        src4[c, :, 384:COLS] = own[c, :, 384:COLS]
    src4[3, :, 0:384] = own_land[:, 0:384].astype(jnp.float32)
    src4[3, :, 384:COLS] = own_land[:, 384:COLS].astype(jnp.float32)
    src4[:, :, COLS:WIDE] = jnp.zeros((4, ROWS, WIDE - COLS), jnp.float32)
    st_c[:, HALO : HALO + ROWS, :] = src4[...]
    lane = lax.broadcasted_iota(jnp.int32, (ROWS, 128), 1)
    right_pack = jnp.zeros((ROWS, 128), jnp.float32)
    left_pack = right_pack
    for c in range(4):
        here = (lane >= c * HALO) & (lane < (c + 1) * HALO)
        right_edge = pltpu.roll(src4[c, :, 384:512], (c * HALO - (COLS - HALO - 384)) % 128, 1)
        left_edge = src4[c, :, 0:128]
        if c:
            left_edge = pltpu.roll(left_edge, c * HALO, 1)
        right_pack = jnp.where(here, right_edge, right_pack)
        left_pack = jnp.where(here, left_edge, left_pack)
    edge_r[...] = right_pack
    edge_l[...] = left_pack

    full = len(sides) - jnp.where((lat == 0) | (lat == LAT - 1), 3, 0)
    extra = jnp.where(polar, 2 * LON + 1, jnp.where(near_y, LON, jnp.where(far, 2 * LON, LON + 1)))
    pl.semaphore_wait(barrier, full + extra)

    def rows(t):
        return pl.ds(pl.multiple_of(t * TILE, TILE), TILE)

    def push(src, dst, send_sem, recv_sem, lon_index, lat_index):
        pltpu.make_async_remote_copy(
            src_ref=src, dst_ref=dst, send_sem=send_sem, recv_sem=recv_sem,
            device_id={"lon": lon_index, "lat": lat_index}, device_id_type=MESH,
        ).start()

    def arrived(ref, sem):
        pltpu.make_async_copy(ref, ref, sem).wait()

    def each_lon(action):
        def one(t, _):
            action(t)
            return 0

        lax.fori_loop(0, LON, one, 0)

    def pack_chunk(q, rest):
        load_chunk(q).wait()
        for i in range(2):
            packed[q, :, :, i * MAIN : (i + 1) * MAIN] = held[
                i, q // LEV, lax.rem(q, LEV), :, 0:MAIN
            ].reshape(LON, TILE, MAIN)
            stage[i, :, 0:TAIL] = held[i, q // LEV, lax.rem(q, LEV), :, MAIN:COLS]
        packed[q, :, :, 2 * MAIN : PACK] = pack_tail(stage[0], stage[1]).reshape(LON, TILE, 128)
        return pack_rest(q, stage[0], stage[1], rest)

    def send_chunk(q, slot, lat_index):
        each_lon(lambda t: push(
            packed.at[q, t], recv.at[slot, lon], fwd_send.at[0], fwd_recv.at[slot], t, lat_index
        ))

    def send_rest(part, lat_index, sem):
        each_lon(lambda t: push(
            rest_out.at[part, rows(t), :], recv_rest.at[part, lon], fwd_send.at[sem], fwd_rest.at[part, lon],
            t, lat_index,
        ))

    @pl.when(polar)
    def _():
        rest_out[0] = pack_chunk(0, jnp.zeros((ROWS, 128), jnp.float32))
        send_rest(0, y_lat, 1)
        send_chunk(0, 0, y_lat)

    row_src = {1: slice(ROWS - HALO, ROWS), 0: slice(0, ROWS), -1: slice(0, HALO)}
    row_dst = {1: slice(0, HALO), 0: slice(HALO, HALO + ROWS), -1: slice(HALO + ROWS, EXT)}
    copies = []
    for n, (dx, dy) in enumerate(sides):
        if dx == 0:
            src = src4.at[:, row_src[dy], :]
            dst = st_c.at[:, row_dst[dy], :]
        else:
            src = (edge_r if dx == 1 else edge_l).at[row_src[dy], :]
            dst = (st_l if dx == 1 else st_r).at[row_dst[dy], :]
        copy = pltpu.make_async_remote_copy(
            src_ref=src, dst_ref=dst, send_sem=halo_send.at[n], recv_sem=halo_recv.at[n],
            device_id=near(dx, dy), device_id_type=MESH,
        )
        when_inside(dy, copy.start)
        copies.append((dy, copy))

    @pl.when(polar)
    def _():
        rest_out[1] = lax.fori_loop(1, CHUNKS, pack_chunk, jnp.zeros((ROWS, 128), jnp.float32))
        send_rest(1, y_lat, 2)
        send_rest(1, far_lat, 3)

        def step(k, _):
            send_chunk(NEAR + k, k, far_lat)
            send_chunk(2 * k + 1, 2 * k + 1, y_lat)
            send_chunk(2 * k + 2, 2 * k + 2, y_lat)
            return 0

        lax.fori_loop(0, FAR, step, 0)

    @pl.when(jnp.logical_not(polar))
    def _():
        keep_own.wait()

    for dy, copy in copies:
        when_inside(dy, copy.wait_send)
        when_inside(-dy, copy.wait_recv)
    for dy in (1, -1):
        @pl.when(jnp.logical_not(inside(-dy)))
        def _(dy=dy):
            st_c[:, row_dst[dy], :] = jnp.zeros((4, HALO, WIDE), jnp.float32)
            st_l[row_dst[dy], :] = jnp.zeros((HALO, 128), jnp.float32)
            st_r[row_dst[dy], :] = jnp.zeros((HALO, 128), jnp.float32)

    lane_ext = lax.broadcasted_iota(jnp.int32, (EXT, 128), 1)
    edge = HALO + COLS - 384
    for c in range(4):
        mid = pltpu.roll(st_c[c], HALO, 1)
        ext[c, :, 128:384] = mid[:, 128:384]
        left = pltpu.roll(st_l[...], 128 - c * HALO, 1) if c else st_l[...]
        ext[c, :, 0:128] = jnp.where(lane_ext < HALO, left, mid[:, 0:128])
        right = pltpu.roll(st_r[...], (edge - c * HALO) % 128, 1)
        right = jnp.where(lane_ext < edge + HALO, right, 0.0)
        ext[c, :, 384:512] = jnp.where(lane_ext >= edge, right, mid[:, 384:512])

    ocean = ext[3]
    row_id = lat * ROWS - HALO + lax.broadcasted_iota(jnp.int32, (EXT, WIDE), 0)
    east_open = ocean * pltpu.roll(ocean, WIDE - 1, 1)
    north_open = jnp.where(row_id == NLAT - 1, 0.0, ocean * pltpu.roll(ocean, EXT - 1, 0))
    opens[0] = east_open
    opens[1] = north_open
    ext[1] = ext[1] * east_open
    ext[2] = ext[2] * north_open
    ext[3] = WAVE * ocean

    def subcycle(_, carry):
        east = ext[1]
        north = ext[2]
        div = east - pltpu.roll(east, 1, 1) + north - pltpu.roll(north, 1, 0)
        surface = ext[0] - ext[3] * div
        ext[0] = surface
        ext[1] = opens[0] * (east - WAVE * (pltpu.roll(surface, WIDE - 1, 1) - surface))
        ext[2] = opens[1] * (north - WAVE * (pltpu.roll(surface, EXT - 1, 0) - surface))
        return carry

    chunks = jnp.where(near_y, NEAR, jnp.where(far, FAR, 0))

    @pl.when(worker)
    def _():
        load_wh.wait()
        load_wl.wait()
        first = (jnp.where(north, 0, 2) + core) * ROWS + lon * TILE
        sub = lax.broadcasted_iota(jnp.int32, (TILE, WIDE), 0)
        wave = LON * lax.broadcasted_iota(jnp.int32, (TILE, WIDE), 1)
        limit = jnp.zeros((TILE, WIDE), jnp.int32)
        for i in range(TILE):
            limit = jnp.where(sub == i, cutoff[first + i], limit)
        for s in range(LON):
            m = wave + s
            folded = jnp.minimum(m, NLON - m)
            mask[s] = jnp.where(folded <= limit, 1.0 / NLON, 0.0)
        back_rest[...] = jnp.zeros_like(back_rest)
        q_first = jnp.where(near_y, 0, NEAR)

        @pl.when(near_y)
        def _():
            each_lon(lambda d: arrived(recv_rest.at[0, d], fwd_rest.at[0, d]))

        def chunk(j, _):
            arrived(recv.at[j], fwd_recv.at[j])

            @pl.when(j == jnp.where(near_y, 1, 0))
            def _():
                each_lon(lambda d: arrived(recv_rest.at[1, d], fwd_rest.at[1, d]))

            filter_chunk(
                j, q_first + j, (recv, recv_rest), (back, back_rest), twist, mask, yh, yl, wh, wl, prod
            )

            @pl.when(near_y)
            def _():
                each_lon(lambda d: push(back.at[j, d], ret.at[j, lon], ret_send.at[j], ret_recv.at[0], d, home))

            @pl.when(far)
            def _():
                each_lon(lambda d: push(
                    back.at[j, d], relay.at[j, lon], ret_send.at[j], relay_recv.at[j, lon], d, relay_lat
                ))

            lax.fori_loop(0, jnp.where(j < SUB // PER_CHUNK, PER_CHUNK, 0), subcycle, 0)
            return 0

        lax.fori_loop(0, chunks, chunk, 0)

        @pl.when(near_y)
        def _():
            each_lon(lambda d: push(
                back_rest.at[d], rest_in.at[0, lon], ret_rest, ret_recv.at[1], d, home
            ))

        @pl.when(far)
        def _():
            each_lon(lambda d: push(
                back_rest.at[d], relay_rest.at[lon], ret_rest, relay_rests.at[lon], d, relay_lat
            ))

    left_over = SUB - PER_CHUNK * jnp.minimum(chunks, SUB // PER_CHUNK)
    lax.fori_loop(0, left_over, subcycle, 0)

    inner = slice(HALO, HALO + ROWS)
    for c in range(3):
        moved = pltpu.roll(ext[c, inner, :], WIDE - HALO, 1)
        state_out[c] = moved[:, :COLS]
    for c in range(2):
        moved = pltpu.roll(opens[c, inner, :], WIDE - HALO, 1)
        open_out[c] = moved[:, :COLS]

    @pl.when(relays)
    def _():
        def pass_chunk(j, _):
            def pass_on(t):
                arrived(relay.at[j, t], relay_recv.at[j, t])
                push(relay.at[j, t], ret.at[NEAR + j, t], relay_send.at[0], ret_recv.at[0], lon, home)

            each_lon(pass_on)
            return 0

        lax.fori_loop(0, FAR, pass_chunk, 0)

        def pass_rest(t):
            arrived(relay_rest.at[t], relay_rests.at[t])
            push(relay_rest.at[t], rest_in.at[1, t], relay_send.at[1], ret_recv.at[2], lon, home)

        each_lon(pass_rest)
        arrived(relay, relay_send.at[0])
        arrived(relay_rest, relay_send.at[1])

    @pl.when(worker)
    def _():
        def sent(j, _):
            arrived(back.at[j], ret_send.at[j])
            return 0

        lax.fori_loop(0, chunks, sent, 0)
        arrived(back_rest, ret_rest)

    @pl.when(polar)
    def _():
        arrived(packed, fwd_send.at[0])
        arrived(rest_out.at[0], fwd_send.at[1])
        arrived(rest_out.at[1], fwd_send.at[2])
        arrived(rest_out.at[1], fwd_send.at[3])
        arrived(ret, ret_recv.at[0])
        arrived(rest_in.at[0], ret_recv.at[1])
        arrived(rest_in.at[1], ret_recv.at[2])


def final_kernel(polar, thick, held, ret, rest_in, state, opens, tracers, velocity, sea):
    total = thick[0]
    for k in range(1, LEV):
        total = total + thick[k]
    tile = pl.program_id(0)
    here = pl.ds(pl.multiple_of(tile * TILE, TILE), TILE)
    sea[...] = state[0, here, :]

    def finish(lo, hi, load):
        pairs = [[load(c, k) for k in range(LEV)] for c in range(2)]
        for c in range(2):
            column = None
            for k in range(LEV):
                tracers[c, k, :, lo:hi] = pairs[c][k][0]
                term = (thick[k] / total) * pairs[c][k][1]
                column = term if column is None else column + term
            shift = state[1 + c, here, lo:hi] - column
            gate = opens[c, here, lo:hi]
            for k in range(LEV):
                velocity[c, k, :, lo:hi] = gate * (pairs[c][k][1] + shift)

    @pl.when(polar[0] == 1)
    def _():
        for lo in range(0, MAIN, 128):
            finish(lo, lo + 128, lambda c, k: (
                ret[c * LEV + k, tile, :, lo : lo + 128],
                ret[c * LEV + k, tile, :, MAIN + lo : MAIN + lo + 128],
            ))

        def tail(c, k):
            q = c * LEV + k
            first, second = unpack_tail(q, ret[q, tile, :, 2 * MAIN : PACK], rest_in[int(q >= NEAR), tile])
            return first[:, :TAIL], second[:, :TAIL]

        finish(MAIN, COLS, tail)

    @pl.when(polar[0] == 0)
    def _():
        for lo, hi in ((0, 128), (128, 256), (256, MAIN), (MAIN, COLS)):
            finish(lo, hi, lambda c, k: (held[0, c, k, here, lo:hi], held[1, c, k, here, lo:hi]))


def body(fields, thickness, cutoff, barotropic, land_sea):
    f32 = jnp.float32
    high, low, twist = tables()
    sds = jax.ShapeDtypeStruct
    split = fields.reshape(2, 2, LEV, ROWS, COLS)
    held, ret, rest, state, opens = pl.pallas_call(
        wave_kernel,
        out_shape=(
            VMEM((2, 2, LEV, ROWS, COLS), f32),
            VMEM((CHUNKS, LON, TILE, PACK), f32),
            VMEM((2, LON, TILE, 128), f32),
            VMEM((3, ROWS, COLS), f32),
            VMEM((2, ROWS, COLS), f32),
        ),
        in_specs=[
            pl.BlockSpec(memory_space=pltpu.HBM),
            pl.BlockSpec(memory_space=pltpu.HBM),
            pl.BlockSpec(memory_space=pltpu.HBM),
            pl.BlockSpec(memory_space=pltpu.SMEM),
            pl.BlockSpec(memory_space=pltpu.HBM),
            pl.BlockSpec(memory_space=pltpu.HBM),
            pl.BlockSpec(memory_space=VMEM),
        ],
        out_specs=[pl.BlockSpec(memory_space=VMEM)] * 5,
        scratch_shapes=[
            VMEM((NEAR, LON, TILE, PACK), f32),
            VMEM((2, LON, TILE, 128), f32),
            VMEM((NEAR, LON, TILE, PACK), f32),
            VMEM((LON, TILE, 128), f32),
            VMEM((FAR, LON, TILE, PACK), f32),
            VMEM((LON, TILE, 128), f32),
            VMEM((2, ROWS, 128), f32),
            VMEM((CHUNKS, LON, TILE, PACK), f32),
            VMEM((2, ROWS, 128), f32),
            VMEM((WIDE, 2 * WIDE), jnp.bfloat16),
            VMEM((WIDE, 2 * WIDE), jnp.bfloat16),
            VMEM((128, WIDE), jnp.bfloat16),
            VMEM((128, WIDE), jnp.bfloat16),
            VMEM((128, 2 * WIDE), f32),
            VMEM((LON, TILE, WIDE), f32),
            VMEM((3, ROWS, COLS), f32),
            VMEM((ROWS, COLS), jnp.int32),
            VMEM((4, ROWS, WIDE), f32),
            VMEM((ROWS, 128), f32),
            VMEM((ROWS, 128), f32),
            VMEM((4, EXT, WIDE), f32),
            VMEM((EXT, 128), f32),
            VMEM((EXT, 128), f32),
            VMEM((4, EXT, WIDE), f32),
            VMEM((2, EXT, WIDE), f32),
            pltpu.SemaphoreType.DMA((4,)),
            pltpu.SemaphoreType.DMA((NEAR,)),
            pltpu.SemaphoreType.DMA((2, LON)),
            pltpu.SemaphoreType.DMA((NEAR,)),
            pltpu.SemaphoreType.DMA,
            pltpu.SemaphoreType.DMA((3,)),
            pltpu.SemaphoreType.DMA((FAR, LON)),
            pltpu.SemaphoreType.DMA((LON,)),
            pltpu.SemaphoreType.DMA((2,)),
            pltpu.SemaphoreType.DMA((8,)),
            pltpu.SemaphoreType.DMA((8,)),
            pltpu.SemaphoreType.DMA((5,)),
            pltpu.SemaphoreType.DMA((CHUNKS,)),
        ],
        compiler_params=pltpu.CompilerParams(
            collective_id=0, has_side_effects=True, vmem_limit_bytes=53 * 1024 * 1024
        ),
        name="wave",
    )(split, barotropic, land_sea, cutoff, jnp.asarray(high), jnp.asarray(low), jnp.asarray(twist))

    lat = lax.axis_index("lat")
    polar = ((lat < POLE_DEV) | (lat >= LAT - POLE_DEV)).astype(jnp.int32).reshape(1)
    return tuple(
        pl.pallas_call(
            final_kernel,
            out_shape=(
                sds((2, LEV, ROWS, COLS), f32),
                sds((2, LEV, ROWS, COLS), f32),
                sds((ROWS, COLS), f32),
            ),
            grid=(ROWS // TILE,),
            in_specs=[
                pl.BlockSpec(memory_space=pltpu.SMEM),
                pl.BlockSpec(memory_space=pltpu.SMEM),
                pl.BlockSpec(memory_space=VMEM),
                pl.BlockSpec(memory_space=VMEM),
                pl.BlockSpec(memory_space=VMEM),
                pl.BlockSpec(memory_space=VMEM),
                pl.BlockSpec(memory_space=VMEM),
            ],
            out_specs=[
                pl.BlockSpec((2, LEV, TILE, COLS), lambda i: (0, 0, i, 0)),
                pl.BlockSpec((2, LEV, TILE, COLS), lambda i: (0, 0, i, 0)),
                pl.BlockSpec((TILE, COLS), lambda i: (i, 0)),
            ],
            compiler_params=pltpu.CompilerParams(vmem_limit_bytes=16 * 1024 * 1024),
            name="final",
        )(polar, thickness, held, ret, rest, state, opens)
    )


def solution(mesh):
    return jax.shard_map(
        body,
        mesh=mesh,
        in_specs=(P(None, None, "lat", "lon"), P(), P(), P(None, "lat", "lon"), P("lat", "lon")),
        out_specs=(P(None, None, "lat", "lon"), P(None, None, "lat", "lon"), P("lat", "lon")),
        check_vma=False,
    )
```

```python
import math

import jax
import jax.numpy as jnp
import ml_dtypes
import numpy as np
from jax import lax
from jax.experimental import pallas as pl
from jax.experimental.pallas import tpu as pltpu
from jax.sharding import PartitionSpec as P

MESH = pl.DeviceIdType.MESH
ANY = pl.ANY
VMEM = pltpu.VMEM

WAVE = 0.65
SUB = 20
POLE_DEV = 2
LON, LAT = 8, 16
ROWS, COLS = 64, 450
NLON = LON * COLS
NLAT = LAT * ROWS
LEV = 8
NF = 4
WIDE = 512
HALO = 24
EXT = ROWS + 2 * HALO
TILE = 8
CHUNKS = 16
NEAR = 11
FAR = CHUNKS - NEAR
PER_CHUNK = 2
FIRST = 2
MAIN = 384
PACK = 2 * MAIN + 128
TAIL = COLS - MAIN
LANE_TILES = ((0, 128), (128, 256), (256, 384), (384, WIDE))


def tables():
    r = np.arange(COLS)
    angle = 2.0 * np.pi * ((r[:, None] * r[None, :]) % COLS) / COLS
    full = np.zeros((WIDE, 2 * WIDE), np.float64)
    full[:COLS, :COLS] = np.cos(angle)
    full[:COLS, WIDE : WIDE + COLS] = np.sin(angle)
    full = full.astype(np.float32)
    high = full.astype(ml_dtypes.bfloat16)
    low = (full - high.astype(np.float32)).astype(ml_dtypes.bfloat16)
    turn = 2.0 * np.pi * (np.arange(LON)[:, None] * r[None, :]) / NLON
    twist = np.zeros((2, LON, WIDE), np.float32)
    twist[0, :, :COLS] = np.cos(turn)
    twist[1, :, :COLS] = np.sin(turn)
    return high, low, twist


def butterflies(z, sign):
    n = len(z)
    if n == 1:
        return z
    even = butterflies(z[0::2], sign)
    odd = butterflies(z[1::2], sign)
    low, high = [], []
    for k in range(n // 2):
        er, ei = even[k]
        tr, ti = odd[k]
        if 4 * k == n:
            tr, ti = (-ti, tr) if sign > 0 else (ti, -tr)
        elif k:
            c = math.cos(2.0 * math.pi * k / n)
            s = sign * math.sin(2.0 * math.pi * k / n)
            tr, ti = c * tr - s * ti, c * ti + s * tr
        low.append((er + tr, ei + ti))
        high.append((er - tr, ei - ti))
    return low + high


def put_split(high_ref, low_ref, s, lanes, re, im):
    value = jnp.concatenate([re, im], axis=0)
    top = value.astype(jnp.bfloat16)
    rows = slice(s * 16, s * 16 + 16)
    high_ref[rows, lanes[0] : lanes[1]] = top
    low_ref[rows, lanes[0] : lanes[1]] = (value - top.astype(jnp.float32)).astype(jnp.bfloat16)


def multiply(high_ref, low_ref, wh_ref, wl_ref, out_ref):
    for block in range(4):
        cols = slice(block * 256, (block + 1) * 256)
        out_ref[:, cols] = (
            jnp.dot(high_ref[...], wh_ref[:, cols], preferred_element_type=jnp.float32)
            + jnp.dot(low_ref[...], wh_ref[:, cols], preferred_element_type=jnp.float32)
            + jnp.dot(high_ref[...], wl_ref[:, cols], preferred_element_type=jnp.float32)
        )


def lanes_of(rows):
    return lax.broadcasted_iota(jnp.int32, (rows, 128), 1)


def pack_tail(first, second):
    return jnp.where(lanes_of(first.shape[0]) < 64, first, pltpu.roll(second, 64, 1))


def pack_rest(q, first, second, rest):
    slot = lanes_of(first.shape[0]) // 2
    rest = jnp.where(slot == 2 * q, pltpu.roll(first, lax.rem(4 * q + 64, 128), 1), rest)
    return jnp.where(slot == 2 * q + 1, pltpu.roll(second, lax.rem(4 * q + 66, 128), 1), rest)


def unpack_tail(q, tail, rest):
    lane = lanes_of(tail.shape[0])
    first = jnp.where(lane < 64, tail, pltpu.roll(rest, (192 - 4 * q) % 128, 1))
    second = jnp.where(lane < 64, pltpu.roll(tail, 64, 1), pltpu.roll(rest, (190 - 4 * q) % 128, 1))
    return jnp.where(lane < TAIL, first, 0.0), jnp.where(lane < TAIL, second, 0.0)


def filter_chunk(j, q, recv, back, twist, mask, yh, yl, wh, wl, prod):
    got, recv_rest = recv
    back, back_rest = back
    for lo, hi in LANE_TILES:
        if lo < MAIN:
            z = [(got[j, d, :, lo:hi], got[j, d, :, MAIN + lo : MAIN + hi]) for d in range(LON)]
        else:
            part = jnp.minimum(q, 1)
            z = [unpack_tail(q, got[j, d, :, 2 * MAIN : PACK], recv_rest[part, d]) for d in range(LON)]
        y = butterflies(z, -1)
        for s in range(LON):
            re, im = y[s]
            if s:
                c = twist[0, s : s + 1, lo:hi]
                n = twist[1, s : s + 1, lo:hi]
                re, im = re * c + im * n, im * c - re * n
            put_split(yh, yl, s, (lo, hi), re, im)
    multiply(yh, yl, wh, wl, prod)
    for lo, hi in LANE_TILES:
        for s in range(LON):
            a = slice(s * 16, s * 16 + 8)
            b = slice(s * 16 + 8, s * 16 + 16)
            keep = mask[s, :, lo:hi]
            re = (prod[a, lo:hi] + prod[b, WIDE + lo : WIDE + hi]) * keep
            im = (prod[b, lo:hi] - prod[a, WIDE + lo : WIDE + hi]) * keep
            put_split(yh, yl, s, (lo, hi), re, im)
    multiply(yh, yl, wh, wl, prod)
    for lo, hi in LANE_TILES:
        z = []
        for s in range(LON):
            a = slice(s * 16, s * 16 + 8)
            b = slice(s * 16 + 8, s * 16 + 16)
            re = prod[a, lo:hi] - prod[b, WIDE + lo : WIDE + hi]
            im = prod[b, lo:hi] + prod[a, WIDE + lo : WIDE + hi]
            if s:
                c = twist[0, s : s + 1, lo:hi]
                n = twist[1, s : s + 1, lo:hi]
                re, im = re * c - im * n, im * c + re * n
            z.append((re, im))
        x = butterflies(z, 1)
        for d in range(LON):
            if lo < MAIN:
                back[j, d, :, lo:hi] = x[d][0]
                back[j, d, :, MAIN + lo : MAIN + hi] = x[d][1]
            else:
                back[j, d, :, 2 * MAIN : PACK] = pack_tail(*x[d])
                back_rest[d] = pack_rest(q, *x[d], back_rest[d])


def wave_kernel(
    fields, baro, land, cutoff, wh_hbm, wl_hbm, twist,
    held, ret, rest_in, state_out, open_out,
    recv, recv_rest, back, back_rest, relay, relay_rest, stage, packed, rest_out, wh, wl, yh, yl, prod, mask,
    own, own_land, src4, edge_r, edge_l, st_c, st_l, st_r, ext, opens,
    fwd_send, fwd_recv, fwd_rest, ret_send, ret_rest, ret_recv,
    relay_recv, relay_rests, relay_send, halo_send, halo_recv, local_sem, load_sem,
):
    lon = lax.axis_index("lon")
    lat = lax.axis_index("lat")
    pair = lat // 2
    core = lax.rem(lat, 2)
    north = lax.rem(pair, 4) < 2
    polar = (pair == 0) | (pair == 7)
    near_y = (pair == 3) | (pair == 4)
    relays = (pair == 1) | (pair == 6)
    far = (pair == 2) | (pair == 5)
    worker = near_y | far
    home = jnp.where(north, 0, LAT - 2) + core
    y_lat = jnp.where(north, 8, 6) + core
    relay_lat = jnp.where(north, 2, 12) + core
    far_lat = jnp.where(north, 10, 4) + core

    load_state = pltpu.make_async_copy(baro, own, local_sem.at[0])
    load_land = pltpu.make_async_copy(land, own_land, local_sem.at[1])
    load_state.start()
    load_land.start()
    load_wh = pltpu.make_async_copy(wh_hbm, wh, local_sem.at[2])
    load_wl = pltpu.make_async_copy(wl_hbm, wl, local_sem.at[3])

    keep_own = pltpu.make_async_copy(fields, held, local_sem.at[4])

    @pl.when(worker)
    def _():
        load_wh.start()
        load_wl.start()

    def load_chunk(q):
        at = (q // LEV, lax.rem(q, LEV))
        return pltpu.make_async_copy(
            fields.at[:, at[0], at[1]], held.at[:, at[0], at[1]], load_sem.at[q]
        )

    @pl.when(polar)
    def _():
        def start(q, _):
            load_chunk(q).start()
            return 0

        lax.fori_loop(0, CHUNKS, start, 0)

    @pl.when(jnp.logical_not(polar))
    def _():
        keep_own.start()

    sides = [(dx, dy) for dy in (0, 1, -1) for dx in (-1, 0, 1) if (dx, dy) != (0, 0)]

    def near(dx, dy):
        return {"lon": lax.rem(lon + dx + LON, LON), "lat": lax.rem(lat + dy + LAT, LAT)}

    def inside(dy):
        return lat < LAT - 1 if dy > 0 else lat > 0

    def when_inside(dy, action):
        if dy == 0:
            action()
        else:
            pl.when(inside(dy))(action)

    barrier = pltpu.get_barrier_semaphore()

    def greet_at(lon_index, lat_index):
        pl.semaphore_signal(
            barrier, inc=1, device_id={"lon": lon_index, "lat": lat_index}, device_id_type=MESH
        )

    def greet_row(lat_index):
        def one(t, _):
            greet_at(t, lat_index)
            return 0

        lax.fori_loop(0, LON, one, 0)

    for dx, dy in sides:
        when_inside(dy, lambda dx=dx, dy=dy: greet_at(near(dx, dy)["lon"], near(dx, dy)["lat"]))

    @pl.when(polar)
    def _():
        greet_row(y_lat)
        greet_row(far_lat)
        greet_at(lon, relay_lat)

    @pl.when(near_y)
    def _():
        greet_row(home)

    @pl.when(far)
    def _():
        greet_row(home)
        greet_row(relay_lat)

    @pl.when(relays)
    def _():
        greet_row(far_lat)
        greet_at(lon, home)

    load_state.wait()
    load_land.wait()
    for c in range(3):
        src4[c, :, 0:384] = own[c, :, 0:384]
        src4[c, :, 384:COLS] = own[c, :, 384:COLS]
    src4[3, :, 0:384] = own_land[:, 0:384].astype(jnp.float32)
    src4[3, :, 384:COLS] = own_land[:, 384:COLS].astype(jnp.float32)
    src4[:, :, COLS:WIDE] = jnp.zeros((4, ROWS, WIDE - COLS), jnp.float32)
    st_c[:, HALO : HALO + ROWS, :] = src4[...]
    lane = lax.broadcasted_iota(jnp.int32, (ROWS, 128), 1)
    right_pack = jnp.zeros((ROWS, 128), jnp.float32)
    left_pack = right_pack
    for c in range(4):
        here = (lane >= c * HALO) & (lane < (c + 1) * HALO)
        right_edge = pltpu.roll(src4[c, :, 384:512], (c * HALO - (COLS - HALO - 384)) % 128, 1)
        left_edge = src4[c, :, 0:128]
        if c:
            left_edge = pltpu.roll(left_edge, c * HALO, 1)
        right_pack = jnp.where(here, right_edge, right_pack)
        left_pack = jnp.where(here, left_edge, left_pack)
    edge_r[...] = right_pack
    edge_l[...] = left_pack

    full = len(sides) - jnp.where((lat == 0) | (lat == LAT - 1), 3, 0)
    extra = jnp.where(polar, 2 * LON + 1, jnp.where(near_y, LON, jnp.where(far, 2 * LON, LON + 1)))
    pl.semaphore_wait(barrier, full + extra)

    def rows(t):
        return pl.ds(pl.multiple_of(t * TILE, TILE), TILE)

    def push(src, dst, send_sem, recv_sem, lon_index, lat_index):
        pltpu.make_async_remote_copy(
            src_ref=src, dst_ref=dst, send_sem=send_sem, recv_sem=recv_sem,
            device_id={"lon": lon_index, "lat": lat_index}, device_id_type=MESH,
        ).start()

    def arrived(ref, sem):
        pltpu.make_async_copy(ref, ref, sem).wait()

    def each_lon(action):
        def one(t, _):
            action(t)
            return 0

        lax.fori_loop(0, LON, one, 0)

    def pack_chunk(q, rest):
        load_chunk(q).wait()
        for i in range(2):
            packed[q, :, :, i * MAIN : (i + 1) * MAIN] = held[
                i, q // LEV, lax.rem(q, LEV), :, 0:MAIN
            ].reshape(LON, TILE, MAIN)
            stage[i, :, 0:TAIL] = held[i, q // LEV, lax.rem(q, LEV), :, MAIN:COLS]
        packed[q, :, :, 2 * MAIN : PACK] = pack_tail(stage[0], stage[1]).reshape(LON, TILE, 128)
        return pack_rest(q, stage[0], stage[1], rest)

    def send_chunk(q, slot, lat_index):
        each_lon(lambda t: push(
            packed.at[q, t], recv.at[slot, lon], fwd_send.at[0], fwd_recv.at[slot], t, lat_index
        ))

    def send_rest(part, lat_index, sem):
        each_lon(lambda t: push(
            rest_out.at[part, rows(t), :], recv_rest.at[part, lon], fwd_send.at[sem], fwd_rest.at[part, lon],
            t, lat_index,
        ))

    @pl.when(polar)
    def _():
        rest_out[0] = pack_chunk(0, jnp.zeros((ROWS, 128), jnp.float32))
        send_rest(0, y_lat, 1)
        send_chunk(0, 0, y_lat)

    row_src = {1: slice(ROWS - HALO, ROWS), 0: slice(0, ROWS), -1: slice(0, HALO)}
    row_dst = {1: slice(0, HALO), 0: slice(HALO, HALO + ROWS), -1: slice(HALO + ROWS, EXT)}
    copies = []
    for n, (dx, dy) in enumerate(sides):
        if dx == 0:
            src = src4.at[:, row_src[dy], :]
            dst = st_c.at[:, row_dst[dy], :]
        else:
            src = (edge_r if dx == 1 else edge_l).at[row_src[dy], :]
            dst = (st_l if dx == 1 else st_r).at[row_dst[dy], :]
        copy = pltpu.make_async_remote_copy(
            src_ref=src, dst_ref=dst, send_sem=halo_send.at[n], recv_sem=halo_recv.at[n],
            device_id=near(dx, dy), device_id_type=MESH,
        )
        when_inside(dy, copy.start)
        copies.append((dy, copy))

    @pl.when(polar)
    def _():
        rest_out[1] = lax.fori_loop(1, CHUNKS, pack_chunk, jnp.zeros((ROWS, 128), jnp.float32))
        send_rest(1, y_lat, 2)
        send_rest(1, far_lat, 3)

        def step(k, _):
            send_chunk(NEAR + k, k, far_lat)
            send_chunk(2 * k + 1, 2 * k + 1, y_lat)
            send_chunk(2 * k + 2, 2 * k + 2, y_lat)
            return 0

        lax.fori_loop(0, FAR, step, 0)

    @pl.when(jnp.logical_not(polar))
    def _():
        keep_own.wait()

    def assemble():
        for dy, copy in copies:
            when_inside(dy, copy.wait_send)
            when_inside(-dy, copy.wait_recv)
        for dy in (1, -1):
            @pl.when(jnp.logical_not(inside(-dy)))
            def _(dy=dy):
                st_c[:, row_dst[dy], :] = jnp.zeros((4, HALO, WIDE), jnp.float32)
                st_l[row_dst[dy], :] = jnp.zeros((HALO, 128), jnp.float32)
                st_r[row_dst[dy], :] = jnp.zeros((HALO, 128), jnp.float32)

        lane_ext = lax.broadcasted_iota(jnp.int32, (EXT, 128), 1)
        edge = HALO + COLS - 384
        for c in range(4):
            mid = pltpu.roll(st_c[c], HALO, 1)
            ext[c, :, 128:384] = mid[:, 128:384]
            left = pltpu.roll(st_l[...], 128 - c * HALO, 1) if c else st_l[...]
            ext[c, :, 0:128] = jnp.where(lane_ext < HALO, left, mid[:, 0:128])
            right = pltpu.roll(st_r[...], (edge - c * HALO) % 128, 1)
            right = jnp.where(lane_ext < edge + HALO, right, 0.0)
            ext[c, :, 384:512] = jnp.where(lane_ext >= edge, right, mid[:, 384:512])

        ocean = ext[3]
        row_id = lat * ROWS - HALO + lax.broadcasted_iota(jnp.int32, (EXT, WIDE), 0)
        east_open = ocean * pltpu.roll(ocean, WIDE - 1, 1)
        north_open = jnp.where(row_id == NLAT - 1, 0.0, ocean * pltpu.roll(ocean, EXT - 1, 0))
        opens[0] = east_open
        opens[1] = north_open
        ext[1] = ext[1] * east_open
        ext[2] = ext[2] * north_open
        ext[3] = WAVE * ocean

    def subcycle(_, carry):
        east = ext[1]
        north = ext[2]
        div = east - pltpu.roll(east, 1, 1) + north - pltpu.roll(north, 1, 0)
        surface = ext[0] - ext[3] * div
        ext[0] = surface
        ext[1] = opens[0] * (east - WAVE * (pltpu.roll(surface, WIDE - 1, 1) - surface))
        ext[2] = opens[1] * (north - WAVE * (pltpu.roll(surface, EXT - 1, 0) - surface))
        return carry

    chunks = jnp.where(near_y, NEAR, jnp.where(far, FAR, 0))

    @pl.when(jnp.logical_not(worker))
    def _():
        assemble()

    @pl.when(worker)
    def _():
        load_wh.wait()
        load_wl.wait()
        first = (jnp.where(north, 0, 2) + core) * ROWS + lon * TILE
        sub = lax.broadcasted_iota(jnp.int32, (TILE, WIDE), 0)
        wave = LON * lax.broadcasted_iota(jnp.int32, (TILE, WIDE), 1)
        limit = jnp.zeros((TILE, WIDE), jnp.int32)
        for i in range(TILE):
            limit = jnp.where(sub == i, cutoff[first + i], limit)
        for s in range(LON):
            m = wave + s
            folded = jnp.minimum(m, NLON - m)
            mask[s] = jnp.where(folded <= limit, 1.0 / NLON, 0.0)
        back_rest[...] = jnp.zeros_like(back_rest)
        q_first = jnp.where(near_y, 0, NEAR)

        @pl.when(near_y)
        def _():
            each_lon(lambda d: arrived(recv_rest.at[0, d], fwd_rest.at[0, d]))

        def chunk(j, _):
            arrived(recv.at[j], fwd_recv.at[j])

            @pl.when(j == jnp.where(near_y, 1, 0))
            def _():
                each_lon(lambda d: arrived(recv_rest.at[1, d], fwd_rest.at[1, d]))

            filter_chunk(
                j, q_first + j, (recv, recv_rest), (back, back_rest), twist, mask, yh, yl, wh, wl, prod
            )

            @pl.when(near_y)
            def _():
                each_lon(lambda d: push(back.at[j, d], ret.at[j, lon], ret_send.at[j], ret_recv.at[0], d, home))

            @pl.when(far)
            def _():
                each_lon(lambda d: push(
                    back.at[j, d], relay.at[j, lon], ret_send.at[j], relay_recv.at[j, lon], d, relay_lat
                ))

            @pl.when(near_y & (j == NEAR - 1))
            def _():
                each_lon(lambda d: push(
                    back_rest.at[d], rest_in.at[0, lon], ret_rest, ret_recv.at[1], d, home
                ))

            @pl.when(far & (j == FAR - 1))
            def _():
                each_lon(lambda d: push(
                    back_rest.at[d], relay_rest.at[lon], ret_rest, relay_rests.at[lon], d, relay_lat
                ))

            pl.when(j == FIRST - 1)(assemble)
            lax.fori_loop(0, jnp.where(j >= FIRST, PER_CHUNK, 0), subcycle, 0)
            return 0

        lax.fori_loop(0, chunks, chunk, 0)

    left_over = SUB - PER_CHUNK * jnp.maximum(chunks - FIRST, 0)
    lax.fori_loop(0, left_over, subcycle, 0)

    inner = slice(HALO, HALO + ROWS)
    for c in range(3):
        moved = pltpu.roll(ext[c, inner, :], WIDE - HALO, 1)
        state_out[c] = moved[:, :COLS]
    for c in range(2):
        moved = pltpu.roll(opens[c, inner, :], WIDE - HALO, 1)
        open_out[c] = moved[:, :COLS]

    @pl.when(relays)
    def _():
        def pass_chunk(j, _):
            def pass_on(t):
                arrived(relay.at[j, t], relay_recv.at[j, t])
                push(relay.at[j, t], ret.at[NEAR + j, t], relay_send.at[0], ret_recv.at[0], lon, home)

            each_lon(pass_on)
            return 0

        lax.fori_loop(0, FAR, pass_chunk, 0)

        def pass_rest(t):
            arrived(relay_rest.at[t], relay_rests.at[t])
            push(relay_rest.at[t], rest_in.at[1, t], relay_send.at[1], ret_recv.at[2], lon, home)

        each_lon(pass_rest)
        arrived(relay, relay_send.at[0])
        arrived(relay_rest, relay_send.at[1])

    @pl.when(worker)
    def _():
        def sent(j, _):
            arrived(back.at[j], ret_send.at[j])
            return 0

        lax.fori_loop(0, chunks, sent, 0)
        arrived(back_rest, ret_rest)

    @pl.when(polar)
    def _():
        arrived(packed, fwd_send.at[0])
        arrived(rest_out.at[0], fwd_send.at[1])
        arrived(rest_out.at[1], fwd_send.at[2])
        arrived(rest_out.at[1], fwd_send.at[3])
        arrived(ret, ret_recv.at[0])
        arrived(rest_in.at[0], ret_recv.at[1])
        arrived(rest_in.at[1], ret_recv.at[2])


def final_kernel(
    thick, held, ret, rest_in, state, opens, tracers_out, velocity_out, sea_out, tracers, velocity, sems
):
    lat = lax.axis_index("lat")
    polar = (lat < POLE_DEV) | (lat >= LAT - POLE_DEV)
    total = thick[0]
    for k in range(1, LEV):
        total = total + thick[k]
    save_sea = pltpu.make_async_copy(state.at[0], sea_out, sems.at[2])
    save_sea.start()

    def finish(tile, lo, hi, load):
        here = pl.ds(pl.multiple_of(tile * TILE, TILE), TILE)
        pairs = [[load(c, k) for k in range(LEV)] for c in range(2)]
        for c in range(2):
            column = None
            for k in range(LEV):
                tracers[c, k, here, lo:hi] = pairs[c][k][0]
                term = (thick[k] / total) * pairs[c][k][1]
                column = term if column is None else column + term
            shift = state[1 + c, here, lo:hi] - column
            gate = opens[c, here, lo:hi]
            for k in range(LEV):
                velocity[c, k, here, lo:hi] = gate * (pairs[c][k][1] + shift)

    def step(tile, _):
        here = pl.ds(pl.multiple_of(tile * TILE, TILE), TILE)

        @pl.when(polar)
        def _():
            for lo in range(0, MAIN, 128):
                finish(tile, lo, lo + 128, lambda c, k: (
                    ret[c * LEV + k, tile, :, lo : lo + 128],
                    ret[c * LEV + k, tile, :, MAIN + lo : MAIN + lo + 128],
                ))

            def tail(c, k):
                q = c * LEV + k
                first, second = unpack_tail(q, ret[q, tile, :, 2 * MAIN : PACK], rest_in[int(q >= NEAR), tile])
                return first[:, :TAIL], second[:, :TAIL]

            finish(tile, MAIN, COLS, tail)

        @pl.when(jnp.logical_not(polar))
        def _():
            for lo, hi in ((0, 128), (128, 256), (256, MAIN), (MAIN, COLS)):
                finish(tile, lo, hi, lambda c, k: (held[0, c, k, here, lo:hi], held[1, c, k, here, lo:hi]))

        pltpu.make_async_copy(tracers.at[:, :, here, :], tracers_out.at[:, :, here, :], sems.at[0]).start()
        pltpu.make_async_copy(velocity.at[:, :, here, :], velocity_out.at[:, :, here, :], sems.at[1]).start()
        return 0

    lax.fori_loop(0, LON, step, 0)
    pltpu.make_async_copy(tracers, tracers_out, sems.at[0]).wait()
    pltpu.make_async_copy(velocity, velocity_out, sems.at[1]).wait()
    save_sea.wait()


def body(fields, thickness, cutoff, barotropic, land_sea):
    f32 = jnp.float32
    high, low, twist = tables()
    sds = jax.ShapeDtypeStruct
    split = fields.reshape(2, 2, LEV, ROWS, COLS)
    held, ret, rest, state, opens = pl.pallas_call(
        wave_kernel,
        out_shape=(
            VMEM((2, 2, LEV, ROWS, COLS), f32),
            VMEM((CHUNKS, LON, TILE, PACK), f32),
            VMEM((2, LON, TILE, 128), f32),
            VMEM((3, ROWS, COLS), f32),
            VMEM((2, ROWS, COLS), f32),
        ),
        in_specs=[
            pl.BlockSpec(memory_space=pltpu.HBM),
            pl.BlockSpec(memory_space=pltpu.HBM),
            pl.BlockSpec(memory_space=pltpu.HBM),
            pl.BlockSpec(memory_space=pltpu.SMEM),
            pl.BlockSpec(memory_space=pltpu.HBM),
            pl.BlockSpec(memory_space=pltpu.HBM),
            pl.BlockSpec(memory_space=VMEM),
        ],
        out_specs=[pl.BlockSpec(memory_space=VMEM)] * 5,
        scratch_shapes=[
            VMEM((NEAR, LON, TILE, PACK), f32),
            VMEM((2, LON, TILE, 128), f32),
            VMEM((NEAR, LON, TILE, PACK), f32),
            VMEM((LON, TILE, 128), f32),
            VMEM((FAR, LON, TILE, PACK), f32),
            VMEM((LON, TILE, 128), f32),
            VMEM((2, ROWS, 128), f32),
            VMEM((CHUNKS, LON, TILE, PACK), f32),
            VMEM((2, ROWS, 128), f32),
            VMEM((WIDE, 2 * WIDE), jnp.bfloat16),
            VMEM((WIDE, 2 * WIDE), jnp.bfloat16),
            VMEM((128, WIDE), jnp.bfloat16),
            VMEM((128, WIDE), jnp.bfloat16),
            VMEM((128, 2 * WIDE), f32),
            VMEM((LON, TILE, WIDE), f32),
            VMEM((3, ROWS, COLS), f32),
            VMEM((ROWS, COLS), jnp.int32),
            VMEM((4, ROWS, WIDE), f32),
            VMEM((ROWS, 128), f32),
            VMEM((ROWS, 128), f32),
            VMEM((4, EXT, WIDE), f32),
            VMEM((EXT, 128), f32),
            VMEM((EXT, 128), f32),
            VMEM((4, EXT, WIDE), f32),
            VMEM((2, EXT, WIDE), f32),
            pltpu.SemaphoreType.DMA((4,)),
            pltpu.SemaphoreType.DMA((NEAR,)),
            pltpu.SemaphoreType.DMA((2, LON)),
            pltpu.SemaphoreType.DMA((NEAR,)),
            pltpu.SemaphoreType.DMA,
            pltpu.SemaphoreType.DMA((3,)),
            pltpu.SemaphoreType.DMA((FAR, LON)),
            pltpu.SemaphoreType.DMA((LON,)),
            pltpu.SemaphoreType.DMA((2,)),
            pltpu.SemaphoreType.DMA((8,)),
            pltpu.SemaphoreType.DMA((8,)),
            pltpu.SemaphoreType.DMA((5,)),
            pltpu.SemaphoreType.DMA((CHUNKS,)),
        ],
        compiler_params=pltpu.CompilerParams(
            collective_id=0, has_side_effects=True, vmem_limit_bytes=53 * 1024 * 1024
        ),
        name="wave",
    )(split, barotropic, land_sea, cutoff, jnp.asarray(high), jnp.asarray(low), jnp.asarray(twist))

    return tuple(
        pl.pallas_call(
            final_kernel,
            out_shape=(
                sds((2, LEV, ROWS, COLS), f32),
                sds((2, LEV, ROWS, COLS), f32),
                sds((ROWS, COLS), f32),
            ),
            in_specs=[
                pl.BlockSpec(memory_space=pltpu.SMEM),
                pl.BlockSpec(memory_space=VMEM),
                pl.BlockSpec(memory_space=VMEM),
                pl.BlockSpec(memory_space=VMEM),
                pl.BlockSpec(memory_space=VMEM),
                pl.BlockSpec(memory_space=VMEM),
            ],
            out_specs=[pl.BlockSpec(memory_space=ANY)] * 3,
            scratch_shapes=[
                VMEM((2, LEV, ROWS, COLS), f32),
                VMEM((2, LEV, ROWS, COLS), f32),
                pltpu.SemaphoreType.DMA((3,)),
            ],
            compiler_params=pltpu.CompilerParams(vmem_limit_bytes=16 * 1024 * 1024),
            name="final",
        )(thickness, held, ret, rest, state, opens)
    )


def solution(mesh):
    return jax.shard_map(
        body,
        mesh=mesh,
        in_specs=(P(None, None, "lat", "lon"), P(), P(), P(None, "lat", "lon"), P("lat", "lon")),
        out_specs=(P(None, None, "lat", "lon"), P(None, None, "lat", "lon"), P("lat", "lon")),
        check_vma=False,
    )
```

```python
import math

import jax
import jax.numpy as jnp
import ml_dtypes
import numpy as np
from jax import lax
from jax.experimental import pallas as pl
from jax.experimental.pallas import tpu as pltpu
from jax.sharding import PartitionSpec as P

MESH = pl.DeviceIdType.MESH
ANY = pl.ANY
VMEM = pltpu.VMEM

WAVE = 0.65
SUB = 20
POLE_DEV = 2
LON, LAT = 8, 16
ROWS, COLS = 64, 450
NLON = LON * COLS
NLAT = LAT * ROWS
LEV = 8
NF = 4
WIDE = 512
HALO = 24
EXT = ROWS + 2 * HALO
TILE = 8
CHUNKS = 16
NEAR = 11
FAR = CHUNKS - NEAR
PER_CHUNK = 2
FIRST = 2
MAIN = 384
PACK = 2 * MAIN + 128
TAIL = COLS - MAIN
LANE_TILES = ((0, 128), (128, 256), (256, 384), (384, WIDE))


def tables():
    r = np.arange(COLS)
    angle = 2.0 * np.pi * ((r[:, None] * r[None, :]) % COLS) / COLS
    full = np.zeros((WIDE, 2 * WIDE), np.float64)
    full[:COLS, :COLS] = np.cos(angle)
    full[:COLS, WIDE : WIDE + COLS] = np.sin(angle)
    full = full.astype(np.float32)
    high = full.astype(ml_dtypes.bfloat16)
    low = (full - high.astype(np.float32)).astype(ml_dtypes.bfloat16)
    turn = 2.0 * np.pi * (np.arange(LON)[:, None] * r[None, :]) / NLON
    twist = np.zeros((2, LON, WIDE), np.float32)
    twist[0, :, :COLS] = np.cos(turn)
    twist[1, :, :COLS] = np.sin(turn)
    return high, low, twist


def butterflies(z, sign):
    n = len(z)
    if n == 1:
        return z
    even = butterflies(z[0::2], sign)
    odd = butterflies(z[1::2], sign)
    low, high = [], []
    for k in range(n // 2):
        er, ei = even[k]
        tr, ti = odd[k]
        if 4 * k == n:
            tr, ti = (-ti, tr) if sign > 0 else (ti, -tr)
        elif k:
            c = math.cos(2.0 * math.pi * k / n)
            s = sign * math.sin(2.0 * math.pi * k / n)
            tr, ti = c * tr - s * ti, c * ti + s * tr
        low.append((er + tr, ei + ti))
        high.append((er - tr, ei - ti))
    return low + high


def put_split(high_ref, low_ref, s, lanes, re, im):
    value = jnp.concatenate([re, im], axis=0)
    top = value.astype(jnp.bfloat16)
    rows = slice(s * 16, s * 16 + 16)
    high_ref[rows, lanes[0] : lanes[1]] = top
    low_ref[rows, lanes[0] : lanes[1]] = (value - top.astype(jnp.float32)).astype(jnp.bfloat16)


def multiply(high_ref, low_ref, wh_ref, wl_ref, out_ref):
    for block in range(4):
        cols = slice(block * 256, (block + 1) * 256)
        out_ref[:, cols] = (
            jnp.dot(high_ref[...], wh_ref[:, cols], preferred_element_type=jnp.float32)
            + jnp.dot(low_ref[...], wh_ref[:, cols], preferred_element_type=jnp.float32)
            + jnp.dot(high_ref[...], wl_ref[:, cols], preferred_element_type=jnp.float32)
        )


def lanes_of(rows):
    return lax.broadcasted_iota(jnp.int32, (rows, 128), 1)


def pack_tail(first, second):
    return jnp.where(lanes_of(first.shape[0]) < 64, first, pltpu.roll(second, 64, 1))


def pack_rest(q, first, second, rest):
    slot = lanes_of(first.shape[0]) // 2
    rest = jnp.where(slot == 2 * q, pltpu.roll(first, lax.rem(4 * q + 64, 128), 1), rest)
    return jnp.where(slot == 2 * q + 1, pltpu.roll(second, lax.rem(4 * q + 66, 128), 1), rest)


def unpack_tail(q, tail, rest):
    lane = lanes_of(tail.shape[0])
    first = jnp.where(lane < 64, tail, pltpu.roll(rest, (192 - 4 * q) % 128, 1))
    second = jnp.where(lane < 64, pltpu.roll(tail, 64, 1), pltpu.roll(rest, (190 - 4 * q) % 128, 1))
    return jnp.where(lane < TAIL, first, 0.0), jnp.where(lane < TAIL, second, 0.0)


def filter_chunk(j, q, recv, back, twist, mask, yh, yl, wh, wl, prod):
    got, recv_rest = recv
    back, back_rest = back
    for lo, hi in LANE_TILES:
        if lo < MAIN:
            z = [(got[j, d, :, lo:hi], got[j, d, :, MAIN + lo : MAIN + hi]) for d in range(LON)]
        else:
            part = jnp.minimum(q, 1)
            z = [unpack_tail(q, got[j, d, :, 2 * MAIN : PACK], recv_rest[part, d]) for d in range(LON)]
        y = butterflies(z, -1)
        for s in range(LON):
            re, im = y[s]
            if s:
                c = twist[0, s : s + 1, lo:hi]
                n = twist[1, s : s + 1, lo:hi]
                re, im = re * c + im * n, im * c - re * n
            put_split(yh, yl, s, (lo, hi), re, im)
    multiply(yh, yl, wh, wl, prod)
    for lo, hi in LANE_TILES:
        for s in range(LON):
            a = slice(s * 16, s * 16 + 8)
            b = slice(s * 16 + 8, s * 16 + 16)
            keep = mask[s, :, lo:hi]
            re = (prod[a, lo:hi] + prod[b, WIDE + lo : WIDE + hi]) * keep
            im = (prod[b, lo:hi] - prod[a, WIDE + lo : WIDE + hi]) * keep
            put_split(yh, yl, s, (lo, hi), re, im)
    multiply(yh, yl, wh, wl, prod)
    for lo, hi in LANE_TILES:
        z = []
        for s in range(LON):
            a = slice(s * 16, s * 16 + 8)
            b = slice(s * 16 + 8, s * 16 + 16)
            re = prod[a, lo:hi] - prod[b, WIDE + lo : WIDE + hi]
            im = prod[b, lo:hi] + prod[a, WIDE + lo : WIDE + hi]
            if s:
                c = twist[0, s : s + 1, lo:hi]
                n = twist[1, s : s + 1, lo:hi]
                re, im = re * c - im * n, im * c + re * n
            z.append((re, im))
        x = butterflies(z, 1)
        for d in range(LON):
            if lo < MAIN:
                back[j, d, :, lo:hi] = x[d][0]
                back[j, d, :, MAIN + lo : MAIN + hi] = x[d][1]
            else:
                back[j, d, :, 2 * MAIN : PACK] = pack_tail(*x[d])
                back_rest[d] = pack_rest(q, *x[d], back_rest[d])


def wave_kernel(
    fields, baro, land, cutoff_hbm, wh_hbm, wl_hbm, twist_hbm, thick_hbm,
    held, ret, rest_in, state_out, open_out, weights,
    cutoff, twist, thick,
    recv, recv_rest, back, back_rest, relay, relay_rest, stage, packed, rest_out, wh, wl, yh, yl, prod, mask,
    own, own_land, src4, edge_r, edge_l, st_c, st_l, st_r, ext, opens,
    fwd_send, fwd_recv, fwd_rest, ret_send, ret_rest, ret_recv,
    relay_recv, relay_rests, relay_send, halo_send, halo_recv, local_sem, load_sem,
):
    lon = lax.axis_index("lon")
    lat = lax.axis_index("lat")
    pair = lat // 2
    core = lax.rem(lat, 2)
    north = lax.rem(pair, 4) < 2
    polar = (pair == 0) | (pair == 7)
    near_y = (pair == 3) | (pair == 4)
    relays = (pair == 1) | (pair == 6)
    far = (pair == 2) | (pair == 5)
    worker = near_y | far
    home = jnp.where(north, 0, LAT - 2) + core
    y_lat = jnp.where(north, 8, 6) + core
    relay_lat = jnp.where(north, 2, 12) + core
    far_lat = jnp.where(north, 10, 4) + core

    load_state = pltpu.make_async_copy(baro, own, local_sem.at[0])
    load_land = pltpu.make_async_copy(land, own_land, local_sem.at[1])
    load_state.start()
    load_land.start()
    load_wh = pltpu.make_async_copy(wh_hbm, wh, local_sem.at[2])
    load_wl = pltpu.make_async_copy(wl_hbm, wl, local_sem.at[3])
    load_twist = pltpu.make_async_copy(twist_hbm, twist, local_sem.at[5])
    load_cutoff = pltpu.make_async_copy(cutoff_hbm, cutoff, local_sem.at[6])
    load_thick = pltpu.make_async_copy(thick_hbm, thick, local_sem.at[7])
    load_thick.start()

    keep_own = pltpu.make_async_copy(fields, held, local_sem.at[4])

    @pl.when(worker)
    def _():
        load_wh.start()
        load_wl.start()
        load_twist.start()
        load_cutoff.start()

    def load_chunk(q):
        at = (q // LEV, lax.rem(q, LEV))
        return pltpu.make_async_copy(
            fields.at[:, at[0], at[1]], held.at[:, at[0], at[1]], load_sem.at[q]
        )

    @pl.when(polar)
    def _():
        def start(q, _):
            load_chunk(q).start()
            return 0

        lax.fori_loop(0, CHUNKS, start, 0)

    @pl.when(jnp.logical_not(polar))
    def _():
        keep_own.start()

    sides = [(dx, dy) for dy in (0, 1, -1) for dx in (-1, 0, 1) if (dx, dy) != (0, 0)]

    def near(dx, dy):
        return {"lon": lax.rem(lon + dx + LON, LON), "lat": lax.rem(lat + dy + LAT, LAT)}

    def inside(dy):
        return lat < LAT - 1 if dy > 0 else lat > 0

    def when_inside(dy, action):
        if dy == 0:
            action()
        else:
            pl.when(inside(dy))(action)

    barrier = pltpu.get_barrier_semaphore()

    def greet_at(lon_index, lat_index):
        pl.semaphore_signal(
            barrier, inc=1, device_id={"lon": lon_index, "lat": lat_index}, device_id_type=MESH
        )

    def greet_row(lat_index):
        def one(t, _):
            greet_at(t, lat_index)
            return 0

        lax.fori_loop(0, LON, one, 0)

    for dx, dy in sides:
        when_inside(dy, lambda dx=dx, dy=dy: greet_at(near(dx, dy)["lon"], near(dx, dy)["lat"]))

    @pl.when(polar)
    def _():
        greet_row(y_lat)
        greet_row(far_lat)
        greet_at(lon, relay_lat)

    @pl.when(near_y)
    def _():
        greet_row(home)

    @pl.when(far)
    def _():
        greet_row(home)
        greet_row(relay_lat)

    @pl.when(relays)
    def _():
        greet_row(far_lat)
        greet_at(lon, home)

    load_state.wait()
    load_land.wait()
    for c in range(3):
        src4[c, :, 0:384] = own[c, :, 0:384]
        src4[c, :, 384:COLS] = own[c, :, 384:COLS]
    src4[3, :, 0:384] = own_land[:, 0:384].astype(jnp.float32)
    src4[3, :, 384:COLS] = own_land[:, 384:COLS].astype(jnp.float32)
    src4[:, :, COLS:WIDE] = jnp.zeros((4, ROWS, WIDE - COLS), jnp.float32)
    st_c[:, HALO : HALO + ROWS, :] = src4[...]
    lane = lax.broadcasted_iota(jnp.int32, (ROWS, 128), 1)
    right_pack = jnp.zeros((ROWS, 128), jnp.float32)
    left_pack = right_pack
    for c in range(4):
        here = (lane >= c * HALO) & (lane < (c + 1) * HALO)
        right_edge = pltpu.roll(src4[c, :, 384:512], (c * HALO - (COLS - HALO - 384)) % 128, 1)
        left_edge = src4[c, :, 0:128]
        if c:
            left_edge = pltpu.roll(left_edge, c * HALO, 1)
        right_pack = jnp.where(here, right_edge, right_pack)
        left_pack = jnp.where(here, left_edge, left_pack)
    edge_r[...] = right_pack
    edge_l[...] = left_pack

    full = len(sides) - jnp.where((lat == 0) | (lat == LAT - 1), 3, 0)
    extra = jnp.where(polar, 2 * LON + 1, jnp.where(near_y, LON, jnp.where(far, 2 * LON, LON + 1)))
    pl.semaphore_wait(barrier, full + extra)

    def rows(t):
        return pl.ds(pl.multiple_of(t * TILE, TILE), TILE)

    def push(src, dst, send_sem, recv_sem, lon_index, lat_index):
        pltpu.make_async_remote_copy(
            src_ref=src, dst_ref=dst, send_sem=send_sem, recv_sem=recv_sem,
            device_id={"lon": lon_index, "lat": lat_index}, device_id_type=MESH,
        ).start()

    def arrived(ref, sem):
        pltpu.make_async_copy(ref, ref, sem).wait()

    def each_lon(action):
        def one(t, _):
            action(t)
            return 0

        lax.fori_loop(0, LON, one, 0)

    def pack_chunk(q, rest):
        load_chunk(q).wait()
        for i in range(2):
            packed[q, :, :, i * MAIN : (i + 1) * MAIN] = held[
                i, q // LEV, lax.rem(q, LEV), :, 0:MAIN
            ].reshape(LON, TILE, MAIN)
            stage[i, :, 0:TAIL] = held[i, q // LEV, lax.rem(q, LEV), :, MAIN:COLS]
        packed[q, :, :, 2 * MAIN : PACK] = pack_tail(stage[0], stage[1]).reshape(LON, TILE, 128)
        return pack_rest(q, stage[0], stage[1], rest)

    def send_chunk(q, slot, lat_index):
        each_lon(lambda t: push(
            packed.at[q, t], recv.at[slot, lon], fwd_send.at[0], fwd_recv.at[slot], t, lat_index
        ))

    def send_rest(part, lat_index, sem):
        each_lon(lambda t: push(
            rest_out.at[part, rows(t), :], recv_rest.at[part, lon], fwd_send.at[sem], fwd_rest.at[part, lon],
            t, lat_index,
        ))

    @pl.when(polar)
    def _():
        rest_out[0] = pack_chunk(0, jnp.zeros((ROWS, 128), jnp.float32))
        send_rest(0, y_lat, 1)
        send_chunk(0, 0, y_lat)

    row_src = {1: slice(ROWS - HALO, ROWS), 0: slice(0, ROWS), -1: slice(0, HALO)}
    row_dst = {1: slice(0, HALO), 0: slice(HALO, HALO + ROWS), -1: slice(HALO + ROWS, EXT)}
    copies = []
    for n, (dx, dy) in enumerate(sides):
        if dx == 0:
            src = src4.at[:, row_src[dy], :]
            dst = st_c.at[:, row_dst[dy], :]
        else:
            src = (edge_r if dx == 1 else edge_l).at[row_src[dy], :]
            dst = (st_l if dx == 1 else st_r).at[row_dst[dy], :]
        copy = pltpu.make_async_remote_copy(
            src_ref=src, dst_ref=dst, send_sem=halo_send.at[n], recv_sem=halo_recv.at[n],
            device_id=near(dx, dy), device_id_type=MESH,
        )
        when_inside(dy, copy.start)
        copies.append((dy, copy))

    @pl.when(polar)
    def _():
        rest_out[1] = lax.fori_loop(1, CHUNKS, pack_chunk, jnp.zeros((ROWS, 128), jnp.float32))
        send_rest(1, y_lat, 2)
        send_rest(1, far_lat, 3)

        def step(k, _):
            send_chunk(NEAR + k, k, far_lat)
            send_chunk(2 * k + 1, 2 * k + 1, y_lat)
            send_chunk(2 * k + 2, 2 * k + 2, y_lat)
            return 0

        lax.fori_loop(0, FAR, step, 0)

    @pl.when(jnp.logical_not(polar))
    def _():
        keep_own.wait()

    def assemble():
        for dy, copy in copies:
            when_inside(dy, copy.wait_send)
            when_inside(-dy, copy.wait_recv)
        for dy in (1, -1):
            @pl.when(jnp.logical_not(inside(-dy)))
            def _(dy=dy):
                st_c[:, row_dst[dy], :] = jnp.zeros((4, HALO, WIDE), jnp.float32)
                st_l[row_dst[dy], :] = jnp.zeros((HALO, 128), jnp.float32)
                st_r[row_dst[dy], :] = jnp.zeros((HALO, 128), jnp.float32)

        lane_ext = lax.broadcasted_iota(jnp.int32, (EXT, 128), 1)
        edge = HALO + COLS - 384
        for c in range(4):
            mid = pltpu.roll(st_c[c], HALO, 1)
            ext[c, :, 128:384] = mid[:, 128:384]
            left = pltpu.roll(st_l[...], 128 - c * HALO, 1) if c else st_l[...]
            ext[c, :, 0:128] = jnp.where(lane_ext < HALO, left, mid[:, 0:128])
            right = pltpu.roll(st_r[...], (edge - c * HALO) % 128, 1)
            right = jnp.where(lane_ext < edge + HALO, right, 0.0)
            ext[c, :, 384:512] = jnp.where(lane_ext >= edge, right, mid[:, 384:512])

        ocean = ext[3]
        row_id = lat * ROWS - HALO + lax.broadcasted_iota(jnp.int32, (EXT, WIDE), 0)
        east_open = ocean * pltpu.roll(ocean, WIDE - 1, 1)
        north_open = jnp.where(row_id == NLAT - 1, 0.0, ocean * pltpu.roll(ocean, EXT - 1, 0))
        opens[0] = east_open
        opens[1] = north_open
        ext[1] = ext[1] * east_open
        ext[2] = ext[2] * north_open
        ext[3] = WAVE * ocean

    def subcycle(_, carry):
        east = ext[1]
        north = ext[2]
        div = east - pltpu.roll(east, 1, 1) + north - pltpu.roll(north, 1, 0)
        surface = ext[0] - ext[3] * div
        ext[0] = surface
        ext[1] = opens[0] * (east - WAVE * (pltpu.roll(surface, WIDE - 1, 1) - surface))
        ext[2] = opens[1] * (north - WAVE * (pltpu.roll(surface, EXT - 1, 0) - surface))
        return carry

    chunks = jnp.where(near_y, NEAR, jnp.where(far, FAR, 0))

    @pl.when(jnp.logical_not(worker))
    def _():
        assemble()

    @pl.when(worker)
    def _():
        load_wh.wait()
        load_wl.wait()
        load_twist.wait()
        load_cutoff.wait()
        first = (jnp.where(north, 0, 2) + core) * ROWS + lon * TILE
        sub = lax.broadcasted_iota(jnp.int32, (TILE, WIDE), 0)
        wave = LON * lax.broadcasted_iota(jnp.int32, (TILE, WIDE), 1)
        limit = jnp.zeros((TILE, WIDE), jnp.int32)
        for i in range(TILE):
            limit = jnp.where(sub == i, cutoff[first + i], limit)
        for s in range(LON):
            m = wave + s
            folded = jnp.minimum(m, NLON - m)
            mask[s] = jnp.where(folded <= limit, 1.0 / NLON, 0.0)
        back_rest[...] = jnp.zeros_like(back_rest)
        q_first = jnp.where(near_y, 0, NEAR)

        @pl.when(near_y)
        def _():
            each_lon(lambda d: arrived(recv_rest.at[0, d], fwd_rest.at[0, d]))

        def chunk(j, _):
            arrived(recv.at[j], fwd_recv.at[j])

            @pl.when(j == jnp.where(near_y, 1, 0))
            def _():
                each_lon(lambda d: arrived(recv_rest.at[1, d], fwd_rest.at[1, d]))

            filter_chunk(
                j, q_first + j, (recv, recv_rest), (back, back_rest), twist, mask, yh, yl, wh, wl, prod
            )

            @pl.when(near_y)
            def _():
                each_lon(lambda d: push(back.at[j, d], ret.at[j, lon], ret_send.at[j], ret_recv.at[0], d, home))

            @pl.when(far)
            def _():
                each_lon(lambda d: push(
                    back.at[j, d], relay.at[j, lon], ret_send.at[j], relay_recv.at[j, lon], d, relay_lat
                ))

            @pl.when(near_y & (j == NEAR - 1))
            def _():
                each_lon(lambda d: push(
                    back_rest.at[d], rest_in.at[0, lon], ret_rest, ret_recv.at[1], d, home
                ))

            @pl.when(far & (j == FAR - 1))
            def _():
                each_lon(lambda d: push(
                    back_rest.at[d], relay_rest.at[lon], ret_rest, relay_rests.at[lon], d, relay_lat
                ))

            pl.when(j == FIRST - 1)(assemble)
            lax.fori_loop(0, jnp.where(j >= FIRST, PER_CHUNK, 0), subcycle, 0)
            return 0

        lax.fori_loop(0, chunks, chunk, 0)

    load_thick.wait()
    total = thick[0]
    for k in range(1, LEV):
        total = total + thick[k]
    for k in range(LEV):
        weights[k : k + 1, :] = jnp.full((1, 128), thick[k]) / total

    left_over = SUB - PER_CHUNK * jnp.maximum(chunks - FIRST, 0)
    lax.fori_loop(0, left_over, subcycle, 0)

    inner = slice(HALO, HALO + ROWS)
    for c in range(3):
        moved = pltpu.roll(ext[c, inner, :], WIDE - HALO, 1)
        state_out[c] = moved[:, :COLS]
    for c in range(2):
        moved = pltpu.roll(opens[c, inner, :], WIDE - HALO, 1)
        open_out[c] = moved[:, :COLS]

    @pl.when(relays)
    def _():
        def pass_chunk(j, _):
            def pass_on(t):
                arrived(relay.at[j, t], relay_recv.at[j, t])
                push(relay.at[j, t], ret.at[NEAR + j, t], relay_send.at[0], ret_recv.at[0], lon, home)

            each_lon(pass_on)
            return 0

        lax.fori_loop(0, FAR, pass_chunk, 0)

        def pass_rest(t):
            arrived(relay_rest.at[t], relay_rests.at[t])
            push(relay_rest.at[t], rest_in.at[1, t], relay_send.at[1], ret_recv.at[2], lon, home)

        each_lon(pass_rest)
        arrived(relay, relay_send.at[0])
        arrived(relay_rest, relay_send.at[1])

    @pl.when(worker)
    def _():
        def sent(j, _):
            arrived(back.at[j], ret_send.at[j])
            return 0

        lax.fori_loop(0, chunks, sent, 0)
        arrived(back_rest, ret_rest)

    @pl.when(polar)
    def _():
        arrived(packed, fwd_send.at[0])
        arrived(rest_out.at[0], fwd_send.at[1])
        arrived(rest_out.at[1], fwd_send.at[2])
        arrived(rest_out.at[1], fwd_send.at[3])
        arrived(ret, ret_recv.at[0])
        arrived(rest_in.at[0], ret_recv.at[1])
        arrived(rest_in.at[1], ret_recv.at[2])


def final_kernel(
    weights, held, ret, rest_in, state, opens, tracers_out, velocity_out, sea_out, tracers, velocity, sems
):
    lat = lax.axis_index("lat")
    polar = (lat < POLE_DEV) | (lat >= LAT - POLE_DEV)
    save_sea = pltpu.make_async_copy(state.at[0], sea_out, sems.at[2])
    save_sea.start()

    def finish(tile, lo, hi, load):
        here = pl.ds(pl.multiple_of(tile * TILE, TILE), TILE)
        pairs = [[load(c, k) for k in range(LEV)] for c in range(2)]
        for c in range(2):
            column = None
            for k in range(LEV):
                tracers[c, k, here, lo:hi] = pairs[c][k][0]
                term = weights[k : k + 1, 0 : hi - lo] * pairs[c][k][1]
                column = term if column is None else column + term
            shift = state[1 + c, here, lo:hi] - column
            gate = opens[c, here, lo:hi]
            for k in range(LEV):
                velocity[c, k, here, lo:hi] = gate * (pairs[c][k][1] + shift)

    def step(tile, _):
        here = pl.ds(pl.multiple_of(tile * TILE, TILE), TILE)

        @pl.when(polar)
        def _():
            for lo in range(0, MAIN, 128):
                finish(tile, lo, lo + 128, lambda c, k: (
                    ret[c * LEV + k, tile, :, lo : lo + 128],
                    ret[c * LEV + k, tile, :, MAIN + lo : MAIN + lo + 128],
                ))

            def tail(c, k):
                q = c * LEV + k
                first, second = unpack_tail(q, ret[q, tile, :, 2 * MAIN : PACK], rest_in[int(q >= NEAR), tile])
                return first[:, :TAIL], second[:, :TAIL]

            finish(tile, MAIN, COLS, tail)

        @pl.when(jnp.logical_not(polar))
        def _():
            for lo, hi in ((0, 128), (128, 256), (256, MAIN), (MAIN, COLS)):
                finish(tile, lo, hi, lambda c, k: (held[0, c, k, here, lo:hi], held[1, c, k, here, lo:hi]))

        pltpu.make_async_copy(tracers.at[:, :, here, :], tracers_out.at[:, :, here, :], sems.at[0]).start()
        pltpu.make_async_copy(velocity.at[:, :, here, :], velocity_out.at[:, :, here, :], sems.at[1]).start()
        return 0

    lax.fori_loop(0, LON, step, 0)
    pltpu.make_async_copy(tracers, tracers_out, sems.at[0]).wait()
    pltpu.make_async_copy(velocity, velocity_out, sems.at[1]).wait()
    save_sea.wait()


def body(fields, thickness, cutoff, barotropic, land_sea):
    f32 = jnp.float32
    high, low, twist = tables()
    sds = jax.ShapeDtypeStruct
    split = fields.reshape(2, 2, LEV, ROWS, COLS)
    held, ret, rest, state, opens, weights = pl.pallas_call(
        wave_kernel,
        out_shape=(
            VMEM((2, 2, LEV, ROWS, COLS), f32),
            VMEM((CHUNKS, LON, TILE, PACK), f32),
            VMEM((2, LON, TILE, 128), f32),
            VMEM((3, ROWS, COLS), f32),
            VMEM((2, ROWS, COLS), f32),
            VMEM((LEV, 128), f32),
        ),
        in_specs=[pl.BlockSpec(memory_space=pltpu.HBM)] * 8,
        out_specs=[pl.BlockSpec(memory_space=VMEM)] * 6,
        scratch_shapes=[
            pltpu.SMEM((2 * POLE_DEV * ROWS,), jnp.int32),
            VMEM((2, LON, WIDE), f32),
            pltpu.SMEM((LEV,), f32),
            VMEM((NEAR, LON, TILE, PACK), f32),
            VMEM((2, LON, TILE, 128), f32),
            VMEM((NEAR, LON, TILE, PACK), f32),
            VMEM((LON, TILE, 128), f32),
            VMEM((FAR, LON, TILE, PACK), f32),
            VMEM((LON, TILE, 128), f32),
            VMEM((2, ROWS, 128), f32),
            VMEM((CHUNKS, LON, TILE, PACK), f32),
            VMEM((2, ROWS, 128), f32),
            VMEM((WIDE, 2 * WIDE), jnp.bfloat16),
            VMEM((WIDE, 2 * WIDE), jnp.bfloat16),
            VMEM((128, WIDE), jnp.bfloat16),
            VMEM((128, WIDE), jnp.bfloat16),
            VMEM((128, 2 * WIDE), f32),
            VMEM((LON, TILE, WIDE), f32),
            VMEM((3, ROWS, COLS), f32),
            VMEM((ROWS, COLS), jnp.int32),
            VMEM((4, ROWS, WIDE), f32),
            VMEM((ROWS, 128), f32),
            VMEM((ROWS, 128), f32),
            VMEM((4, EXT, WIDE), f32),
            VMEM((EXT, 128), f32),
            VMEM((EXT, 128), f32),
            VMEM((4, EXT, WIDE), f32),
            VMEM((2, EXT, WIDE), f32),
            pltpu.SemaphoreType.DMA((4,)),
            pltpu.SemaphoreType.DMA((NEAR,)),
            pltpu.SemaphoreType.DMA((2, LON)),
            pltpu.SemaphoreType.DMA((NEAR,)),
            pltpu.SemaphoreType.DMA,
            pltpu.SemaphoreType.DMA((3,)),
            pltpu.SemaphoreType.DMA((FAR, LON)),
            pltpu.SemaphoreType.DMA((LON,)),
            pltpu.SemaphoreType.DMA((2,)),
            pltpu.SemaphoreType.DMA((8,)),
            pltpu.SemaphoreType.DMA((8,)),
            pltpu.SemaphoreType.DMA((8,)),
            pltpu.SemaphoreType.DMA((CHUNKS,)),
        ],
        compiler_params=pltpu.CompilerParams(
            collective_id=0, has_side_effects=True, vmem_limit_bytes=53 * 1024 * 1024
        ),
        name="wave",
    )(split, barotropic, land_sea, cutoff, jnp.asarray(high), jnp.asarray(low), jnp.asarray(twist), thickness)

    return tuple(
        pl.pallas_call(
            final_kernel,
            out_shape=(
                sds((2, LEV, ROWS, COLS), f32),
                sds((2, LEV, ROWS, COLS), f32),
                sds((ROWS, COLS), f32),
            ),
            in_specs=[
                pl.BlockSpec(memory_space=VMEM),
                pl.BlockSpec(memory_space=VMEM),
                pl.BlockSpec(memory_space=VMEM),
                pl.BlockSpec(memory_space=VMEM),
                pl.BlockSpec(memory_space=VMEM),
                pl.BlockSpec(memory_space=VMEM),
            ],
            out_specs=[pl.BlockSpec(memory_space=ANY)] * 3,
            scratch_shapes=[
                VMEM((2, LEV, ROWS, COLS), f32),
                VMEM((2, LEV, ROWS, COLS), f32),
                pltpu.SemaphoreType.DMA((3,)),
            ],
            compiler_params=pltpu.CompilerParams(vmem_limit_bytes=16 * 1024 * 1024),
            name="final",
        )(weights, held, ret, rest, state, opens)
    )


def solution(mesh):
    return jax.shard_map(
        body,
        mesh=mesh,
        in_specs=(P(None, None, "lat", "lon"), P(), P(), P(None, "lat", "lon"), P("lat", "lon")),
        out_specs=(P(None, None, "lat", "lon"), P(None, None, "lat", "lon"), P("lat", "lon")),
        check_vma=False,
    )
```

```python
import math

import jax
import jax.numpy as jnp
import ml_dtypes
import numpy as np
from jax import lax
from jax.experimental import pallas as pl
from jax.experimental.pallas import tpu as pltpu
from jax.sharding import PartitionSpec as P

MESH = pl.DeviceIdType.MESH
ANY = pl.ANY
VMEM = pltpu.VMEM

WAVE = 0.65
SUB = 20
POLE_DEV = 2
LON, LAT = 8, 16
ROWS, COLS = 64, 450
NLON = LON * COLS
NLAT = LAT * ROWS
LEV = 8
NF = 4
WIDE = 512
HALO = 24
EXT = ROWS + 2 * HALO
TILE = 8
CHUNKS = 16
NEAR = 11
FAR = CHUNKS - NEAR
PER_CHUNK = 2
FIRST = 2
MAIN = 384
PACK = 2 * MAIN + 128
TAIL = COLS - MAIN
LANE_TILES = ((0, 128), (128, 256), (256, 384), (384, WIDE))


def tables():
    r = np.arange(COLS)
    angle = 2.0 * np.pi * ((r[:, None] * r[None, :]) % COLS) / COLS
    full = np.zeros((WIDE, 2 * WIDE), np.float64)
    full[:COLS, :COLS] = np.cos(angle)
    full[:COLS, WIDE : WIDE + COLS] = np.sin(angle)
    full = full.astype(np.float32)
    high = full.astype(ml_dtypes.bfloat16)
    low = (full - high.astype(np.float32)).astype(ml_dtypes.bfloat16)
    turn = 2.0 * np.pi * (np.arange(LON)[:, None] * r[None, :]) / NLON
    twist = np.zeros((2, LON, WIDE), np.float32)
    twist[0, :, :COLS] = np.cos(turn)
    twist[1, :, :COLS] = np.sin(turn)
    return high, low, twist


def butterflies(z, sign):
    n = len(z)
    if n == 1:
        return z
    even = butterflies(z[0::2], sign)
    odd = butterflies(z[1::2], sign)
    low, high = [], []
    for k in range(n // 2):
        er, ei = even[k]
        tr, ti = odd[k]
        if 4 * k == n:
            tr, ti = (-ti, tr) if sign > 0 else (ti, -tr)
        elif k:
            c = math.cos(2.0 * math.pi * k / n)
            s = sign * math.sin(2.0 * math.pi * k / n)
            tr, ti = c * tr - s * ti, c * ti + s * tr
        low.append((er + tr, ei + ti))
        high.append((er - tr, ei - ti))
    return low + high


def put_split(high_ref, low_ref, s, lanes, re, im):
    value = jnp.concatenate([re, im], axis=0)
    top = value.astype(jnp.bfloat16)
    rows = slice(s * 16, s * 16 + 16)
    high_ref[rows, lanes[0] : lanes[1]] = top
    low_ref[rows, lanes[0] : lanes[1]] = (value - top.astype(jnp.float32)).astype(jnp.bfloat16)


def multiply(high_ref, low_ref, wh_ref, wl_ref, out_ref):
    for block in range(4):
        cols = slice(block * 256, (block + 1) * 256)
        out_ref[:, cols] = (
            jnp.dot(high_ref[...], wh_ref[:, cols], preferred_element_type=jnp.float32)
            + jnp.dot(low_ref[...], wh_ref[:, cols], preferred_element_type=jnp.float32)
            + jnp.dot(high_ref[...], wl_ref[:, cols], preferred_element_type=jnp.float32)
        )


def lanes_of(rows):
    return lax.broadcasted_iota(jnp.int32, (rows, 128), 1)


def pack_tail(first, second):
    return jnp.where(lanes_of(first.shape[0]) < 64, first, pltpu.roll(second, 64, 1))


def pack_rest(q, first, second, rest):
    slot = lanes_of(first.shape[0]) // 2
    rest = jnp.where(slot == 2 * q, pltpu.roll(first, lax.rem(4 * q + 64, 128), 1), rest)
    return jnp.where(slot == 2 * q + 1, pltpu.roll(second, lax.rem(4 * q + 66, 128), 1), rest)


def unpack_tail(q, tail, rest):
    lane = lanes_of(tail.shape[0])
    first = jnp.where(lane < 64, tail, pltpu.roll(rest, (192 - 4 * q) % 128, 1))
    second = jnp.where(lane < 64, pltpu.roll(tail, 64, 1), pltpu.roll(rest, (190 - 4 * q) % 128, 1))
    return jnp.where(lane < TAIL, first, 0.0), jnp.where(lane < TAIL, second, 0.0)


def filter_chunk(j, q, recv, back, twist, mask, yh, yl, wh, wl, prod):
    got, recv_rest = recv
    back, back_rest = back
    for lo, hi in LANE_TILES:
        if lo < MAIN:
            z = [(got[j, d, :, lo:hi], got[j, d, :, MAIN + lo : MAIN + hi]) for d in range(LON)]
        else:
            part = jnp.minimum(q, 1)
            z = [unpack_tail(q, got[j, d, :, 2 * MAIN : PACK], recv_rest[part, d]) for d in range(LON)]
        y = butterflies(z, -1)
        for s in range(LON):
            re, im = y[s]
            if s:
                c = twist[0, s : s + 1, lo:hi]
                n = twist[1, s : s + 1, lo:hi]
                re, im = re * c + im * n, im * c - re * n
            put_split(yh, yl, s, (lo, hi), re, im)
    multiply(yh, yl, wh, wl, prod)
    for lo, hi in LANE_TILES:
        for s in range(LON):
            a = slice(s * 16, s * 16 + 8)
            b = slice(s * 16 + 8, s * 16 + 16)
            keep = mask[s, :, lo:hi]
            re = (prod[a, lo:hi] + prod[b, WIDE + lo : WIDE + hi]) * keep
            im = (prod[b, lo:hi] - prod[a, WIDE + lo : WIDE + hi]) * keep
            put_split(yh, yl, s, (lo, hi), re, im)
    multiply(yh, yl, wh, wl, prod)
    for lo, hi in LANE_TILES:
        z = []
        for s in range(LON):
            a = slice(s * 16, s * 16 + 8)
            b = slice(s * 16 + 8, s * 16 + 16)
            re = prod[a, lo:hi] - prod[b, WIDE + lo : WIDE + hi]
            im = prod[b, lo:hi] + prod[a, WIDE + lo : WIDE + hi]
            if s:
                c = twist[0, s : s + 1, lo:hi]
                n = twist[1, s : s + 1, lo:hi]
                re, im = re * c - im * n, im * c + re * n
            z.append((re, im))
        x = butterflies(z, 1)
        for d in range(LON):
            if lo < MAIN:
                back[j, d, :, lo:hi] = x[d][0]
                back[j, d, :, MAIN + lo : MAIN + hi] = x[d][1]
            else:
                back[j, d, :, 2 * MAIN : PACK] = pack_tail(*x[d])
                back_rest[d] = pack_rest(q, *x[d], back_rest[d])


def wave_kernel(
    fields, baro, land, cutoff_hbm, wh_hbm, wl_hbm, twist_hbm, thick_hbm,
    held, ret, rest_in, state_out, open_out, weights,
    cutoff, twist, thick,
    recv, recv_rest, back, back_rest, relay, relay_rest, stage, packed, rest_out, wh, wl, yh, yl, prod, mask,
    own, own_land, src4, edge_r, edge_l, st_c, st_l, st_r, ext, opens,
    fwd_send, fwd_recv, fwd_rest, ret_send, ret_rest, ret_recv,
    relay_recv, relay_rests, relay_send, halo_send, halo_recv, local_sem, load_sem,
):
    lon = lax.axis_index("lon")
    lat = lax.axis_index("lat")
    pair = lat // 2
    core = lax.rem(lat, 2)
    north = lax.rem(pair, 4) < 2
    polar = (pair == 0) | (pair == 7)
    near_y = (pair == 3) | (pair == 4)
    relays = (pair == 1) | (pair == 6)
    far = (pair == 2) | (pair == 5)
    worker = near_y | far
    home = jnp.where(north, 0, LAT - 2) + core
    y_lat = jnp.where(north, 8, 6) + core
    relay_lat = jnp.where(north, 2, 12) + core
    far_lat = jnp.where(north, 10, 4) + core

    load_state = pltpu.make_async_copy(baro, own, local_sem.at[0])
    load_land = pltpu.make_async_copy(land, own_land, local_sem.at[1])
    load_wh = pltpu.make_async_copy(wh_hbm, wh, local_sem.at[2])
    load_wl = pltpu.make_async_copy(wl_hbm, wl, local_sem.at[3])
    load_twist = pltpu.make_async_copy(twist_hbm, twist, local_sem.at[5])
    load_cutoff = pltpu.make_async_copy(cutoff_hbm, cutoff, local_sem.at[6])
    load_thick = pltpu.make_async_copy(thick_hbm, thick, local_sem.at[7])
    load_thick.start()

    keep_own = pltpu.make_async_copy(fields, held, local_sem.at[4])

    @pl.when(worker)
    def _():
        load_wh.start()
        load_wl.start()
        load_twist.start()
        load_cutoff.start()

    def load_chunk(q):
        at = (q // LEV, lax.rem(q, LEV))
        return pltpu.make_async_copy(
            fields.at[:, at[0], at[1]], held.at[:, at[0], at[1]], load_sem.at[q]
        )

    @pl.when(polar)
    def _():
        load_chunk(0).start()

    load_state.start()
    load_land.start()

    @pl.when(polar)
    def _():
        def start(q, _):
            load_chunk(q).start()
            return 0

        lax.fori_loop(1, CHUNKS, start, 0)

    @pl.when(jnp.logical_not(polar))
    def _():
        keep_own.start()

    sides = [(dx, dy) for dy in (0, 1, -1) for dx in (-1, 0, 1) if (dx, dy) != (0, 0)]

    def near(dx, dy):
        return {"lon": lax.rem(lon + dx + LON, LON), "lat": lax.rem(lat + dy + LAT, LAT)}

    def inside(dy):
        return lat < LAT - 1 if dy > 0 else lat > 0

    def when_inside(dy, action):
        if dy == 0:
            action()
        else:
            pl.when(inside(dy))(action)

    barrier = pltpu.get_barrier_semaphore()

    def greet_at(lon_index, lat_index):
        pl.semaphore_signal(
            barrier, inc=1, device_id={"lon": lon_index, "lat": lat_index}, device_id_type=MESH
        )

    def greet_row(lat_index):
        def one(t, _):
            greet_at(t, lat_index)
            return 0

        lax.fori_loop(0, LON, one, 0)

    for dx, dy in sides:
        when_inside(dy, lambda dx=dx, dy=dy: greet_at(near(dx, dy)["lon"], near(dx, dy)["lat"]))

    @pl.when(polar)
    def _():
        greet_row(y_lat)
        greet_row(far_lat)
        greet_at(lon, relay_lat)

    @pl.when(near_y)
    def _():
        greet_row(home)

    @pl.when(far)
    def _():
        greet_row(home)
        greet_row(relay_lat)

    @pl.when(relays)
    def _():
        greet_row(far_lat)
        greet_at(lon, home)

    def rows(t):
        return pl.ds(pl.multiple_of(t * TILE, TILE), TILE)

    def push(src, dst, send_sem, recv_sem, lon_index, lat_index):
        pltpu.make_async_remote_copy(
            src_ref=src, dst_ref=dst, send_sem=send_sem, recv_sem=recv_sem,
            device_id={"lon": lon_index, "lat": lat_index}, device_id_type=MESH,
        ).start()

    def arrived(ref, sem):
        pltpu.make_async_copy(ref, ref, sem).wait()

    def each_lon(action):
        def one(t, _):
            action(t)
            return 0

        lax.fori_loop(0, LON, one, 0)

    def pack_chunk(q, rest):
        load_chunk(q).wait()
        for i in range(2):
            packed[q, :, :, i * MAIN : (i + 1) * MAIN] = held[
                i, q // LEV, lax.rem(q, LEV), :, 0:MAIN
            ].reshape(LON, TILE, MAIN)
            stage[i, :, 0:TAIL] = held[i, q // LEV, lax.rem(q, LEV), :, MAIN:COLS]
        packed[q, :, :, 2 * MAIN : PACK] = pack_tail(stage[0], stage[1]).reshape(LON, TILE, 128)
        return pack_rest(q, stage[0], stage[1], rest)

    def send_chunk(q, slot, lat_index):
        each_lon(lambda t: push(
            packed.at[q, t], recv.at[slot, lon], fwd_send.at[0], fwd_recv.at[slot], t, lat_index
        ))

    def send_rest(part, lat_index, sem):
        each_lon(lambda t: push(
            rest_out.at[part, rows(t), :], recv_rest.at[part, lon], fwd_send.at[sem], fwd_rest.at[part, lon],
            t, lat_index,
        ))

    @pl.when(polar)
    def _():
        rest_out[0] = pack_chunk(0, jnp.zeros((ROWS, 128), jnp.float32))

    full = len(sides) - jnp.where((lat == 0) | (lat == LAT - 1), 3, 0)
    extra = jnp.where(polar, 2 * LON + 1, jnp.where(near_y, LON, jnp.where(far, 2 * LON, LON + 1)))
    pl.semaphore_wait(barrier, full + extra)

    @pl.when(polar)
    def _():
        send_rest(0, y_lat, 1)
        send_chunk(0, 0, y_lat)

    load_state.wait()
    load_land.wait()
    for c in range(3):
        src4[c, :, 0:384] = own[c, :, 0:384]
        src4[c, :, 384:COLS] = own[c, :, 384:COLS]
    src4[3, :, 0:384] = own_land[:, 0:384].astype(jnp.float32)
    src4[3, :, 384:COLS] = own_land[:, 384:COLS].astype(jnp.float32)
    src4[:, :, COLS:WIDE] = jnp.zeros((4, ROWS, WIDE - COLS), jnp.float32)
    st_c[:, HALO : HALO + ROWS, :] = src4[...]
    lane = lax.broadcasted_iota(jnp.int32, (ROWS, 128), 1)
    right_pack = jnp.zeros((ROWS, 128), jnp.float32)
    left_pack = right_pack
    for c in range(4):
        here = (lane >= c * HALO) & (lane < (c + 1) * HALO)
        right_edge = pltpu.roll(src4[c, :, 384:512], (c * HALO - (COLS - HALO - 384)) % 128, 1)
        left_edge = src4[c, :, 0:128]
        if c:
            left_edge = pltpu.roll(left_edge, c * HALO, 1)
        right_pack = jnp.where(here, right_edge, right_pack)
        left_pack = jnp.where(here, left_edge, left_pack)
    edge_r[...] = right_pack
    edge_l[...] = left_pack

    row_src = {1: slice(ROWS - HALO, ROWS), 0: slice(0, ROWS), -1: slice(0, HALO)}
    row_dst = {1: slice(0, HALO), 0: slice(HALO, HALO + ROWS), -1: slice(HALO + ROWS, EXT)}
    copies = []
    for n, (dx, dy) in enumerate(sides):
        if dx == 0:
            src = src4.at[:, row_src[dy], :]
            dst = st_c.at[:, row_dst[dy], :]
        else:
            src = (edge_r if dx == 1 else edge_l).at[row_src[dy], :]
            dst = (st_l if dx == 1 else st_r).at[row_dst[dy], :]
        copy = pltpu.make_async_remote_copy(
            src_ref=src, dst_ref=dst, send_sem=halo_send.at[n], recv_sem=halo_recv.at[n],
            device_id=near(dx, dy), device_id_type=MESH,
        )
        when_inside(dy, copy.start)
        copies.append((dy, copy))

    @pl.when(polar)
    def _():
        rest_out[1] = lax.fori_loop(1, CHUNKS, pack_chunk, jnp.zeros((ROWS, 128), jnp.float32))
        send_rest(1, y_lat, 2)
        send_rest(1, far_lat, 3)

        def step(k, _):
            send_chunk(NEAR + k, k, far_lat)
            send_chunk(2 * k + 1, 2 * k + 1, y_lat)
            send_chunk(2 * k + 2, 2 * k + 2, y_lat)
            return 0

        lax.fori_loop(0, FAR, step, 0)

    @pl.when(jnp.logical_not(polar))
    def _():
        keep_own.wait()

    def assemble():
        for dy, copy in copies:
            when_inside(dy, copy.wait_send)
            when_inside(-dy, copy.wait_recv)
        for dy in (1, -1):
            @pl.when(jnp.logical_not(inside(-dy)))
            def _(dy=dy):
                st_c[:, row_dst[dy], :] = jnp.zeros((4, HALO, WIDE), jnp.float32)
                st_l[row_dst[dy], :] = jnp.zeros((HALO, 128), jnp.float32)
                st_r[row_dst[dy], :] = jnp.zeros((HALO, 128), jnp.float32)

        lane_ext = lax.broadcasted_iota(jnp.int32, (EXT, 128), 1)
        edge = HALO + COLS - 384
        for c in range(4):
            mid = pltpu.roll(st_c[c], HALO, 1)
            ext[c, :, 128:384] = mid[:, 128:384]
            left = pltpu.roll(st_l[...], 128 - c * HALO, 1) if c else st_l[...]
            ext[c, :, 0:128] = jnp.where(lane_ext < HALO, left, mid[:, 0:128])
            right = pltpu.roll(st_r[...], (edge - c * HALO) % 128, 1)
            right = jnp.where(lane_ext < edge + HALO, right, 0.0)
            ext[c, :, 384:512] = jnp.where(lane_ext >= edge, right, mid[:, 384:512])

        ocean = ext[3]
        row_id = lat * ROWS - HALO + lax.broadcasted_iota(jnp.int32, (EXT, WIDE), 0)
        east_open = ocean * pltpu.roll(ocean, WIDE - 1, 1)
        north_open = jnp.where(row_id == NLAT - 1, 0.0, ocean * pltpu.roll(ocean, EXT - 1, 0))
        opens[0] = east_open
        opens[1] = north_open
        ext[1] = ext[1] * east_open
        ext[2] = ext[2] * north_open
        ext[3] = WAVE * ocean

    def subcycle(_, carry):
        east = ext[1]
        north = ext[2]
        div = east - pltpu.roll(east, 1, 1) + north - pltpu.roll(north, 1, 0)
        surface = ext[0] - ext[3] * div
        ext[0] = surface
        ext[1] = opens[0] * (east - WAVE * (pltpu.roll(surface, WIDE - 1, 1) - surface))
        ext[2] = opens[1] * (north - WAVE * (pltpu.roll(surface, EXT - 1, 0) - surface))
        return carry

    chunks = jnp.where(near_y, NEAR, jnp.where(far, FAR, 0))

    @pl.when(jnp.logical_not(worker))
    def _():
        assemble()

    @pl.when(worker)
    def _():
        load_wh.wait()
        load_wl.wait()
        load_twist.wait()
        load_cutoff.wait()
        first = (jnp.where(north, 0, 2) + core) * ROWS + lon * TILE
        sub = lax.broadcasted_iota(jnp.int32, (TILE, WIDE), 0)
        wave = LON * lax.broadcasted_iota(jnp.int32, (TILE, WIDE), 1)
        limit = jnp.zeros((TILE, WIDE), jnp.int32)
        for i in range(TILE):
            limit = jnp.where(sub == i, cutoff[first + i], limit)
        for s in range(LON):
            m = wave + s
            folded = jnp.minimum(m, NLON - m)
            mask[s] = jnp.where(folded <= limit, 1.0 / NLON, 0.0)
        back_rest[...] = jnp.zeros_like(back_rest)
        q_first = jnp.where(near_y, 0, NEAR)

        @pl.when(near_y)
        def _():
            each_lon(lambda d: arrived(recv_rest.at[0, d], fwd_rest.at[0, d]))

        def chunk(j, _):
            arrived(recv.at[j], fwd_recv.at[j])

            @pl.when(j == jnp.where(near_y, 1, 0))
            def _():
                each_lon(lambda d: arrived(recv_rest.at[1, d], fwd_rest.at[1, d]))

            filter_chunk(
                j, q_first + j, (recv, recv_rest), (back, back_rest), twist, mask, yh, yl, wh, wl, prod
            )

            @pl.when(near_y)
            def _():
                def reply(n):
                    k = n // 2
                    hops = jnp.where(k == 0, 2, jnp.where(k == 3, 0, 2 * k - 1))
                    d = 2 * lax.rem(lon // 2 + hops, LON // 2) + lax.rem(n, 2)
                    push(back.at[j, d], ret.at[j, lon], ret_send.at[j], ret_recv.at[0], d, home)

                each_lon(reply)

            @pl.when(far)
            def _():
                each_lon(lambda d: push(
                    back.at[j, d], relay.at[j, lon], ret_send.at[j], relay_recv.at[j, lon], d, relay_lat
                ))

            @pl.when(near_y & (j == NEAR - 1))
            def _():
                each_lon(lambda d: push(
                    back_rest.at[d], rest_in.at[0, lon], ret_rest, ret_recv.at[1], d, home
                ))

            @pl.when(far & (j == FAR - 1))
            def _():
                each_lon(lambda d: push(
                    back_rest.at[d], relay_rest.at[lon], ret_rest, relay_rests.at[lon], d, relay_lat
                ))

            pl.when(j == FIRST - 1)(assemble)
            lax.fori_loop(0, jnp.where(j >= FIRST, PER_CHUNK, 0), subcycle, 0)
            return 0

        lax.fori_loop(0, chunks, chunk, 0)

    load_thick.wait()
    total = thick[0]
    for k in range(1, LEV):
        total = total + thick[k]
    for k in range(LEV):
        weights[k : k + 1, :] = jnp.full((1, 128), thick[k]) / total

    left_over = SUB - PER_CHUNK * jnp.maximum(chunks - FIRST, 0)
    lax.fori_loop(0, left_over, subcycle, 0)

    inner = slice(HALO, HALO + ROWS)
    for c in range(3):
        moved = pltpu.roll(ext[c, inner, :], WIDE - HALO, 1)
        state_out[c] = moved[:, :COLS]
    for c in range(2):
        moved = pltpu.roll(opens[c, inner, :], WIDE - HALO, 1)
        open_out[c] = moved[:, :COLS]

    @pl.when(relays)
    def _():
        def pass_chunk(j, _):
            def pass_on(t):
                arrived(relay.at[j, t], relay_recv.at[j, t])
                push(relay.at[j, t], ret.at[NEAR + j, t], relay_send.at[0], ret_recv.at[0], lon, home)

            each_lon(pass_on)
            return 0

        lax.fori_loop(0, FAR, pass_chunk, 0)

        def pass_rest(t):
            arrived(relay_rest.at[t], relay_rests.at[t])
            push(relay_rest.at[t], rest_in.at[1, t], relay_send.at[1], ret_recv.at[2], lon, home)

        each_lon(pass_rest)
        arrived(relay, relay_send.at[0])
        arrived(relay_rest, relay_send.at[1])

    @pl.when(worker)
    def _():
        def sent(j, _):
            arrived(back.at[j], ret_send.at[j])
            return 0

        lax.fori_loop(0, chunks, sent, 0)
        arrived(back_rest, ret_rest)

    @pl.when(polar)
    def _():
        arrived(packed, fwd_send.at[0])
        arrived(rest_out.at[0], fwd_send.at[1])
        arrived(rest_out.at[1], fwd_send.at[2])
        arrived(rest_out.at[1], fwd_send.at[3])
        arrived(ret, ret_recv.at[0])
        arrived(rest_in.at[0], ret_recv.at[1])
        arrived(rest_in.at[1], ret_recv.at[2])


def final_kernel(
    weights, held, ret, rest_in, state, opens, tracers_out, velocity_out, sea_out, tracers, velocity, sems
):
    lat = lax.axis_index("lat")
    polar = (lat < POLE_DEV) | (lat >= LAT - POLE_DEV)
    save_sea = pltpu.make_async_copy(state.at[0], sea_out, sems.at[2])
    save_sea.start()

    def finish(tile, lo, hi, load):
        here = pl.ds(pl.multiple_of(tile * TILE, TILE), TILE)
        pairs = [[load(c, k) for k in range(LEV)] for c in range(2)]
        for c in range(2):
            column = None
            for k in range(LEV):
                tracers[c, k, here, lo:hi] = pairs[c][k][0]
                term = weights[k : k + 1, 0 : hi - lo] * pairs[c][k][1]
                column = term if column is None else column + term
            shift = state[1 + c, here, lo:hi] - column
            gate = opens[c, here, lo:hi]
            for k in range(LEV):
                velocity[c, k, here, lo:hi] = gate * (pairs[c][k][1] + shift)

    def step(tile, _):
        here = pl.ds(pl.multiple_of(tile * TILE, TILE), TILE)

        @pl.when(polar)
        def _():
            for lo in range(0, MAIN, 128):
                finish(tile, lo, lo + 128, lambda c, k: (
                    ret[c * LEV + k, tile, :, lo : lo + 128],
                    ret[c * LEV + k, tile, :, MAIN + lo : MAIN + lo + 128],
                ))

            def tail(c, k):
                q = c * LEV + k
                first, second = unpack_tail(q, ret[q, tile, :, 2 * MAIN : PACK], rest_in[int(q >= NEAR), tile])
                return first[:, :TAIL], second[:, :TAIL]

            finish(tile, MAIN, COLS, tail)

        @pl.when(jnp.logical_not(polar))
        def _():
            for lo, hi in ((0, 128), (128, 256), (256, MAIN), (MAIN, COLS)):
                finish(tile, lo, hi, lambda c, k: (held[0, c, k, here, lo:hi], held[1, c, k, here, lo:hi]))

        pltpu.make_async_copy(tracers.at[:, :, here, :], tracers_out.at[:, :, here, :], sems.at[0]).start()
        pltpu.make_async_copy(velocity.at[:, :, here, :], velocity_out.at[:, :, here, :], sems.at[1]).start()
        return 0

    lax.fori_loop(0, LON, step, 0)
    pltpu.make_async_copy(tracers, tracers_out, sems.at[0]).wait()
    pltpu.make_async_copy(velocity, velocity_out, sems.at[1]).wait()
    save_sea.wait()


def body(fields, thickness, cutoff, barotropic, land_sea):
    f32 = jnp.float32
    high, low, twist = tables()
    sds = jax.ShapeDtypeStruct
    split = fields.reshape(2, 2, LEV, ROWS, COLS)
    held, ret, rest, state, opens, weights = pl.pallas_call(
        wave_kernel,
        out_shape=(
            VMEM((2, 2, LEV, ROWS, COLS), f32),
            VMEM((CHUNKS, LON, TILE, PACK), f32),
            VMEM((2, LON, TILE, 128), f32),
            VMEM((3, ROWS, COLS), f32),
            VMEM((2, ROWS, COLS), f32),
            VMEM((LEV, 128), f32),
        ),
        in_specs=[pl.BlockSpec(memory_space=pltpu.HBM)] * 8,
        out_specs=[pl.BlockSpec(memory_space=VMEM)] * 6,
        scratch_shapes=[
            pltpu.SMEM((2 * POLE_DEV * ROWS,), jnp.int32),
            VMEM((2, LON, WIDE), f32),
            pltpu.SMEM((LEV,), f32),
            VMEM((NEAR, LON, TILE, PACK), f32),
            VMEM((2, LON, TILE, 128), f32),
            VMEM((NEAR, LON, TILE, PACK), f32),
            VMEM((LON, TILE, 128), f32),
            VMEM((FAR, LON, TILE, PACK), f32),
            VMEM((LON, TILE, 128), f32),
            VMEM((2, ROWS, 128), f32),
            VMEM((CHUNKS, LON, TILE, PACK), f32),
            VMEM((2, ROWS, 128), f32),
            VMEM((WIDE, 2 * WIDE), jnp.bfloat16),
            VMEM((WIDE, 2 * WIDE), jnp.bfloat16),
            VMEM((128, WIDE), jnp.bfloat16),
            VMEM((128, WIDE), jnp.bfloat16),
            VMEM((128, 2 * WIDE), f32),
            VMEM((LON, TILE, WIDE), f32),
            VMEM((3, ROWS, COLS), f32),
            VMEM((ROWS, COLS), jnp.int32),
            VMEM((4, ROWS, WIDE), f32),
            VMEM((ROWS, 128), f32),
            VMEM((ROWS, 128), f32),
            VMEM((4, EXT, WIDE), f32),
            VMEM((EXT, 128), f32),
            VMEM((EXT, 128), f32),
            VMEM((4, EXT, WIDE), f32),
            VMEM((2, EXT, WIDE), f32),
            pltpu.SemaphoreType.DMA((4,)),
            pltpu.SemaphoreType.DMA((NEAR,)),
            pltpu.SemaphoreType.DMA((2, LON)),
            pltpu.SemaphoreType.DMA((NEAR,)),
            pltpu.SemaphoreType.DMA,
            pltpu.SemaphoreType.DMA((3,)),
            pltpu.SemaphoreType.DMA((FAR, LON)),
            pltpu.SemaphoreType.DMA((LON,)),
            pltpu.SemaphoreType.DMA((2,)),
            pltpu.SemaphoreType.DMA((8,)),
            pltpu.SemaphoreType.DMA((8,)),
            pltpu.SemaphoreType.DMA((8,)),
            pltpu.SemaphoreType.DMA((CHUNKS,)),
        ],
        compiler_params=pltpu.CompilerParams(
            collective_id=0, has_side_effects=True, vmem_limit_bytes=53 * 1024 * 1024
        ),
        name="wave",
    )(split, barotropic, land_sea, cutoff, jnp.asarray(high), jnp.asarray(low), jnp.asarray(twist), thickness)

    return tuple(
        pl.pallas_call(
            final_kernel,
            out_shape=(
                sds((2, LEV, ROWS, COLS), f32),
                sds((2, LEV, ROWS, COLS), f32),
                sds((ROWS, COLS), f32),
            ),
            in_specs=[
                pl.BlockSpec(memory_space=VMEM),
                pl.BlockSpec(memory_space=VMEM),
                pl.BlockSpec(memory_space=VMEM),
                pl.BlockSpec(memory_space=VMEM),
                pl.BlockSpec(memory_space=VMEM),
                pl.BlockSpec(memory_space=VMEM),
            ],
            out_specs=[pl.BlockSpec(memory_space=ANY)] * 3,
            scratch_shapes=[
                VMEM((2, LEV, ROWS, COLS), f32),
                VMEM((2, LEV, ROWS, COLS), f32),
                pltpu.SemaphoreType.DMA((3,)),
            ],
            compiler_params=pltpu.CompilerParams(vmem_limit_bytes=16 * 1024 * 1024),
            name="final",
        )(weights, held, ret, rest, state, opens)
    )


def solution(mesh):
    return jax.shard_map(
        body,
        mesh=mesh,
        in_specs=(P(None, None, "lat", "lon"), P(), P(), P(None, "lat", "lon"), P("lat", "lon")),
        out_specs=(P(None, None, "lat", "lon"), P(None, None, "lat", "lon"), P("lat", "lon")),
        check_vma=False,
    )
```

```python
import math

import jax
import jax.numpy as jnp
import ml_dtypes
import numpy as np
from jax import lax
from jax.experimental import pallas as pl
from jax.experimental.pallas import tpu as pltpu
from jax.sharding import PartitionSpec as P

MESH = pl.DeviceIdType.MESH
ANY = pl.ANY
VMEM = pltpu.VMEM

WAVE = 0.65
SUB = 20
POLE_DEV = 2
LON, LAT = 8, 16
ROWS, COLS = 64, 450
NLON = LON * COLS
NLAT = LAT * ROWS
LEV = 8
NF = 4
WIDE = 512
HALO = 24
EXT = ROWS + 2 * HALO
TILE = 8
CHUNKS = 16
NEAR = 11
FAR = CHUNKS - NEAR
PER_CHUNK = 2
FIRST = 2
MAIN = 384
PACK = 2 * MAIN + 128
TAIL = COLS - MAIN
LANE_TILES = ((0, 128), (128, 256), (256, 384), (384, WIDE))


def tables():
    r = np.arange(COLS)
    angle = 2.0 * np.pi * ((r[:, None] * r[None, :]) % COLS) / COLS
    full = np.zeros((WIDE, 2 * WIDE), np.float64)
    full[:COLS, :COLS] = np.cos(angle)
    full[:COLS, WIDE : WIDE + COLS] = np.sin(angle)
    full = full.astype(np.float32)
    high = full.astype(ml_dtypes.bfloat16)
    low = (full - high.astype(np.float32)).astype(ml_dtypes.bfloat16)
    turn = 2.0 * np.pi * (np.arange(LON)[:, None] * r[None, :]) / NLON
    twist = np.zeros((2, LON, WIDE), np.float32)
    twist[0, :, :COLS] = np.cos(turn)
    twist[1, :, :COLS] = np.sin(turn)
    return high, low, twist


def butterflies(z, sign):
    n = len(z)
    if n == 1:
        return z
    even = butterflies(z[0::2], sign)
    odd = butterflies(z[1::2], sign)
    low, high = [], []
    for k in range(n // 2):
        er, ei = even[k]
        tr, ti = odd[k]
        if 4 * k == n:
            tr, ti = (-ti, tr) if sign > 0 else (ti, -tr)
        elif k:
            c = math.cos(2.0 * math.pi * k / n)
            s = sign * math.sin(2.0 * math.pi * k / n)
            tr, ti = c * tr - s * ti, c * ti + s * tr
        low.append((er + tr, ei + ti))
        high.append((er - tr, ei - ti))
    return low + high


def put_split(high_ref, low_ref, s, lanes, re, im):
    value = jnp.concatenate([re, im], axis=0)
    top = value.astype(jnp.bfloat16)
    rows = slice(s * 16, s * 16 + 16)
    high_ref[rows, lanes[0] : lanes[1]] = top
    low_ref[rows, lanes[0] : lanes[1]] = (value - top.astype(jnp.float32)).astype(jnp.bfloat16)


def multiply(high_ref, low_ref, wh_ref, wl_ref, out_ref):
    for block in range(4):
        cols = slice(block * 256, (block + 1) * 256)
        out_ref[:, cols] = (
            jnp.dot(high_ref[...], wh_ref[:, cols], preferred_element_type=jnp.float32)
            + jnp.dot(low_ref[...], wh_ref[:, cols], preferred_element_type=jnp.float32)
            + jnp.dot(high_ref[...], wl_ref[:, cols], preferred_element_type=jnp.float32)
        )


def lanes_of(rows):
    return lax.broadcasted_iota(jnp.int32, (rows, 128), 1)


def pack_tail(first, second):
    return jnp.where(lanes_of(first.shape[0]) < 64, first, pltpu.roll(second, 64, 1))


def pack_rest(q, first, second, rest):
    slot = lanes_of(first.shape[0]) // 2
    rest = jnp.where(slot == 2 * q, pltpu.roll(first, lax.rem(4 * q + 64, 128), 1), rest)
    return jnp.where(slot == 2 * q + 1, pltpu.roll(second, lax.rem(4 * q + 66, 128), 1), rest)


def unpack_tail(q, tail, rest):
    lane = lanes_of(tail.shape[0])
    first = jnp.where(lane < 64, tail, pltpu.roll(rest, (192 - 4 * q) % 128, 1))
    second = jnp.where(lane < 64, pltpu.roll(tail, 64, 1), pltpu.roll(rest, (190 - 4 * q) % 128, 1))
    return jnp.where(lane < TAIL, first, 0.0), jnp.where(lane < TAIL, second, 0.0)


def filter_chunk(j, q, recv, back, twist, mask, yh, yl, wh, wl, prod):
    got, recv_rest = recv
    back, back_rest = back
    for lo, hi in LANE_TILES:
        if lo < MAIN:
            z = [(got[j, d, :, lo:hi], got[j, d, :, MAIN + lo : MAIN + hi]) for d in range(LON)]
        else:
            part = jnp.minimum(q, 1)
            z = [unpack_tail(q, got[j, d, :, 2 * MAIN : PACK], recv_rest[part, d]) for d in range(LON)]
        y = butterflies(z, -1)
        for s in range(LON):
            re, im = y[s]
            if s:
                c = twist[0, s : s + 1, lo:hi]
                n = twist[1, s : s + 1, lo:hi]
                re, im = re * c + im * n, im * c - re * n
            put_split(yh, yl, s, (lo, hi), re, im)
    multiply(yh, yl, wh, wl, prod)
    for lo, hi in LANE_TILES:
        for s in range(LON):
            a = slice(s * 16, s * 16 + 8)
            b = slice(s * 16 + 8, s * 16 + 16)
            keep = mask[s, :, lo:hi]
            re = (prod[a, lo:hi] + prod[b, WIDE + lo : WIDE + hi]) * keep
            im = (prod[b, lo:hi] - prod[a, WIDE + lo : WIDE + hi]) * keep
            put_split(yh, yl, s, (lo, hi), re, im)
    multiply(yh, yl, wh, wl, prod)
    for lo, hi in LANE_TILES:
        z = []
        for s in range(LON):
            a = slice(s * 16, s * 16 + 8)
            b = slice(s * 16 + 8, s * 16 + 16)
            re = prod[a, lo:hi] - prod[b, WIDE + lo : WIDE + hi]
            im = prod[b, lo:hi] + prod[a, WIDE + lo : WIDE + hi]
            if s:
                c = twist[0, s : s + 1, lo:hi]
                n = twist[1, s : s + 1, lo:hi]
                re, im = re * c - im * n, im * c + re * n
            z.append((re, im))
        x = butterflies(z, 1)
        for d in range(LON):
            if lo < MAIN:
                back[j, d, :, lo:hi] = x[d][0]
                back[j, d, :, MAIN + lo : MAIN + hi] = x[d][1]
            else:
                back[j, d, :, 2 * MAIN : PACK] = pack_tail(*x[d])
                back_rest[d] = pack_rest(q, *x[d], back_rest[d])


def wave_kernel(
    fields, baro, land, cutoff_hbm, wh_hbm, wl_hbm, twist_hbm, thick_hbm,
    held, ret, rest_in, state_out, open_out, weights,
    cutoff, twist, thick,
    recv, recv_rest, back, back_rest, relay, relay_rest, stage, packed, rest_out, wh, wl, yh, yl, prod, mask,
    own, own_land, src4, edge_r, edge_l, st_c, st_l, st_r, ext, opens,
    fwd_send, fwd_recv, fwd_rest, ret_send, ret_rest, ret_recv,
    relay_recv, relay_rests, relay_send, halo_send, halo_recv, local_sem, load_sem,
):
    lon = lax.axis_index("lon")
    lat = lax.axis_index("lat")
    pair = lat // 2
    core = lax.rem(lat, 2)
    north = lax.rem(pair, 4) < 2
    polar = (pair == 0) | (pair == 7)
    near_y = (pair == 3) | (pair == 4)
    relays = (pair == 1) | (pair == 6)
    far = (pair == 2) | (pair == 5)
    worker = near_y | far
    home = jnp.where(north, 0, LAT - 2) + core
    y_lat = jnp.where(north, 8, 6) + core
    relay_lat = jnp.where(north, 2, 12) + core
    far_lat = jnp.where(north, 10, 4) + core

    load_state = pltpu.make_async_copy(baro, own, local_sem.at[0])
    load_land = pltpu.make_async_copy(land, own_land, local_sem.at[1])
    load_wh = pltpu.make_async_copy(wh_hbm, wh, local_sem.at[2])
    load_wl = pltpu.make_async_copy(wl_hbm, wl, local_sem.at[3])
    load_twist = pltpu.make_async_copy(twist_hbm, twist, local_sem.at[5])
    load_cutoff = pltpu.make_async_copy(cutoff_hbm, cutoff, local_sem.at[6])
    load_thick = pltpu.make_async_copy(thick_hbm, thick, local_sem.at[7])
    load_thick.start()

    keep_own = pltpu.make_async_copy(fields, held, local_sem.at[4])

    @pl.when(worker)
    def _():
        load_wh.start()
        load_wl.start()
        load_twist.start()
        load_cutoff.start()

    def load_chunk(q):
        at = (q // LEV, lax.rem(q, LEV))
        return pltpu.make_async_copy(
            fields.at[:, at[0], at[1]], held.at[:, at[0], at[1]], load_sem.at[q]
        )

    @pl.when(polar)
    def _():
        load_chunk(0).start()

    load_state.start()
    load_land.start()

    @pl.when(polar)
    def _():
        def start(q, _):
            load_chunk(q).start()
            return 0

        lax.fori_loop(1, CHUNKS, start, 0)

    @pl.when(jnp.logical_not(polar))
    def _():
        keep_own.start()

    sides = [(dx, dy) for dy in (0, 1, -1) for dx in (-1, 0, 1) if (dx, dy) != (0, 0)]

    def near(dx, dy):
        return {"lon": lax.rem(lon + dx + LON, LON), "lat": lax.rem(lat + dy + LAT, LAT)}

    def inside(dy):
        return lat < LAT - 1 if dy > 0 else lat > 0

    def when_inside(dy, action):
        if dy == 0:
            action()
        else:
            pl.when(inside(dy))(action)

    barrier = pltpu.get_barrier_semaphore()

    def greet_at(lon_index, lat_index):
        pl.semaphore_signal(
            barrier, inc=1, device_id={"lon": lon_index, "lat": lat_index}, device_id_type=MESH
        )

    def greet_row(lat_index):
        def one(t, _):
            greet_at(t, lat_index)
            return 0

        lax.fori_loop(0, LON, one, 0)

    for dx, dy in sides:
        when_inside(dy, lambda dx=dx, dy=dy: greet_at(near(dx, dy)["lon"], near(dx, dy)["lat"]))

    @pl.when(polar)
    def _():
        greet_row(y_lat)
        greet_row(far_lat)
        greet_at(lon, relay_lat)

    @pl.when(near_y)
    def _():
        greet_row(home)

    @pl.when(far)
    def _():
        greet_row(home)
        greet_row(relay_lat)

    @pl.when(relays)
    def _():
        greet_row(far_lat)
        greet_at(lon, home)

    def rows(t):
        return pl.ds(pl.multiple_of(t * TILE, TILE), TILE)

    def push(src, dst, send_sem, recv_sem, lon_index, lat_index):
        pltpu.make_async_remote_copy(
            src_ref=src, dst_ref=dst, send_sem=send_sem, recv_sem=recv_sem,
            device_id={"lon": lon_index, "lat": lat_index}, device_id_type=MESH,
        ).start()

    def arrived(ref, sem):
        pltpu.make_async_copy(ref, ref, sem).wait()

    def each_lon(action):
        def one(t, _):
            action(t)
            return 0

        lax.fori_loop(0, LON, one, 0)

    def pack_chunk(q, rest):
        load_chunk(q).wait()
        for i in range(2):
            packed[q, :, :, i * MAIN : (i + 1) * MAIN] = held[
                i, q // LEV, lax.rem(q, LEV), :, 0:MAIN
            ].reshape(LON, TILE, MAIN)
            stage[i, :, 0:TAIL] = held[i, q // LEV, lax.rem(q, LEV), :, MAIN:COLS]
        packed[q, :, :, 2 * MAIN : PACK] = pack_tail(stage[0], stage[1]).reshape(LON, TILE, 128)
        return pack_rest(q, stage[0], stage[1], rest)

    def send_chunk(q, slot, lat_index):
        each_lon(lambda t: push(
            packed.at[q, t], recv.at[slot, lon], fwd_send.at[0], fwd_recv.at[slot], t, lat_index
        ))

    def send_rest(part, lat_index, sem):
        each_lon(lambda t: push(
            rest_out.at[part, rows(t), :], recv_rest.at[part, lon], fwd_send.at[sem], fwd_rest.at[part, lon],
            t, lat_index,
        ))

    @pl.when(polar)
    def _():
        rest_out[0] = pack_chunk(0, jnp.zeros((ROWS, 128), jnp.float32))

    full = len(sides) - jnp.where((lat == 0) | (lat == LAT - 1), 3, 0)
    extra = jnp.where(polar, 2 * LON + 1, jnp.where(near_y, LON, jnp.where(far, 2 * LON, LON + 1)))
    pl.semaphore_wait(barrier, full + extra)

    @pl.when(polar)
    def _():
        send_rest(0, y_lat, 1)
        send_chunk(0, 0, y_lat)

    load_state.wait()
    load_land.wait()
    for c in range(3):
        src4[c, :, 0:384] = own[c, :, 0:384]
        src4[c, :, 384:COLS] = own[c, :, 384:COLS]
    src4[3, :, 0:384] = own_land[:, 0:384].astype(jnp.float32)
    src4[3, :, 384:COLS] = own_land[:, 384:COLS].astype(jnp.float32)
    src4[:, :, COLS:WIDE] = jnp.zeros((4, ROWS, WIDE - COLS), jnp.float32)
    st_c[:, HALO : HALO + ROWS, :] = src4[...]
    lane = lax.broadcasted_iota(jnp.int32, (ROWS, 128), 1)
    right_pack = jnp.zeros((ROWS, 128), jnp.float32)
    left_pack = right_pack
    for c in range(4):
        here = (lane >= c * HALO) & (lane < (c + 1) * HALO)
        right_edge = pltpu.roll(src4[c, :, 384:512], (c * HALO - (COLS - HALO - 384)) % 128, 1)
        left_edge = src4[c, :, 0:128]
        if c:
            left_edge = pltpu.roll(left_edge, c * HALO, 1)
        right_pack = jnp.where(here, right_edge, right_pack)
        left_pack = jnp.where(here, left_edge, left_pack)
    edge_r[...] = right_pack
    edge_l[...] = left_pack

    row_src = {1: slice(ROWS - HALO, ROWS), 0: slice(0, ROWS), -1: slice(0, HALO)}
    row_dst = {1: slice(0, HALO), 0: slice(HALO, HALO + ROWS), -1: slice(HALO + ROWS, EXT)}
    copies = []
    for n, (dx, dy) in enumerate(sides):
        if dx == 0:
            src = src4.at[:, row_src[dy], :]
            dst = st_c.at[:, row_dst[dy], :]
        else:
            src = (edge_r if dx == 1 else edge_l).at[row_src[dy], :]
            dst = (st_l if dx == 1 else st_r).at[row_dst[dy], :]
        copy = pltpu.make_async_remote_copy(
            src_ref=src, dst_ref=dst, send_sem=halo_send.at[n], recv_sem=halo_recv.at[n],
            device_id=near(dx, dy), device_id_type=MESH,
        )
        when_inside(dy, copy.start)
        copies.append((dy, copy))

    @pl.when(polar)
    def _():
        rest = pack_chunk(NEAR, jnp.zeros((ROWS, 128), jnp.float32))
        send_chunk(NEAR, 0, far_lat)
        rest = lax.fori_loop(1, NEAR, pack_chunk, rest)
        rest_out[1] = lax.fori_loop(NEAR + 1, CHUNKS, pack_chunk, rest)
        send_rest(1, y_lat, 2)
        send_rest(1, far_lat, 3)

        def step(k, _):
            pl.when(k > 0)(lambda: send_chunk(NEAR + k, k, far_lat))
            send_chunk(2 * k + 1, 2 * k + 1, y_lat)
            send_chunk(2 * k + 2, 2 * k + 2, y_lat)
            return 0

        lax.fori_loop(0, FAR, step, 0)

    @pl.when(jnp.logical_not(polar))
    def _():
        keep_own.wait()

    def assemble():
        for dy, copy in copies:
            when_inside(dy, copy.wait_send)
            when_inside(-dy, copy.wait_recv)
        for dy in (1, -1):
            @pl.when(jnp.logical_not(inside(-dy)))
            def _(dy=dy):
                st_c[:, row_dst[dy], :] = jnp.zeros((4, HALO, WIDE), jnp.float32)
                st_l[row_dst[dy], :] = jnp.zeros((HALO, 128), jnp.float32)
                st_r[row_dst[dy], :] = jnp.zeros((HALO, 128), jnp.float32)

        lane_ext = lax.broadcasted_iota(jnp.int32, (EXT, 128), 1)
        edge = HALO + COLS - 384
        for c in range(4):
            mid = pltpu.roll(st_c[c], HALO, 1)
            ext[c, :, 128:384] = mid[:, 128:384]
            left = pltpu.roll(st_l[...], 128 - c * HALO, 1) if c else st_l[...]
            ext[c, :, 0:128] = jnp.where(lane_ext < HALO, left, mid[:, 0:128])
            right = pltpu.roll(st_r[...], (edge - c * HALO) % 128, 1)
            right = jnp.where(lane_ext < edge + HALO, right, 0.0)
            ext[c, :, 384:512] = jnp.where(lane_ext >= edge, right, mid[:, 384:512])

        ocean = ext[3]
        row_id = lat * ROWS - HALO + lax.broadcasted_iota(jnp.int32, (EXT, WIDE), 0)
        east_open = ocean * pltpu.roll(ocean, WIDE - 1, 1)
        north_open = jnp.where(row_id == NLAT - 1, 0.0, ocean * pltpu.roll(ocean, EXT - 1, 0))
        opens[0] = east_open
        opens[1] = north_open
        ext[1] = ext[1] * east_open
        ext[2] = ext[2] * north_open
        ext[3] = WAVE * ocean

    def subcycle(_, carry):
        east = ext[1]
        north = ext[2]
        div = east - pltpu.roll(east, 1, 1) + north - pltpu.roll(north, 1, 0)
        surface = ext[0] - ext[3] * div
        ext[0] = surface
        ext[1] = opens[0] * (east - WAVE * (pltpu.roll(surface, WIDE - 1, 1) - surface))
        ext[2] = opens[1] * (north - WAVE * (pltpu.roll(surface, EXT - 1, 0) - surface))
        return carry

    chunks = jnp.where(near_y, NEAR, jnp.where(far, FAR, 0))

    @pl.when(jnp.logical_not(worker))
    def _():
        assemble()

    @pl.when(worker)
    def _():
        load_wh.wait()
        load_wl.wait()
        load_twist.wait()
        load_cutoff.wait()
        first = (jnp.where(north, 0, 2) + core) * ROWS + lon * TILE
        sub = lax.broadcasted_iota(jnp.int32, (TILE, WIDE), 0)
        wave = LON * lax.broadcasted_iota(jnp.int32, (TILE, WIDE), 1)
        limit = jnp.zeros((TILE, WIDE), jnp.int32)
        for i in range(TILE):
            limit = jnp.where(sub == i, cutoff[first + i], limit)
        for s in range(LON):
            m = wave + s
            folded = jnp.minimum(m, NLON - m)
            mask[s] = jnp.where(folded <= limit, 1.0 / NLON, 0.0)
        back_rest[...] = jnp.zeros_like(back_rest)
        q_first = jnp.where(near_y, 0, NEAR)

        @pl.when(near_y)
        def _():
            each_lon(lambda d: arrived(recv_rest.at[0, d], fwd_rest.at[0, d]))

        def chunk(j, _):
            arrived(recv.at[j], fwd_recv.at[j])

            @pl.when(j == jnp.where(near_y, 1, 0))
            def _():
                each_lon(lambda d: arrived(recv_rest.at[1, d], fwd_rest.at[1, d]))

            filter_chunk(
                j, q_first + j, (recv, recv_rest), (back, back_rest), twist, mask, yh, yl, wh, wl, prod
            )

            @pl.when(near_y)
            def _():
                def reply(n):
                    k = n // 2
                    hops = jnp.where(k == 0, 2, jnp.where(k == 3, 0, 2 * k - 1))
                    d = 2 * lax.rem(lon // 2 + hops, LON // 2) + lax.rem(n, 2)
                    push(back.at[j, d], ret.at[j, lon], ret_send.at[j], ret_recv.at[0], d, home)

                each_lon(reply)

            @pl.when(far)
            def _():
                each_lon(lambda d: push(
                    back.at[j, d], relay.at[j, lon], ret_send.at[j], relay_recv.at[j, lon], d, relay_lat
                ))

            @pl.when(near_y & (j == NEAR - 1))
            def _():
                each_lon(lambda d: push(
                    back_rest.at[d], rest_in.at[0, lon], ret_rest, ret_recv.at[1], d, home
                ))

            @pl.when(far & (j == FAR - 1))
            def _():
                each_lon(lambda d: push(
                    back_rest.at[d], relay_rest.at[lon], ret_rest, relay_rests.at[lon], d, relay_lat
                ))

            pl.when(j == FIRST - 1)(assemble)
            lax.fori_loop(0, jnp.where(j >= FIRST, PER_CHUNK, 0), subcycle, 0)
            return 0

        lax.fori_loop(0, chunks, chunk, 0)

    load_thick.wait()
    total = thick[0]
    for k in range(1, LEV):
        total = total + thick[k]
    for k in range(LEV):
        weights[k : k + 1, :] = jnp.full((1, 128), thick[k]) / total

    left_over = SUB - PER_CHUNK * jnp.maximum(chunks - FIRST, 0)
    lax.fori_loop(0, left_over, subcycle, 0)

    inner = slice(HALO, HALO + ROWS)
    for c in range(3):
        moved = pltpu.roll(ext[c, inner, :], WIDE - HALO, 1)
        state_out[c] = moved[:, :COLS]
    for c in range(2):
        moved = pltpu.roll(opens[c, inner, :], WIDE - HALO, 1)
        open_out[c] = moved[:, :COLS]

    @pl.when(relays)
    def _():
        def pass_chunk(j, _):
            def pass_on(t):
                arrived(relay.at[j, t], relay_recv.at[j, t])
                push(relay.at[j, t], ret.at[NEAR + j, t], relay_send.at[0], ret_recv.at[0], lon, home)

            each_lon(pass_on)
            return 0

        lax.fori_loop(0, FAR, pass_chunk, 0)

        def pass_rest(t):
            arrived(relay_rest.at[t], relay_rests.at[t])
            push(relay_rest.at[t], rest_in.at[1, t], relay_send.at[1], ret_recv.at[2], lon, home)

        each_lon(pass_rest)
        arrived(relay, relay_send.at[0])
        arrived(relay_rest, relay_send.at[1])

    @pl.when(worker)
    def _():
        def sent(j, _):
            arrived(back.at[j], ret_send.at[j])
            return 0

        lax.fori_loop(0, chunks, sent, 0)
        arrived(back_rest, ret_rest)

    @pl.when(polar)
    def _():
        arrived(packed, fwd_send.at[0])
        arrived(rest_out.at[0], fwd_send.at[1])
        arrived(rest_out.at[1], fwd_send.at[2])
        arrived(rest_out.at[1], fwd_send.at[3])
        arrived(ret, ret_recv.at[0])
        arrived(rest_in.at[0], ret_recv.at[1])
        arrived(rest_in.at[1], ret_recv.at[2])


def final_kernel(
    weights, held, ret, rest_in, state, opens, tracers_out, velocity_out, sea_out, tracers, velocity, sems
):
    lat = lax.axis_index("lat")
    polar = (lat < POLE_DEV) | (lat >= LAT - POLE_DEV)
    save_sea = pltpu.make_async_copy(state.at[0], sea_out, sems.at[2])
    save_sea.start()

    def finish(tile, lo, hi, load):
        here = pl.ds(pl.multiple_of(tile * TILE, TILE), TILE)
        pairs = [[load(c, k) for k in range(LEV)] for c in range(2)]
        for c in range(2):
            column = None
            for k in range(LEV):
                tracers[c, k, here, lo:hi] = pairs[c][k][0]
                term = weights[k : k + 1, 0 : hi - lo] * pairs[c][k][1]
                column = term if column is None else column + term
            shift = state[1 + c, here, lo:hi] - column
            gate = opens[c, here, lo:hi]
            for k in range(LEV):
                velocity[c, k, here, lo:hi] = gate * (pairs[c][k][1] + shift)

    def step(tile, _):
        here = pl.ds(pl.multiple_of(tile * TILE, TILE), TILE)

        @pl.when(polar)
        def _():
            for lo in range(0, MAIN, 128):
                finish(tile, lo, lo + 128, lambda c, k: (
                    ret[c * LEV + k, tile, :, lo : lo + 128],
                    ret[c * LEV + k, tile, :, MAIN + lo : MAIN + lo + 128],
                ))

            def tail(c, k):
                q = c * LEV + k
                first, second = unpack_tail(q, ret[q, tile, :, 2 * MAIN : PACK], rest_in[int(q >= NEAR), tile])
                return first[:, :TAIL], second[:, :TAIL]

            finish(tile, MAIN, COLS, tail)

        @pl.when(jnp.logical_not(polar))
        def _():
            for lo, hi in ((0, 128), (128, 256), (256, MAIN), (MAIN, COLS)):
                finish(tile, lo, hi, lambda c, k: (held[0, c, k, here, lo:hi], held[1, c, k, here, lo:hi]))

        pltpu.make_async_copy(tracers.at[:, :, here, :], tracers_out.at[:, :, here, :], sems.at[0]).start()
        pltpu.make_async_copy(velocity.at[:, :, here, :], velocity_out.at[:, :, here, :], sems.at[1]).start()
        return 0

    lax.fori_loop(0, LON, step, 0)
    pltpu.make_async_copy(tracers, tracers_out, sems.at[0]).wait()
    pltpu.make_async_copy(velocity, velocity_out, sems.at[1]).wait()
    save_sea.wait()


def body(fields, thickness, cutoff, barotropic, land_sea):
    f32 = jnp.float32
    high, low, twist = tables()
    sds = jax.ShapeDtypeStruct
    split = fields.reshape(2, 2, LEV, ROWS, COLS)
    held, ret, rest, state, opens, weights = pl.pallas_call(
        wave_kernel,
        out_shape=(
            VMEM((2, 2, LEV, ROWS, COLS), f32),
            VMEM((CHUNKS, LON, TILE, PACK), f32),
            VMEM((2, LON, TILE, 128), f32),
            VMEM((3, ROWS, COLS), f32),
            VMEM((2, ROWS, COLS), f32),
            VMEM((LEV, 128), f32),
        ),
        in_specs=[pl.BlockSpec(memory_space=pltpu.HBM)] * 8,
        out_specs=[pl.BlockSpec(memory_space=VMEM)] * 6,
        scratch_shapes=[
            pltpu.SMEM((2 * POLE_DEV * ROWS,), jnp.int32),
            VMEM((2, LON, WIDE), f32),
            pltpu.SMEM((LEV,), f32),
            VMEM((NEAR, LON, TILE, PACK), f32),
            VMEM((2, LON, TILE, 128), f32),
            VMEM((NEAR, LON, TILE, PACK), f32),
            VMEM((LON, TILE, 128), f32),
            VMEM((FAR, LON, TILE, PACK), f32),
            VMEM((LON, TILE, 128), f32),
            VMEM((2, ROWS, 128), f32),
            VMEM((CHUNKS, LON, TILE, PACK), f32),
            VMEM((2, ROWS, 128), f32),
            VMEM((WIDE, 2 * WIDE), jnp.bfloat16),
            VMEM((WIDE, 2 * WIDE), jnp.bfloat16),
            VMEM((128, WIDE), jnp.bfloat16),
            VMEM((128, WIDE), jnp.bfloat16),
            VMEM((128, 2 * WIDE), f32),
            VMEM((LON, TILE, WIDE), f32),
            VMEM((3, ROWS, COLS), f32),
            VMEM((ROWS, COLS), jnp.int32),
            VMEM((4, ROWS, WIDE), f32),
            VMEM((ROWS, 128), f32),
            VMEM((ROWS, 128), f32),
            VMEM((4, EXT, WIDE), f32),
            VMEM((EXT, 128), f32),
            VMEM((EXT, 128), f32),
            VMEM((4, EXT, WIDE), f32),
            VMEM((2, EXT, WIDE), f32),
            pltpu.SemaphoreType.DMA((4,)),
            pltpu.SemaphoreType.DMA((NEAR,)),
            pltpu.SemaphoreType.DMA((2, LON)),
            pltpu.SemaphoreType.DMA((NEAR,)),
            pltpu.SemaphoreType.DMA,
            pltpu.SemaphoreType.DMA((3,)),
            pltpu.SemaphoreType.DMA((FAR, LON)),
            pltpu.SemaphoreType.DMA((LON,)),
            pltpu.SemaphoreType.DMA((2,)),
            pltpu.SemaphoreType.DMA((8,)),
            pltpu.SemaphoreType.DMA((8,)),
            pltpu.SemaphoreType.DMA((8,)),
            pltpu.SemaphoreType.DMA((CHUNKS,)),
        ],
        compiler_params=pltpu.CompilerParams(
            collective_id=0, has_side_effects=True, vmem_limit_bytes=53 * 1024 * 1024
        ),
        name="wave",
    )(split, barotropic, land_sea, cutoff, jnp.asarray(high), jnp.asarray(low), jnp.asarray(twist), thickness)

    return tuple(
        pl.pallas_call(
            final_kernel,
            out_shape=(
                sds((2, LEV, ROWS, COLS), f32),
                sds((2, LEV, ROWS, COLS), f32),
                sds((ROWS, COLS), f32),
            ),
            in_specs=[
                pl.BlockSpec(memory_space=VMEM),
                pl.BlockSpec(memory_space=VMEM),
                pl.BlockSpec(memory_space=VMEM),
                pl.BlockSpec(memory_space=VMEM),
                pl.BlockSpec(memory_space=VMEM),
                pl.BlockSpec(memory_space=VMEM),
            ],
            out_specs=[pl.BlockSpec(memory_space=ANY)] * 3,
            scratch_shapes=[
                VMEM((2, LEV, ROWS, COLS), f32),
                VMEM((2, LEV, ROWS, COLS), f32),
                pltpu.SemaphoreType.DMA((3,)),
            ],
            compiler_params=pltpu.CompilerParams(vmem_limit_bytes=16 * 1024 * 1024),
            name="final",
        )(weights, held, ret, rest, state, opens)
    )


def solution(mesh):
    return jax.shard_map(
        body,
        mesh=mesh,
        in_specs=(P(None, None, "lat", "lon"), P(), P(), P(None, "lat", "lon"), P("lat", "lon")),
        out_specs=(P(None, None, "lat", "lon"), P(None, None, "lat", "lon"), P("lat", "lon")),
        check_vma=False,
    )
```
